128 devices in a mesh: dp: 1, ty: 16 (over z, y), tx: 8 (over x, core).
Axes of the slice: x: 4, y: 4, z: 4, core: 2. Of those that a mesh axis runs over, the one named last changes fastest.
Arguments:
- x_in: bfloat16 [16, 512, 4096], P(('dp', 'ty'), None, 'tx')
- w_q: bfloat16 [4096, 4096], P('tx', 'ty')
- w_k: bfloat16 [4096, 4096], P('tx', 'ty')
- w_v: bfloat16 [4096, 4096], P('tx', 'ty')
- w_o: bfloat16 [4096, 4096], P('ty', 'tx')
- w_gate: bfloat16 [4096, 11008], P('tx', 'ty')
- w_up: bfloat16 [4096, 11008], P('tx', 'ty')
- w_down: bfloat16 [11008, 4096], P('ty', 'tx')
Outputs:
- output: bfloat16 [16, 512, 4096], P(('dp', 'ty'), None, 'tx')
All inputs are finite; a program needn't handle non-finite values.
Results may differ from the reference program's by a relative error of at most 0.02.
Values are sent between devices in bfloat16 or wider.
A program may use at most 1 GiB of HBM per device.

```python
import jax
import jax.numpy as jnp
from jax import lax

NSEQ = 16
SEQ = 512
D = 4096
FF = 11008
HEADS = 32

HEAD_DIM = D // HEADS
EPS = 1e-5
THETA = 10000.0


def setup_inputs(seed: int = 0, part: int = 0) -> dict:
    root_key = jax.random.key(seed)
    act_root, weight_root = jax.random.split(root_key)
    part_key = jax.random.fold_in(act_root, part)
    key_tok, key_scale, key_shift, key_slope, key_walk = jax.random.split(part_key, 5)
    tok_noise = jax.random.normal(key_tok, (NSEQ, SEQ, D), jnp.float32)
    tok_scale = jax.random.uniform(key_scale, (NSEQ, SEQ, 1), jnp.float32, 0.5, 2.0)
    tok_shift = 0.5 * jax.random.normal(key_shift, (NSEQ, SEQ, 1), jnp.float32)
    col_slope = jax.random.uniform(key_slope, (), jnp.float32, 1.0, 2.0)
    col_pos = jnp.arange(D, dtype=jnp.float32) / D - 0.5
    col_walk = jnp.cumsum(jax.random.normal(key_walk, (D,), jnp.float32)) * (1.5 * D ** -0.5)
    col_offset = 2.0 * col_slope * col_pos + col_walk
    x_in = (tok_scale * tok_noise + tok_shift + col_offset).astype(jnp.bfloat16)
    weight_keys = jax.random.split(weight_root, 7)

    def draw_weight(key_w, fan_in, fan_out, gain_mul):
        return (gain_mul * fan_in ** -0.5 * jax.random.normal(key_w, (fan_in, fan_out), jnp.float32)).astype(jnp.bfloat16)

    return {
        "x_in": x_in,
        "w_q": draw_weight(weight_keys[0], D, D, 1.5),
        "w_k": draw_weight(weight_keys[1], D, D, 1.5),
        "w_v": draw_weight(weight_keys[2], D, D, 1.0),
        "w_o": draw_weight(weight_keys[3], D, D, 2.5),
        "w_gate": draw_weight(weight_keys[4], D, FF, 1.0),
        "w_up": draw_weight(weight_keys[5], D, FF, 1.0),
        "w_down": draw_weight(weight_keys[6], FF, D, 2.0),
    }


def layer_norm(values_bf):
    values = values_bf.astype(jnp.float32)
    mean_val = jnp.mean(values, axis=-1, keepdims=True)
    var_val = jnp.mean(values * values, axis=-1, keepdims=True) - mean_val * mean_val
    return ((values - mean_val) * lax.rsqrt(var_val + EPS)).astype(jnp.bfloat16)


def rotary(heads_bf):
    seq_len = heads_bf.shape[1]
    half_dim = HEAD_DIM // 2
    inv_freq = THETA ** (-2.0 * jnp.arange(half_dim, dtype=jnp.float32) / HEAD_DIM)
    angles = jnp.arange(seq_len, dtype=jnp.float32)[:, None] * inv_freq[None, :]
    cos_t = jnp.cos(angles)[:, None, :]
    sin_t = jnp.sin(angles)[:, None, :]
    values = heads_bf.astype(jnp.float32)
    lower_half = values[..., :half_dim]
    upper_half = values[..., half_dim:]
    return jnp.concatenate([lower_half * cos_t - upper_half * sin_t, upper_half * cos_t + lower_half * sin_t], axis=-1).astype(jnp.bfloat16)


def causal_attention(q_heads, k_heads, v_heads):
    seq_len = q_heads.shape[1]
    q_block = min(seq_len, 128)
    key_pos = jnp.arange(seq_len)
    k_vals = k_heads.astype(jnp.float32)
    v_vals = v_heads.astype(jnp.float32)

    def one_block(block_idx, out_acc):
        q_start = block_idx * q_block
        q_blk = lax.dynamic_slice_in_dim(q_heads, q_start, q_block, axis=1).astype(jnp.float32)
        scores = jnp.einsum("nqhd,nkhd->nhqk", q_blk, k_vals) * HEAD_DIM ** -0.5
        q_pos = q_start + jnp.arange(q_block)
        allowed = q_pos[:, None] >= key_pos[None, :]
        scores = jnp.where(allowed, scores, -1e30)
        prob_blk = jax.nn.softmax(scores, axis=-1).astype(jnp.bfloat16).astype(jnp.float32)
        blk_out = jnp.einsum("nhqk,nkhd->nqhd", prob_blk, v_vals).astype(jnp.bfloat16)
        return lax.dynamic_update_slice_in_dim(out_acc, blk_out, q_start, axis=1)

    return lax.fori_loop(0, seq_len // q_block, one_block, jnp.zeros_like(q_heads))


def project(rows_bf, weight):
    return jnp.dot(rows_bf, weight, preferred_element_type=jnp.float32).astype(jnp.bfloat16)


def reference(x_in, w_q, w_k, w_v, w_o, w_gate, w_up, w_down):
    n_seqs, seq_len, d_model = x_in.shape
    head_shape = (n_seqs, seq_len, HEADS, HEAD_DIM)
    x_rows = x_in.reshape(n_seqs * seq_len, d_model)
    normed = layer_norm(x_rows)
    q_heads = rotary(project(normed, w_q).reshape(head_shape))
    k_heads = rotary(project(normed, w_k).reshape(head_shape))
    v_heads = project(normed, w_v).reshape(head_shape)
    attn_heads = causal_attention(q_heads, k_heads, v_heads)
    attn_out = project(attn_heads.reshape(n_seqs * seq_len, d_model), w_o)
    resid_h = (x_rows.astype(jnp.float32) + attn_out.astype(jnp.float32)).astype(jnp.bfloat16)
    normed_mlp = layer_norm(resid_h)
    gate_val = project(normed_mlp, w_gate)
    up_val = project(normed_mlp, w_up)
    act_val = (jax.nn.silu(gate_val.astype(jnp.float32)) * up_val.astype(jnp.float32)).astype(jnp.bfloat16)
    mlp_out = project(act_val, w_down)
    y_out = (resid_h.astype(jnp.float32) + mlp_out.astype(jnp.float32)).astype(jnp.bfloat16)
    return y_out.reshape(n_seqs, seq_len, d_model)
```

```python
import jax
import jax.numpy as jnp
from jax import lax
from jax.sharding import PartitionSpec as P

HEAD_DIM = 128
EPS = 1e-5
THETA = 10000.0


def rotary(heads_bf):
    seq_len = heads_bf.shape[1]
    half_dim = HEAD_DIM // 2
    inv_freq = THETA ** (-2.0 * jnp.arange(half_dim, dtype=jnp.float32) / HEAD_DIM)
    angles = jnp.arange(seq_len, dtype=jnp.float32)[:, None] * inv_freq[None, :]
    cos_t = jnp.cos(angles)[:, None, :]
    sin_t = jnp.sin(angles)[:, None, :]
    values = heads_bf.astype(jnp.float32)
    lower_half = values[..., :half_dim]
    upper_half = values[..., half_dim:]
    return jnp.concatenate([lower_half * cos_t - upper_half * sin_t, upper_half * cos_t + lower_half * sin_t], axis=-1).astype(jnp.bfloat16)


def causal_attention(q_heads, k_heads, v_heads):
    seq_len = q_heads.shape[1]
    pos = jnp.arange(seq_len)
    scores = jnp.einsum("nqhd,nkhd->nhqk", q_heads, k_heads, preferred_element_type=jnp.float32) * HEAD_DIM ** -0.5
    scores = jnp.where(pos[:, None] >= pos[None, :], scores, -1e30)
    prob = jax.nn.softmax(scores, axis=-1).astype(jnp.bfloat16)
    return jnp.einsum("nhqk,nkhd->nqhd", prob, v_heads, preferred_element_type=jnp.float32).astype(jnp.bfloat16)


def norm_full(values_bf):
    values = values_bf.astype(jnp.float32)
    mean_val = jnp.mean(values, axis=-1, keepdims=True)
    var_val = jnp.mean(values * values, axis=-1, keepdims=True) - mean_val * mean_val
    return ((values - mean_val) * lax.rsqrt(var_val + EPS)).astype(jnp.bfloat16)


def project(rows_bf, weight):
    return jnp.einsum("...c,ch->...h", rows_bf, weight, preferred_element_type=jnp.float32).astype(jnp.bfloat16)


def solution(mesh):
    act_spec = P(("dp", "ty"), None, "tx")
    col_spec = P("tx", "ty")
    row_spec = P("ty", "tx")

    def layer_fn(x_blk, w_q, w_k, w_v, w_o, w_gate, w_up, w_down):
        wq, wk, wv, wg, wu = (lax.all_gather(w, "tx", axis=0, tiled=True) for w in (w_q, w_k, w_v, w_gate, w_up))
        wo, wd = (lax.all_gather(w, "tx", axis=1, tiled=True) for w in (w_o, w_down))
        x_tok = lax.all_to_all(x_blk, "tx", split_axis=1, concat_axis=2, tiled=True)
        normed_all = lax.all_gather(norm_full(x_tok), "ty", axis=0, tiled=True)
        qkv = jnp.concatenate([project(normed_all, w) for w in (wq, wk, wv)], axis=-1)
        qkv = lax.all_to_all(qkv, "tx", split_axis=0, concat_axis=1, tiled=True)
        n_seqs, seq_len, three = qkv.shape
        q_h, k_h, v_h = (t.reshape(n_seqs, seq_len, -1, HEAD_DIM) for t in jnp.split(qkv, 3, axis=-1))
        heads = causal_attention(rotary(q_h), rotary(k_h), v_h).reshape(n_seqs, seq_len, three // 3)
        heads = lax.all_to_all(heads, "tx", split_axis=1, concat_axis=0, tiled=True)
        attn_out = lax.psum_scatter(project(heads, wo), "ty", scatter_dimension=0, tiled=True)
        resid_h = (x_tok.astype(jnp.float32) + attn_out.astype(jnp.float32)).astype(jnp.bfloat16)
        normed_mlp = lax.all_gather(norm_full(resid_h), "ty", axis=0, tiled=True)
        gate, up = project(normed_mlp, wg), project(normed_mlp, wu)
        act = (jax.nn.silu(gate.astype(jnp.float32)) * up.astype(jnp.float32)).astype(jnp.bfloat16)
        mlp_out = lax.psum_scatter(project(act, wd), "ty", scatter_dimension=0, tiled=True)
        y_tok = (resid_h.astype(jnp.float32) + mlp_out.astype(jnp.float32)).astype(jnp.bfloat16)
        return lax.all_to_all(y_tok, "tx", split_axis=2, concat_axis=1, tiled=True)

    return jax.shard_map(layer_fn, mesh=mesh, in_specs=(act_spec, col_spec, col_spec, col_spec, row_spec, col_spec, col_spec, row_spec), out_specs=act_spec, check_vma=False)
```

```python
import functools

import numpy as np
import jax
import jax.numpy as jnp
from jax import lax
from jax.experimental import pallas as pl
from jax.experimental.pallas import tpu as pltpu
from jax.sharding import PartitionSpec as P

HEAD_DIM = 128
EPS = 1e-5
THETA = 10000.0
RING = 4
MESH = pl.DeviceIdType.MESH
BF16 = jnp.bfloat16
F32 = jnp.float32
AWAY = (0, -1, 1, 2)
NEAR_LAST = (2, -1, 1, 0)


def wrap(v, n):
    return lax.rem(v + 2 * n, n)


class Torus:
    def __init__(self):
        t = lax.axis_index("ty")
        self.me = t
        self.pos = (lax.div(t, RING), lax.rem(t, RING))

    def slot(self, first, a_off, b_off):
        a = wrap(self.pos[first] + a_off, RING)
        b = wrap(self.pos[1 - first] + b_off, RING)
        return a * RING + b if first == 0 else b * RING + a


def entry_barrier(tor, tx_count):
    sem = pltpu.get_barrier_semaphore()
    for first in (0, 1):
        for d in (1, -1):
            pl.semaphore_signal(sem, inc=1, device_id={"ty": tor.slot(first, d, 0)}, device_id_type=MESH)
    me = lax.axis_index("tx")
    for k in range(1, tx_count):
        pl.semaphore_signal(sem, inc=1, device_id={"tx": lax.rem(me + k, tx_count)}, device_id_type=MESH)
    pl.semaphore_wait(sem, 4 + tx_count - 1)


def remote(src, dst, ssem, rsem, device):
    return pltpu.make_async_remote_copy(src_ref=src, dst_ref=dst, send_sem=ssem, recv_sem=rsem, device_id=device, device_id_type=MESH)


class Gather:
    SEMS = 40

    def __init__(self, tor, buf, ssem, rsem):
        self.tor, self.buf, self.ssem, self.rsem = tor, buf, ssem, rsem
        self.q = buf.shape[1] // 4

    def first(self, c):
        return 1 if c == 0 else 0

    def rows(self, c, d, half):
        if not half:
            return pl.ds(c * 2 * self.q, 2 * self.q)
        return pl.ds(c * 2 * self.q + (0 if d == 1 else self.q), self.q)

    def sem(self, c, ph, off, d, half):
        base = c * 20 + (0 if ph == 1 else 4 + 4 * AWAY.index(off))
        return base + (0 if d == 1 else 2) + (1 if half else 0)

    def copy(self, c, ph, off, d, half, hops):
        first = self.first(c)
        back = -d * hops
        s = self.tor.slot(first, back, 0) if ph == 1 else self.tor.slot(first, off, back)
        to = self.tor.slot(first, d, 0) if ph == 1 else self.tor.slot(first, 0, d)
        view = self.buf.at[s, self.rows(c, d, half)]
        i = self.sem(c, ph, off, d, half)
        return remote(view, view, self.ssem.at[i], self.rsem.at[i], {"ty": to})

    def send(self, c, ph, off, d, half=False):
        self.copy(c, ph, off, d, half, 1 if half else 0).start()

    def recv(self, c, ph, off, d, half=False):
        self.copy(c, ph, off, d, half, 2 if half else 1).wait_recv()

    def start(self):
        for ph in (1, 2):
            for c in (0, 1):
                for d in (1, -1):
                    self.send(c, ph, 0, d)

    def near(self):
        for d in (1, -1):
            for c in (0, 1):
                self.recv(c, 1, 0, d)
                self.send(c, 1, 0, d, True)
                self.send(c, 2, -d, 1)
                self.send(c, 2, -d, -1)

    def relay(self, off):
        for d in (1, -1):
            for c in (0, 1):
                self.recv(c, 2, off, d)
                self.send(c, 2, off, d, True)

    def far(self):
        for c in (0, 1):
            for d in (1, -1):
                self.recv(c, 1, 0, d, True)
            for d in (1, -1):
                self.send(c, 2, 2, d)

    def halves(self, off):
        for c in (0, 1):
            for d in (1, -1):
                self.recv(c, 2, off, d, True)

    def drain(self):
        for c in (0, 1):
            for d in (1, -1):
                for half in (False, True):
                    self.copy(c, 1, 0, d, half, 1 if half else 0).wait_send()
                    for off in AWAY:
                        self.copy(c, 2, off, d, half, 1 if half else 0).wait_send()


def add_rows(dst, srcs, width=512):
    d = dst.shape[-1]
    width = min(width, d)

    @pl.loop(0, d // width)
    def _(i):
        cols = pl.ds(pl.multiple_of(i * width, width), width)
        tot = srcs[0][:, cols].astype(F32)
        for s in srcs[1:]:
            tot += s[:, cols].astype(F32)
        dst[:, cols] = tot.astype(dst.dtype)


class Scatter:
    SEMS = 60

    @staticmethod
    def buffers(tok, d):
        q = tok // 4
        return [
            pltpu.VMEM((2, 4, 2, q, d), BF16),
            pltpu.VMEM((2, 4, 2, 2 * q, d), BF16),
            pltpu.VMEM((2, 3, 2 * q, d), BF16),
            pltpu.VMEM((2, 2, q, d), BF16),
            pltpu.VMEM((2, 2, 2 * q, d), BF16),
            pltpu.SemaphoreType.DMA((Scatter.SEMS,)),
            pltpu.SemaphoreType.DMA((Scatter.SEMS,)),
        ]

    def __init__(self, tor, part, bufs):
        self.tor, self.part = tor, part
        self.h1, self.f1, self.mid, self.h2, self.f2, self.ssem, self.rsem = bufs
        self.q = part.shape[1] // 4

    def copy(self, c, ph, bi, d, kind):
        q, first = self.q, c
        di = 0 if d == 1 else 1
        h = di if kind in (0, 2) else 1 - di
        step = 2 * d if kind == 0 else d
        if ph == 1:
            i = c * 30 + bi * 6 + di * 3 + kind
            src = self.part.at[self.tor.slot(first, step, NEAR_LAST[bi]), pl.ds(c * 2 * q + h * q, q)]
            dst = self.h1.at[c, bi, di] if kind == 0 else self.f1.at[c, bi, di, pl.ds(h * q, q)]
            to = self.tor.slot(first, d, 0)
        else:
            i = c * 30 + 24 + di * 3 + kind
            src = self.mid.at[c, 0 if kind == 0 else NEAR_LAST.index(d), pl.ds(h * q, q)]
            dst = self.h2.at[c, di] if kind == 0 else self.f2.at[c, di, pl.ds(h * q, q)]
            to = self.tor.slot(first, 0, d)
        return remote(src, dst, self.ssem.at[i], self.rsem.at[i], {"ty": to})

    def issue(self, bi):
        for kind in (0, 1):
            for c in (0, 1):
                for d in (1, -1):
                    self.copy(c, 1, bi, d, kind).start()

    def augment(self, bi):
        q = self.q
        for c in (0, 1):
            for d in (1, -1):
                di = 0 if d == 1 else 1
                self.copy(c, 1, bi, d, 0).wait_recv()
                mine = self.part.at[self.tor.slot(c, d, NEAR_LAST[bi]), pl.ds(c * 2 * q + di * q, q)]
                add_rows(mine, [mine, self.h1.at[c, bi, di]])
                self.copy(c, 1, bi, d, 2).start()

    def arrived(self, bi):
        q = self.q
        for c in (0, 1):
            for d in (1, -1):
                for kind in (1, 2):
                    self.copy(c, 1, bi, d, kind).wait_recv()
            if bi == 3:
                continue
            own = self.part.at[self.tor.slot(c, 0, NEAR_LAST[bi]), pl.ds(c * 2 * q, 2 * q)]
            add_rows(self.mid.at[c, bi], [own, self.f1.at[c, bi, 0], self.f1.at[c, bi, 1]])
            if bi == 0:
                for d in (1, -1):
                    self.copy(c, 2, 0, d, 0).start()
            else:
                self.copy(c, 2, 0, NEAR_LAST[bi], 1).start()

    def augment2(self):
        q = self.q
        for c in (0, 1):
            for d in (1, -1):
                di = 0 if d == 1 else 1
                self.copy(c, 2, 0, d, 0).wait_recv()
                mine = self.mid.at[c, NEAR_LAST.index(d), pl.ds(di * q, q)]
                add_rows(mine, [mine, self.h2.at[c, di]])
                self.copy(c, 2, 0, d, 2).start()

    def run(self):
        self.issue(0)
        self.issue(1)
        self.augment(0)
        self.issue(2)
        self.augment(1)
        self.issue(3)
        self.arrived(0)
        self.augment(2)
        self.arrived(1)
        self.augment(3)
        self.arrived(2)
        self.augment2()
        self.arrived(3)
        for c in (0, 1):
            for d in (1, -1):
                for kind in (1, 2):
                    self.copy(c, 2, 0, d, kind).wait_recv()

    def finish(self, resid, out):
        q, d = self.q, out.shape[-1]
        width = min(512, d)
        for c in (0, 1):
            rows = pl.ds(c * 2 * q, 2 * q)

            @pl.loop(0, d // width)
            def _(i):
                cols = pl.ds(pl.multiple_of(i * width, width), width)
                tot = self.part[self.tor.me, rows, cols].astype(F32)
                for di in (0, 1):
                    tot += self.f1[c, 3, di, :, cols].astype(F32)
                for di in (0, 1):
                    tot += self.f2[c, di, :, cols].astype(F32)
                tot = tot.astype(BF16).astype(F32)
                out[rows, cols] = (resid[rows, cols].astype(F32) + tot).astype(BF16)

    def drain(self):
        for c in (0, 1):
            for d in (1, -1):
                for kind in (0, 1, 2):
                    self.copy(c, 2, 0, d, kind).wait_send()
                    for bi in range(4):
                        self.copy(c, 1, bi, d, kind).wait_send()


class Exchange:
    def __init__(self, tx_count, src, dst, ssem, rsem):
        self.n, self.src, self.dst, self.ssem, self.rsem = tx_count, src, dst, ssem, rsem
        self.me = lax.axis_index("tx")

    def copy(self, k, sending):
        p = lax.rem(self.me + k, self.n) if sending else self.me
        owner = self.me if sending else lax.rem(self.me + self.n - k, self.n)
        return remote(self.src(p), self.dst(owner), self.ssem.at[k], self.rsem.at[k], {"tx": p})

    def start(self):
        for k in range(1, self.n):
            self.copy(k, True).start()
        self.local().start()

    def local(self):
        return pltpu.make_async_copy(self.src(self.me), self.dst(self.me), self.rsem.at[0])

    def wait(self):
        self.local().wait()
        for k in range(1, self.n):
            self.copy(k, False).wait_recv()

    def drain(self):
        for k in range(1, self.n):
            self.copy(k, True).wait_send()


def norm_rows(src, dst):
    tok, d = src.shape
    step = 16

    @pl.loop(0, tok // step)
    def _(i):
        rows = pl.ds(pl.multiple_of(i * step, step), step)
        v = src[rows, :].astype(F32)
        mean = jnp.sum(v, axis=-1, keepdims=True) * (1.0 / d)
        var = jnp.sum(v * v, axis=-1, keepdims=True) * (1.0 / d) - mean * mean
        dst[rows, :] = ((v - mean) * lax.rsqrt(var + EPS)).astype(BF16)


def gather_kernel(tx_count, x_ref, tok_ref, all_ref, xt, buf, xs, xr, gs, gr, out_sem):
    tok, d = xt.shape
    dx = x_ref.shape[1]
    tor = Torus()
    entry_barrier(tor, tx_count)
    ex = Exchange(
        tx_count,
        lambda p: x_ref.at[pl.ds(pl.multiple_of(p * tok, tok), tok)],
        lambda o: xt.at[:, pl.ds(pl.multiple_of(o * dx, dx), dx)],
        xs,
        xr,
    )
    ex.start()
    ex.wait()
    norm_rows(xt, buf.at[tor.me])
    g = Gather(tor, buf, gs, gr)
    g.start()
    tok_ref[...] = xt[...]
    g.near()
    g.relay(0)
    g.far()
    g.relay(-1)
    g.relay(1)
    g.halves(0)
    g.relay(2)
    g.halves(-1)
    g.halves(1)
    g.halves(2)
    out = pltpu.make_async_copy(buf, all_ref, out_sem)
    out.start()
    ex.drain()
    g.drain()
    out.wait()


def attention_kernel(tx_count, hc, all_ref, w_ref, tok_ref, cos_ref, sin_ref, h_ref, xp, w, acc, qs, qr, kv, hs, hr, load_sem, es, er, os_, or_, *rs_bufs):
    n_dev, tok, d = xp.shape
    dx = w.shape[1]
    seq = tok * tx_count
    spd = n_dev // tx_count
    heads = hc // HEAD_DIM
    tor = Torus()
    w_load = pltpu.make_async_copy(w_ref, w, load_sem.at[4])
    w_load.start()
    x_loads = [pltpu.make_async_copy(all_ref.at[pl.ds(4 * m, 4)], xp.at[pl.ds(4 * m, 4)], load_sem.at[m]) for m in range(4)]
    for cp in x_loads:
        cp.start()
    entry_barrier(tor, tx_count)
    w_load.wait()
    for cp in x_loads:
        cp.wait()
    rows = 4 * tok

    @pl.loop(0, n_dev // 4)
    def _(m):
        slots = pl.ds(m * 4, 4)

        @pl.loop(0, tx_count)
        def _(x):
            lhs = xp[slots, :, pl.ds(pl.multiple_of(x * dx, dx), dx)].reshape(rows, dx)
            part = jnp.dot(lhs, w[x, :, pl.ds(0, 3 * hc)], preferred_element_type=F32)

            @pl.when(x == 0)
            def _():
                acc[...] = part

            @pl.when(x > 0)
            def _():
                acc[...] += part

        qs[slots] = acc[...].astype(BF16).reshape(4, tok, 3 * hc)

    ex = Exchange(
        tx_count,
        lambda p: qs.at[pl.ds(p * spd, spd)],
        lambda o: qr.at[o],
        es,
        er,
    )
    ex.start()
    ex.wait()
    block = min(seq, 128)

    @pl.loop(0, spd)
    def _(s):
        for hd in range(heads):
            def part(which):
                return qr[:, s, :, pl.ds(which * hc + hd * HEAD_DIM, HEAD_DIM)].reshape(seq, HEAD_DIM)

            for which in (0, 1):
                v = part(which).astype(F32)
                rot = v * cos_ref[...] + pltpu.roll(v, HEAD_DIM // 2, 1) * sin_ref[...]
                kv[which] = rot.astype(BF16)
            kv[2] = part(2)
            for b in range(seq // block):
                keys = (b + 1) * block
                sc = lax.dot_general(kv[0, pl.ds(b * block, block)], kv[1, pl.ds(0, keys)], (((1,), (1,)), ((), ())), preferred_element_type=F32)
                sc = sc * HEAD_DIM ** -0.5
                q_pos = b * block + lax.broadcasted_iota(jnp.int32, (block, keys), 0)
                k_pos = lax.broadcasted_iota(jnp.int32, (block, keys), 1)
                sc = jnp.where(q_pos >= k_pos, sc, -1e30)
                e = jnp.exp(sc - jnp.max(sc, axis=-1, keepdims=True))
                prob = (e / jnp.sum(e, axis=-1, keepdims=True)).astype(BF16)
                o = jnp.dot(prob, kv[2, pl.ds(0, keys)], preferred_element_type=F32).astype(BF16)
                n_p = block // tok
                hs[pl.ds(b * n_p, n_p), s, :, pl.ds(hd * HEAD_DIM, HEAD_DIM)] = o.reshape(n_p, tok, HEAD_DIM)

    oe = Exchange(
        tx_count,
        lambda p: hs.at[p],
        lambda o: hr.at[pl.ds(o * spd, spd)],
        os_,
        or_,
    )
    oe.start()
    oe.wait()

    @pl.loop(0, n_dev // 4)
    def _(m):
        slots = pl.ds(m * 4, 4)
        lhs = hr[slots].reshape(rows, hc)

        @pl.loop(0, tx_count)
        def _(x):
            for j in range(dx // hc):
                o = jnp.dot(lhs, w[x, pl.ds(j * hc, hc), pl.ds(3 * hc, hc)], preferred_element_type=F32)
                cols = pl.ds(pl.multiple_of(x * dx + j * hc, hc), hc)
                xp[slots, :, cols] = o.astype(BF16).reshape(4, tok, hc)

    sc = Scatter(tor, xp, rs_bufs)
    sc.run()
    sc.finish(tok_ref, h_ref)
    sc.drain()
    ex.drain()
    oe.drain()


def mlp_kernel(tx_count, h_ref, w_ref, y_ref, buf, wg, wu, wd, part, act, acc_g, acc_u, yt, yr, load_sem, gs, gr, ys, yrs, *rs_bufs):
    n_dev, tok, d = buf.shape
    fp, dx = wg.shape[1:]
    f = w_ref.shape[2]
    tor = Torus()
    loads = [pltpu.make_async_copy(w_ref.at[:, i], dst.at[:, pl.ds(0, f)], load_sem.at[i]) for i, dst in enumerate((wg, wu, wd))]
    for cp in loads:
        cp.start()
    norm_rows(h_ref, buf.at[tor.me])
    entry_barrier(tor, tx_count)
    g = Gather(tor, buf, gs, gr)
    g.start()
    if fp > f:
        for dst in (wg, wu, wd):
            dst[:, pl.ds(f, fp - f), :] = jnp.zeros((tx_count, fp - f, dx), BF16)
    g.near()
    g.relay(0)
    g.far()
    g.relay(-1)
    g.relay(1)
    g.halves(0)
    g.relay(2)
    g.halves(-1)
    g.halves(1)
    g.halves(2)
    for cp in loads:
        cp.wait()
    rows = 4 * tok

    @pl.loop(0, n_dev // 4)
    def _(m):
        slots = pl.ds(m * 4, 4)

        @pl.loop(0, tx_count)
        def _(x):
            lhs = buf[slots, :, pl.ds(pl.multiple_of(x * dx, dx), dx)].reshape(rows, dx)
            for acc, wt in ((acc_g, wg), (acc_u, wu)):
                val = lax.dot_general(lhs, wt[x], (((1,), (1,)), ((), ())), preferred_element_type=F32)

                @pl.when(x == 0)
                def _():
                    acc[...] = val

                @pl.when(x > 0)
                def _():
                    acc[...] += val

        gate = acc_g[...].astype(BF16).astype(F32)
        up = acc_u[...].astype(BF16).astype(F32)
        act[...] = (gate * jax.nn.sigmoid(gate) * up).astype(BF16)

        @pl.loop(0, tx_count)
        def _(x):
            o = jnp.dot(act[...], wd[x], preferred_element_type=F32)
            part[slots, :, pl.ds(pl.multiple_of(x * dx, dx), dx)] = o.astype(BF16).reshape(4, tok, dx)

    sc = Scatter(tor, part, rs_bufs)
    sc.run()
    sc.finish(h_ref, yt)
    ye = Exchange(
        tx_count,
        lambda p: yt.at[:, pl.ds(pl.multiple_of(p * dx, dx), dx)],
        lambda o: yr.at[pl.ds(pl.multiple_of(o * tok, tok), tok)],
        ys,
        yrs,
    )
    ye.start()
    g.drain()
    sc.drain()
    ye.wait()
    y_ref[...] = yr[...]
    ye.drain()


VMEM_SPEC = pl.BlockSpec(memory_space=pltpu.VMEM)
ANY_SPEC = pl.BlockSpec(memory_space=pl.ANY)


def rotary_tables(seq_len):
    half = HEAD_DIM // 2
    inv_freq = THETA ** (-2.0 * jnp.arange(half, dtype=F32) / HEAD_DIM)
    angles = jnp.arange(seq_len, dtype=F32)[:, None] * inv_freq[None, :]
    cos_t, sin_t = jnp.cos(angles), jnp.sin(angles)
    return jnp.concatenate([cos_t, cos_t], -1), jnp.concatenate([-sin_t, sin_t], -1)


def call(kernel, name, ident, out_shape, in_specs, out_specs, scratch, flops, nbytes):
    return pl.pallas_call(
        kernel,
        name=name,
        out_shape=out_shape,
        in_specs=in_specs,
        out_specs=out_specs,
        scratch_shapes=scratch,
        cost_estimate=pl.CostEstimate(flops=flops, bytes_accessed=nbytes, transcendentals=0),
        compiler_params=pltpu.CompilerParams(collective_id=ident, has_side_effects=True, vmem_limit_bytes=62 * 2**20),
    )


def solution(mesh):
    tx_count, n_dev = mesh.shape["tx"], mesh.shape["ty"]
    act_spec = P(("dp", "ty"), None, "tx")
    col_spec = P("tx", "ty")
    row_spec = P("ty", "tx")
    dma = pltpu.SemaphoreType.DMA

    def layer_fn(x_blk, w_q, w_k, w_v, w_o, w_gate, w_up, w_down):
        seq, dx = x_blk.shape[1:]
        hc, f = w_q.shape[1], w_gate.shape[1]
        tok, d = seq // tx_count, dx * tx_count
        spd = n_dev // tx_count
        fp = -(-f // 128) * 128
        shape = jax.ShapeDtypeStruct
        w_o_rows = w_o.reshape(hc, dx // hc, hc).transpose(1, 0, 2).reshape(dx, hc)
        attn_w = lax.all_gather(jnp.concatenate([w_q, w_k, w_v, w_o_rows], axis=1), "tx", axis=0, tiled=True).reshape(tx_count, dx, 4 * hc)
        mlp_w = lax.all_gather(jnp.concatenate([w_gate.T, w_up.T, w_down], axis=0), "tx", axis=0, tiled=True).reshape(tx_count, 3, f, dx)
        cos_t, sin_t = rotary_tables(seq)

        x_tok, x_all = call(
            functools.partial(gather_kernel, tx_count), "norm_gather", 1,
            (shape((tok, d), BF16), shape((n_dev, tok, d), BF16)),
            [VMEM_SPEC], (VMEM_SPEC, ANY_SPEC),
            [pltpu.VMEM((tok, d), BF16), pltpu.VMEM((n_dev, tok, d), BF16), dma((tx_count,)), dma((tx_count,)),
             dma((Gather.SEMS,)), dma((Gather.SEMS,)), dma],
            2 * n_dev * tok * d * 3 * hc, n_dev * tok * d * 4,
        )(x_blk[0])
        h = call(
            functools.partial(attention_kernel, tx_count, hc), "attention", 2,
            shape((tok, d), BF16),
            [ANY_SPEC, ANY_SPEC, VMEM_SPEC, VMEM_SPEC, VMEM_SPEC], VMEM_SPEC,
            [pltpu.VMEM((n_dev, tok, d), BF16), pltpu.VMEM((tx_count, dx, 4 * hc), BF16), pltpu.VMEM((4 * tok, 3 * hc), F32),
             pltpu.VMEM((n_dev, tok, 3 * hc), BF16), pltpu.VMEM((tx_count, spd, tok, 3 * hc), BF16), pltpu.VMEM((3, seq, HEAD_DIM), BF16),
             pltpu.VMEM((tx_count, spd, tok, hc), BF16), pltpu.VMEM((n_dev, tok, hc), BF16),
             dma((5,)), dma((tx_count,)), dma((tx_count,)), dma((tx_count,)), dma((tx_count,))] + Scatter.buffers(tok, d),
            2 * n_dev * tok * d * 4 * hc, n_dev * tok * d * 4,
        )(x_all, attn_w, x_tok, cos_t, sin_t)
        y = call(
            functools.partial(mlp_kernel, tx_count), "mlp", 3,
            shape((seq, dx), BF16),
            [VMEM_SPEC, ANY_SPEC], VMEM_SPEC,
            [pltpu.VMEM((n_dev, tok, d), BF16)] + [pltpu.VMEM((tx_count, fp, dx), BF16)] * 3
            + [pltpu.VMEM((n_dev, tok, d), BF16), pltpu.VMEM((4 * tok, fp), BF16), pltpu.VMEM((4 * tok, fp), F32), pltpu.VMEM((4 * tok, fp), F32),
               pltpu.VMEM((tok, d), BF16), pltpu.VMEM((seq, dx), BF16), dma((3,)), dma((Gather.SEMS,)), dma((Gather.SEMS,)),
               dma((tx_count,)), dma((tx_count,))] + Scatter.buffers(tok, d),
            2 * n_dev * tok * d * 3 * f, n_dev * tok * d * 4,
        )(h, mlp_w)
        return y[None]

    return jax.shard_map(layer_fn, mesh=mesh, in_specs=(act_spec, col_spec, col_spec, col_spec, row_spec, col_spec, col_spec, row_spec), out_specs=act_spec, check_vma=False)
```

```python
import functools

import numpy as np
import jax
import jax.numpy as jnp
from jax import lax
from jax.experimental import pallas as pl
from jax.experimental.pallas import tpu as pltpu
from jax.sharding import PartitionSpec as P

HEAD_DIM = 128
EPS = 1e-5
THETA = 10000.0
RING = 4
MESH = pl.DeviceIdType.MESH
BF16 = jnp.bfloat16
F32 = jnp.float32
AWAY = (0, -1, 1, 2)
ORDER = (-1, 2, 1, 0)


def wrap(v, n):
    return lax.rem(v + 2 * n, n)


class Torus:
    def __init__(self):
        t = lax.axis_index("ty")
        self.me = t
        self.pos = (lax.div(t, RING), lax.rem(t, RING))

    def slot(self, first, a_off, b_off):
        a = wrap(self.pos[first] + a_off, RING)
        b = wrap(self.pos[1 - first] + b_off, RING)
        return a * RING + b if first == 0 else b * RING + a


def entry_barrier(tor, tx_count):
    sem = pltpu.get_barrier_semaphore()
    for first in (0, 1):
        for d in (1, -1):
            pl.semaphore_signal(sem, inc=1, device_id={"ty": tor.slot(first, d, 0)}, device_id_type=MESH)
    me = lax.axis_index("tx")
    for k in range(1, tx_count):
        pl.semaphore_signal(sem, inc=1, device_id={"tx": lax.rem(me + k, tx_count)}, device_id_type=MESH)
    pl.semaphore_wait(sem, 4 + tx_count - 1)


def remote(src, dst, ssem, rsem, device):
    return pltpu.make_async_remote_copy(src_ref=src, dst_ref=dst, send_sem=ssem, recv_sem=rsem, device_id=device, device_id_type=MESH)


class Gather:
    SEMS = 40

    def __init__(self, tor, buf, ssem, rsem):
        self.tor, self.buf, self.ssem, self.rsem = tor, buf, ssem, rsem
        self.q = buf.shape[1] // 4

    def first(self, c):
        return 1 if c == 0 else 0

    def rows(self, c, d, half):
        if not half:
            return pl.ds(c * 2 * self.q, 2 * self.q)
        return pl.ds(c * 2 * self.q + (0 if d == 1 else self.q), self.q)

    def sem(self, c, ph, off, d, half):
        base = c * 20 + (0 if ph == 1 else 4 + 4 * AWAY.index(off))
        return base + (0 if d == 1 else 2) + (1 if half else 0)

    def copy(self, c, ph, off, d, half, hops):
        first = self.first(c)
        back = -d * hops
        s = self.tor.slot(first, back, 0) if ph == 1 else self.tor.slot(first, off, back)
        to = self.tor.slot(first, d, 0) if ph == 1 else self.tor.slot(first, 0, d)
        view = self.buf.at[s, self.rows(c, d, half)]
        i = self.sem(c, ph, off, d, half)
        return remote(view, view, self.ssem.at[i], self.rsem.at[i], {"ty": to})

    def send(self, c, ph, off, d, half=False):
        self.copy(c, ph, off, d, half, 1 if half else 0).start()

    def recv(self, c, ph, off, d, half=False):
        self.copy(c, ph, off, d, half, 2 if half else 1).wait_recv()

    def start(self):
        for ph in (1, 2):
            for c in (0, 1):
                for d in (1, -1):
                    self.send(c, ph, 0, d)

    def near(self):
        for d in (1, -1):
            for c in (0, 1):
                self.recv(c, 1, 0, d)
                self.send(c, 1, 0, d, True)
                self.send(c, 2, -d, 1)
                self.send(c, 2, -d, -1)

    def relay(self, off):
        for d in (1, -1):
            for c in (0, 1):
                self.recv(c, 2, off, d)
                self.send(c, 2, off, d, True)

    def far(self):
        for c in (0, 1):
            for d in (1, -1):
                self.recv(c, 1, 0, d, True)
            for d in (1, -1):
                self.send(c, 2, 2, d)

    def halves(self, off):
        for c in (0, 1):
            for d in (1, -1):
                self.recv(c, 2, off, d, True)

    def drain(self):
        for c in (0, 1):
            for d in (1, -1):
                for half in (False, True):
                    self.copy(c, 1, 0, d, half, 1 if half else 0).wait_send()
                    for off in AWAY:
                        self.copy(c, 2, off, d, half, 1 if half else 0).wait_send()


def add_rows(dst, srcs, width=512):
    d = dst.shape[-1]
    width = min(width, d)

    @pl.loop(0, d // width)
    def _(i):
        cols = pl.ds(pl.multiple_of(i * width, width), width)
        tot = srcs[0][:, cols].astype(F32)
        for s in srcs[1:]:
            tot += s[:, cols].astype(F32)
        dst[:, cols] = tot.astype(dst.dtype)


class Scatter:
    SEMS = 60

    @staticmethod
    def buffers(tok, d):
        q = tok // 4
        return [
            pltpu.VMEM((2, 4, 2, q, d), BF16),
            pltpu.VMEM((2, 4, 2, 2 * q, d), BF16),
            pltpu.VMEM((2, 3, 2 * q, d), BF16),
            pltpu.VMEM((2, 2, q, d), BF16),
            pltpu.VMEM((2, 2, 2 * q, d), BF16),
            pltpu.SemaphoreType.DMA((Scatter.SEMS,)),
            pltpu.SemaphoreType.DMA((Scatter.SEMS,)),
        ]

    def __init__(self, tor, part, bufs):
        self.tor, self.part = tor, part
        self.h1, self.f1, self.mid, self.h2, self.f2, self.ssem, self.rsem = bufs
        self.q = part.shape[1] // 4

    def copy(self, c, ph, bi, d, kind):
        q, first = self.q, c
        di = 0 if d == 1 else 1
        h = di if kind in (0, 2) else 1 - di
        step = 2 * d if kind == 0 else d
        if ph == 1:
            i = c * 30 + bi * 6 + di * 3 + kind
            src = self.part.at[self.tor.slot(first, step, ORDER[bi]), pl.ds(c * 2 * q + h * q, q)]
            dst = self.h1.at[c, bi, di] if kind == 0 else self.f1.at[c, bi, di, pl.ds(h * q, q)]
            to = self.tor.slot(first, d, 0)
        else:
            i = c * 30 + 24 + di * 3 + kind
            src = self.mid.at[c, ORDER.index(2 if kind == 0 else d), pl.ds(h * q, q)]
            dst = self.h2.at[c, di] if kind == 0 else self.f2.at[c, di, pl.ds(h * q, q)]
            to = self.tor.slot(first, 0, d)
        return remote(src, dst, self.ssem.at[i], self.rsem.at[i], {"ty": to})

    def issue(self, bi):
        for kind in (0, 1):
            for c in (0, 1):
                for d in (1, -1):
                    self.copy(c, 1, bi, d, kind).start()

    def augment(self, bi):
        q = self.q
        for c in (0, 1):
            for d in (1, -1):
                di = 0 if d == 1 else 1
                self.copy(c, 1, bi, d, 0).wait_recv()
                mine = self.part.at[self.tor.slot(c, d, ORDER[bi]), pl.ds(c * 2 * q + di * q, q)]
                add_rows(mine, [mine, self.h1.at[c, bi, di]])
                self.copy(c, 1, bi, d, 2).start()

    def arrived(self, bi):
        q = self.q
        for c in (0, 1):
            for d in (1, -1):
                for kind in (1, 2):
                    self.copy(c, 1, bi, d, kind).wait_recv()
            if bi == 3:
                continue
            own = self.part.at[self.tor.slot(c, 0, ORDER[bi]), pl.ds(c * 2 * q, 2 * q)]
            add_rows(self.mid.at[c, bi], [own, self.f1.at[c, bi, 0], self.f1.at[c, bi, 1]])
            if ORDER[bi] == 2:
                for d in (1, -1):
                    self.copy(c, 2, 0, d, 0).start()
            else:
                self.copy(c, 2, 0, ORDER[bi], 1).start()

    def augment2(self):
        q = self.q
        for c in (0, 1):
            for d in (1, -1):
                di = 0 if d == 1 else 1
                self.copy(c, 2, 0, d, 0).wait_recv()
                mine = self.mid.at[c, ORDER.index(d), pl.ds(di * q, q)]
                add_rows(mine, [mine, self.h2.at[c, di]])
                self.copy(c, 2, 0, d, 2).start()

    def run(self, compute, after):
        for bi in (0, 1):
            compute(bi)
            self.issue(bi)
        self.augment(0)
        compute(2)
        self.issue(2)
        self.augment(1)
        compute(3)
        self.issue(3)
        self.arrived(0)
        after(0)
        self.augment(2)
        self.arrived(1)
        after(1)
        self.augment(3)
        self.arrived(2)
        after(2)
        self.augment2()
        self.arrived(3)
        for c in (0, 1):
            for d in (1, -1):
                for kind in (1, 2):
                    self.copy(c, 2, 0, d, kind).wait_recv()
        after(3)

    def finish(self, resid, out):
        q, d = self.q, out.shape[-1]
        width = min(512, d)
        for c in (0, 1):
            rows = pl.ds(c * 2 * q, 2 * q)

            @pl.loop(0, d // width)
            def _(i):
                cols = pl.ds(pl.multiple_of(i * width, width), width)
                tot = self.part[self.tor.me, rows, cols].astype(F32)
                for di in (0, 1):
                    tot += self.f1[c, 3, di, :, cols].astype(F32)
                for di in (0, 1):
                    tot += self.f2[c, di, :, cols].astype(F32)
                tot = tot.astype(BF16).astype(F32)
                out[rows, cols] = (resid[rows, cols].astype(F32) + tot).astype(BF16)

    def drain(self):
        for c in (0, 1):
            for d in (1, -1):
                for kind in (0, 1, 2):
                    self.copy(c, 2, 0, d, kind).wait_send()
                    for bi in range(4):
                        self.copy(c, 1, bi, d, kind).wait_send()


class Exchange:
    def __init__(self, tx_count, src, dst, ssem, rsem):
        self.n, self.src, self.dst, self.ssem, self.rsem = tx_count, src, dst, ssem, rsem
        self.me = lax.axis_index("tx")

    def copy(self, k, sending):
        p = lax.rem(self.me + k, self.n) if sending else self.me
        owner = self.me if sending else lax.rem(self.me + self.n - k, self.n)
        return remote(self.src(p), self.dst(owner), self.ssem.at[k], self.rsem.at[k], {"tx": p})

    def start(self):
        for k in range(1, self.n):
            self.copy(k, True).start()
        self.local().start()

    def local(self):
        return pltpu.make_async_copy(self.src(self.me), self.dst(self.me), self.rsem.at[0])

    def wait(self):
        self.local().wait()
        for k in range(1, self.n):
            self.copy(k, False).wait_recv()

    def drain(self):
        for k in range(1, self.n):
            self.copy(k, True).wait_send()


def norm_rows(src, dst):
    tok, d = src.shape
    step = 16

    @pl.loop(0, tok // step)
    def _(i):
        rows = pl.ds(pl.multiple_of(i * step, step), step)
        v = src[rows, :].astype(F32)
        mean = jnp.sum(v, axis=-1, keepdims=True) * (1.0 / d)
        var = jnp.sum(v * v, axis=-1, keepdims=True) * (1.0 / d) - mean * mean
        dst[rows, :] = ((v - mean) * lax.rsqrt(var + EPS)).astype(BF16)


class Ring:
    SEMS = 9

    def __init__(self, tx_count, rows, src, slot, ssem, rsem, base):
        self.nx, self.rows, self.src, self.slot, self.ssem, self.rsem, self.base = tx_count // 2, rows, src, slot, ssem, rsem, base
        me = lax.axis_index("tx")
        self.me, self.x, self.core = me, lax.div(me, 2), lax.rem(me, 2)
        self.split = (rows // 2 + 15) // 16 * 16

    def tx(self, dx, other=False):
        return wrap(self.x + dx, self.nx) * 2 + (1 - self.core if other else self.core)

    def half(self, view, d):
        return view.at[pl.ds(0, self.split)] if d == 1 else view.at[pl.ds(self.split, self.rows - self.split)]

    def copy(self, i, src, dst, to):
        i += self.base
        return remote(src, dst, self.ssem.at[i], self.rsem.at[i], {"tx": to})

    def pass_on(self, d, recv=False):
        view = self.slot(self.tx(-d if recv else 0))
        return self.copy(0 if d == 1 else 1, view if recv else self.src, view, self.tx(d))

    def relay(self, d, recv=False):
        view = self.half(self.slot(self.tx(-2 * d if recv else -d)), d)
        return self.copy(2 if d == 1 else 3, view, view, self.tx(d))

    def across(self, which, recv=False):
        view = self.slot(self.tx(which, recv))
        if abs(which) == 2:
            view = self.half(view, which // 2)
        src = self.src if which == 0 and not recv else view
        return self.copy(6 + which, src, view, self.tx(0, True))

    def all_across(self):
        return (0, 1, -1, 2, -2) if self.nx > 1 else (0,)

    def own(self):
        return pltpu.make_async_copy(self.src, self.slot(self.me), self.rsem.at[self.base + 8 + 1])

    def start(self, place=True):
        if self.nx > 1:
            for d in (1, -1):
                self.pass_on(d).start()
        self.across(0).start()
        if place:
            self.own().start()

    def step(self):
        if self.nx > 1:
            for d in (1, -1):
                self.pass_on(d, True).wait_recv()
                self.relay(d).start()
                self.across(-d).start()

    def step2(self):
        if self.nx > 1:
            for d in (1, -1):
                self.relay(d, True).wait_recv()
                self.across(2 * d).start()

    def finish(self, place=True):
        for which in self.all_across():
            self.across(which, True).wait_recv()
        if place:
            self.own().wait()

    def drain(self):
        if self.nx > 1:
            for d in (1, -1):
                self.pass_on(d).wait_send()
                self.relay(d).wait_send()
        for which in self.all_across():
            self.across(which).wait_send()


RING_SEMS = 10


def layer_kernel(tx_count, x_ref, wq_ref, wk_ref, wv_ref, wo_ref, wg_ref, wu_ref, wd_ref, cos_ref, sin_ref, y_ref,
                 xp, x2, wqkv, wo, wg, wu, wd, xs, os_, act, kv, xt, h, yr,
                 load_sem, a2a_s, a2a_r, qkv_s, qkv_r, gs, gr, ws, wr, *rs_bufs):
    n_dev, tok, d = xp.shape
    dx = x_ref.shape[1]
    hc = wq_ref.shape[1]
    f, fp = wg_ref.shape[0], wg.shape[2]
    seq = tok * tx_count
    spd = n_dev // tx_count
    heads = hc // HEAD_DIM
    q2 = tok // 2
    c3 = 3 * hc
    tor = Torus()
    me_tx = lax.axis_index("tx")

    def exchange(i, src, dst):
        return Exchange(tx_count, src, dst, a2a_s.at[i], a2a_r.at[i])

    def col(start, width):
        return pl.ds(pl.multiple_of(start, width), width)

    def ring(i, src, slot):
        return Ring(tx_count, src.shape[0], src, slot, ws, wr, i * RING_SEMS)

    rings = [ring(i, src, lambda o, i=i: wqkv.at[o, :, pl.ds(i * hc, hc)]) for i, src in enumerate((wq_ref, wk_ref, wv_ref))]
    rings.append(ring(3, wo_ref, lambda o: wo.at[o]))
    r_gate = ring(4, wg.at[me_tx], lambda o: wg.at[o])
    r_up = ring(5, wu.at[me_tx], lambda o: wu.at[o])
    r_down = ring(6, wd_ref, lambda o: wd.at[o, pl.ds(0, f)])

    raw = [pltpu.make_async_copy(src, wd.at[i, pl.ds(0, f)], load_sem.at[i]) for i, src in enumerate((wg_ref, wu_ref))]
    for cp in raw:
        cp.start()
    entry_barrier(tor, tx_count)
    xe = exchange(
        0,
        lambda p: x_ref.at[pl.ds(pl.multiple_of(p * tok, tok), tok)],
        lambda o: xt.at[:, col(o * dx, dx)],
    )
    xe.start()
    if fp > f:
        wd[:, pl.ds(f, fp - f), :] = jnp.zeros((tx_count, fp - f, dx), BF16)
    xe.wait()
    norm_rows(xt, xp.at[tor.me])
    g1 = Gather(tor, xp, gs, gr)
    g1.start()
    for r in rings:
        r.start()
    for cp in raw:
        cp.wait()
    for i, dst in enumerate((wg, wu)):
        for j in range(fp // 128):
            dst[me_tx, :, pl.ds(j * 128, 128)] = wd[i, pl.ds(j * 128, 128), :].T

    def pieces(off):
        return [(c, tor.slot(1 - c, off, n), (c * 4 + n) * q2) for c in (0, 1) for n in range(RING)]

    def stage(src, off, dst, cols):
        for c, s, at in pieces(off):
            dst[pl.ds(at, q2), :] = src[s, pl.ds(c * q2, q2), cols]

    def qkv_copy(s_owner, k, sl, c, sending, src_slot):
        rows = pl.ds(c * q2, q2)
        i = k * spd * 2 + sl * 2 + c
        src = x2.at[src_slot, rows, pl.ds(0, c3)]
        dst = x2.at[sl * tx_count + s_owner, rows, pl.ds(c3, c3)]
        return src, dst, i

    def qkv_group(off):
        stage(xp, off, xs, pl.ds(0, d))

        @pl.loop(0, 3)
        def _(n):
            cols = col(n * hc, hc)
            out = jnp.dot(xs[...], wqkv[:, :, cols].reshape(d, hc), preferred_element_type=F32).astype(BF16)
            for c, s, at in pieces(off):
                x2[s, pl.ds(c * q2, q2), cols] = out[at : at + q2]

        for c, s, _ in pieces(off):
            p, sl = lax.div(s, spd), lax.rem(s, spd)
            k = lax.rem(p - me_tx + tx_count, tx_count)
            src, dst, i = qkv_copy(me_tx, k, sl, c, True, s)

            @pl.when(k == 0)
            def _():
                pltpu.make_async_copy(src, dst, qkv_r.at[i]).start()

            @pl.when(k != 0)
            def _():
                remote(src, dst, qkv_s.at[i], qkv_r.at[i], {"tx": p}).start()

    g1.near()
    rings[0].step()
    g1.relay(0)
    for r in rings[1:]:
        r.step()
    for r in rings:
        r.step2()
    g1.far()
    g1.relay(-1)
    g1.relay(1)
    g1.halves(0)
    for r in rings[:3]:
        r.finish()
    qkv_group(0)
    g1.relay(2)
    g1.halves(-1)
    qkv_group(-1)
    g1.halves(1)
    qkv_group(1)
    g1.halves(2)
    qkv_group(2)

    for k in range(tx_count):
        owner = lax.rem(me_tx + tx_count - k, tx_count)
        for sl in range(spd):
            for c in (0, 1):
                src, dst, i = qkv_copy(owner, k, sl, c, False, me_tx * spd + sl)
                if k == 0:
                    pltpu.make_async_copy(src, dst, qkv_r.at[i]).wait()
                else:
                    remote(src, dst, qkv_s.at[i], qkv_r.at[i], {"tx": me_tx}).wait_recv()
    block = min(seq, 128)

    @pl.loop(0, spd)
    def _(s):
        for hd in range(heads):
            def part(which):
                return x2[pl.ds(s * tx_count, tx_count), :, pl.ds(c3 + which * hc + hd * HEAD_DIM, HEAD_DIM)].reshape(seq, HEAD_DIM)

            for which in (0, 1):
                v = part(which).astype(F32)
                rot = v * cos_ref[...] + pltpu.roll(v, HEAD_DIM // 2, 1) * sin_ref[...]
                kv[which] = rot.astype(BF16)
            kv[2] = part(2)
            for b in range(seq // block):
                keys = (b + 1) * block
                sc = lax.dot_general(kv[0, pl.ds(b * block, block)], kv[1, pl.ds(0, keys)], (((1,), (1,)), ((), ())), preferred_element_type=F32)
                sc = sc * HEAD_DIM ** -0.5
                q_pos = b * block + lax.broadcasted_iota(jnp.int32, (block, keys), 0)
                k_pos = lax.broadcasted_iota(jnp.int32, (block, keys), 1)
                sc = jnp.where(q_pos >= k_pos, sc, -1e30)
                e = jnp.exp(sc - jnp.max(sc, axis=-1, keepdims=True))
                prob = (e / jnp.sum(e, axis=-1, keepdims=True)).astype(BF16)
                o = jnp.dot(prob, kv[2, pl.ds(0, keys)], preferred_element_type=F32).astype(BF16)
                for n in range(block // tok):
                    at = (b * (block // tok) + n) * spd + s
                    x2[at, :, pl.ds(2 * c3 + hd * HEAD_DIM, HEAD_DIM)] = o[n * tok : (n + 1) * tok]

    oe = exchange(
        1,
        lambda p: x2.at[pl.ds(p * spd, spd), :, pl.ds(2 * c3, hc)],
        lambda o: x2.at[pl.ds(o * spd, spd), :, pl.ds(2 * c3 + hc, hc)],
    )
    oe.start()
    rings[3].finish()
    g1.drain()
    for k in range(1, tx_count):
        for sl in range(spd):
            for c in (0, 1):
                src, dst, i = qkv_copy(me_tx, k, sl, c, True, me_tx * spd + sl)
                remote(src, dst, qkv_s.at[i], qkv_r.at[i], {"tx": me_tx}).wait_send()
    oe.wait()
    oe.drain()
    r_gate.start(place=False)
    r_up.start(place=False)
    r_down.start()

    def put(off, x, out):
        for c, s, at in pieces(off):
            xp[s, pl.ds(c * q2, q2), col(x * dx, dx)] = out[at : at + q2]

    def o_group(bi):
        off = ORDER[bi]
        stage(x2, off, os_, pl.ds(2 * c3 + hc, hc))

        @pl.loop(0, tx_count)
        def _(x):
            put(off, x, jnp.dot(os_[...], wo[x], preferred_element_type=F32).astype(BF16))

    def weights_1(n):
        if n == 1:
            r_gate.step()
        if n == 3:
            r_up.step()

    sc1 = Scatter(tor, xp, rs_bufs)
    sc1.run(o_group, weights_1)
    sc1.finish(xt, h)
    norm_rows(h, x2.at[tor.me])
    g2 = Gather(tor, x2, gs, gr)
    g2.start()
    sc1.drain()
    xe.drain()

    def mlp_group(off):
        stage(x2, off, xs, pl.ds(0, d))
        width = 256 if fp % 256 == 0 else 128

        @pl.loop(0, fp // width)
        def _(n):
            cols = col(n * width, width)
            gate = jnp.dot(xs[...], wg[:, :, cols].reshape(d, width), preferred_element_type=F32).astype(BF16).astype(F32)
            up = jnp.dot(xs[...], wu[:, :, cols].reshape(d, width), preferred_element_type=F32).astype(BF16).astype(F32)
            act[:, cols] = (gate * jax.nn.sigmoid(gate) * up).astype(BF16)

        @pl.loop(0, tx_count)
        def _(x):
            put(off, x, jnp.dot(act[...], wd[x], preferred_element_type=F32).astype(BF16))

    g2.near()
    r_down.step()
    g2.relay(0)
    r_gate.step2()
    g2.far()
    r_up.step2()
    g2.relay(-1)
    g2.relay(1)
    g2.halves(0)
    r_down.step2()
    r_gate.finish(place=False)
    r_up.finish(place=False)
    r_down.finish()
    mlp_group(0)
    g2.relay(2)
    g2.halves(-1)
    mlp_group(-1)
    g2.halves(1)
    mlp_group(1)
    g2.halves(2)

    def mlp_rest(bi):
        if ORDER[bi] == 2:
            mlp_group(2)

    sc2 = Scatter(tor, xp, rs_bufs)
    sc2.run(mlp_rest, lambda n: None)
    sc2.finish(h, xt)
    ye = exchange(
        2,
        lambda p: xt.at[:, col(p * dx, dx)],
        lambda o: yr.at[pl.ds(pl.multiple_of(o * tok, tok), tok)],
    )
    ye.start()
    g2.drain()
    sc2.drain()
    for r in rings + [r_gate, r_up, r_down]:
        r.drain()
    ye.wait()
    y_ref[...] = yr[...]
    ye.drain()


VMEM_SPEC = pl.BlockSpec(memory_space=pltpu.VMEM)
ANY_SPEC = pl.BlockSpec(memory_space=pl.ANY)


def rotary_tables(seq_len):
    half = HEAD_DIM // 2
    inv_freq = (THETA ** (-2.0 * np.arange(half) / HEAD_DIM)).astype(np.float32)
    angles = np.arange(seq_len, dtype=np.float32)[:, None] * inv_freq[None, :]
    cos_t, sin_t = np.cos(angles), np.sin(angles)
    return np.concatenate([cos_t, cos_t], -1), np.concatenate([-sin_t, sin_t], -1)


def solution(mesh):
    tx_count, n_dev = mesh.shape["tx"], mesh.shape["ty"]
    act_spec = P(("dp", "ty"), None, "tx")
    col_spec = P("tx", "ty")
    row_spec = P("ty", "tx")
    dma = pltpu.SemaphoreType.DMA

    def layer_fn(x_blk, w_q, w_k, w_v, w_o, w_gate, w_up, w_down):
        seq, dx = x_blk.shape[1:]
        hc, f = w_q.shape[1], w_gate.shape[1]
        tok, d = seq // tx_count, dx * tx_count
        fp = -(-f // 128) * 128
        rows = 4 * tok
        cos_t, sin_t = rotary_tables(seq)
        bf = lambda *shape: pltpu.VMEM(shape, BF16)
        scratch = [
            bf(n_dev, tok, d), bf(n_dev, tok, d), bf(tx_count, dx, 3 * hc), bf(tx_count, hc, dx),
            bf(tx_count, dx, fp), bf(tx_count, dx, fp), bf(tx_count, fp, dx),
            bf(rows, d), bf(rows, hc), bf(rows, fp), bf(3, seq, HEAD_DIM), bf(tok, d), bf(tok, d), bf(seq, dx),
            dma((2,)), dma((3, tx_count)), dma((3, tx_count)), dma((2 * n_dev,)), dma((2 * n_dev,)),
            dma((Gather.SEMS,)), dma((Gather.SEMS,)), dma((7 * RING_SEMS,)), dma((7 * RING_SEMS,)),
        ] + Scatter.buffers(tok, d)
        y = pl.pallas_call(
            functools.partial(layer_kernel, tx_count),
            name="layer",
            out_shape=jax.ShapeDtypeStruct((seq, dx), BF16),
            in_specs=[VMEM_SPEC] + [ANY_SPEC] * 7 + [VMEM_SPEC] * 2,
            out_specs=VMEM_SPEC,
            scratch_shapes=scratch,
            compiler_params=pltpu.CompilerParams(collective_id=1, has_side_effects=True, vmem_limit_bytes=67043328),
        )(x_blk[0], w_q, w_k, w_v, w_o, w_gate.T, w_up.T, w_down, cos_t, sin_t)
        return y[None]

    return jax.shard_map(layer_fn, mesh=mesh, in_specs=(act_spec, col_spec, col_spec, col_spec, row_spec, col_spec, col_spec, row_spec), out_specs=act_spec, check_vma=False)
```

```python
import functools

import numpy as np
import jax
import jax.numpy as jnp
from jax import lax
from jax.experimental import pallas as pl
from jax.experimental.pallas import tpu as pltpu
from jax.sharding import PartitionSpec as P

HEAD_DIM = 128
EPS = 1e-5
THETA = 10000.0
RING = 4
MESH = pl.DeviceIdType.MESH
BF16 = jnp.bfloat16
F32 = jnp.float32
AWAY = (0, -1, 1, 2)


def wrap(v, n):
    return lax.rem(v + 2 * n, n)


class Torus:
    def __init__(self):
        t = lax.axis_index("ty")
        self.me = t
        self.pos = (lax.div(t, RING), lax.rem(t, RING))

    def slot(self, first, a_off, b_off):
        a = wrap(self.pos[first] + a_off, RING)
        b = wrap(self.pos[1 - first] + b_off, RING)
        return a * RING + b if first == 0 else b * RING + a


def entry_barrier(tor, tx_count):
    sem = pltpu.get_barrier_semaphore()
    for first in (0, 1):
        for d in (1, -1):
            pl.semaphore_signal(sem, inc=1, device_id={"ty": tor.slot(first, d, 0)}, device_id_type=MESH)
    me = lax.axis_index("tx")
    for k in range(1, tx_count):
        pl.semaphore_signal(sem, inc=1, device_id={"tx": lax.rem(me + k, tx_count)}, device_id_type=MESH)
    pl.semaphore_wait(sem, 4 + tx_count - 1)


def remote(src, dst, ssem, rsem, device):
    return pltpu.make_async_remote_copy(src_ref=src, dst_ref=dst, send_sem=ssem, recv_sem=rsem, device_id=device, device_id_type=MESH)


class Gather:
    SEMS = 25

    def __init__(self, tor, buf, ssem, rsem):
        self.tor, self.buf, self.ssem, self.rsem = tor, buf, ssem, rsem
        self.q = buf.shape[1] // 4

    def first(self, c):
        return 1 if c == 0 else 0

    def rows(self, c, d, half):
        if not half:
            return pl.ds(c * 2 * self.q, 2 * self.q)
        return pl.ds(c * 2 * self.q + (0 if d == 1 else self.q), self.q)

    def sem(self, c, ph, off, d, half):
        if half:
            return 20 + (0 if ph == 1 else 1 + AWAY.index(off))
        return (0 if ph == 1 else 4 + 4 * AWAY.index(off)) + c * 2 + (0 if d == 1 else 1)

    def copy(self, c, ph, off, d, half, hops):
        first = self.first(c)
        back = -d * hops
        s = self.tor.slot(first, back, 0) if ph == 1 else self.tor.slot(first, off, back)
        to = self.tor.slot(first, d, 0) if ph == 1 else self.tor.slot(first, 0, d)
        view = self.buf.at[s, self.rows(c, d, half)]
        return remote(view, view, self.ssem, self.rsem.at[self.sem(c, ph, off, d, half)], {"ty": to})

    def send(self, c, ph, off, d, half=False):
        self.copy(c, ph, off, d, half, 1 if half else 0).start()

    def recv(self, c, ph, off, d):
        self.copy(c, ph, off, d, False, 1).wait_recv()

    def recv_halves(self, ph, off):
        view = self.buf.at[0]
        remote(view, view, self.ssem, self.rsem.at[self.sem(0, ph, off, 1, True)], {"ty": self.tor.me}).wait_recv()

    def start(self):
        for ph in (1, 2):
            for c in (0, 1):
                for d in (1, -1):
                    self.send(c, ph, 0, d)

    def near(self):
        for d in (1, -1):
            for c in (0, 1):
                self.recv(c, 1, 0, d)
                self.send(c, 1, 0, d, True)

    def spread(self, off):
        for c in (0, 1):
            for d in (1, -1):
                self.send(c, 2, off, d)

    def relay(self, off):
        for d in (1, -1):
            for c in (0, 1):
                self.recv(c, 2, off, d)
                self.send(c, 2, off, d, True)

    def far(self):
        self.recv_halves(1, 0)
        self.spread(2)

    def halves(self, off):
        self.recv_halves(2, off)

    def drain(self):
        view = self.buf.at[pl.ds(0, self.buf.shape[0] - 1)]
        remote(view, view, self.ssem, self.rsem.at[0], {"ty": self.tor.me}).wait_send()


def add_rows(dst, srcs, width=512):
    d = dst.shape[-1]
    width = min(width, d)

    @pl.loop(0, d // width)
    def _(i):
        cols = pl.ds(pl.multiple_of(i * width, width), width)
        tot = srcs[0][:, cols].astype(F32)
        for s in srcs[1:]:
            tot += s[:, cols].astype(F32)
        dst[:, cols] = tot.astype(dst.dtype)


class Scatter:
    SEMS = 30

    @staticmethod
    def buffers(tok, d):
        q = tok // 4
        return [
            pltpu.VMEM((2, 4, 2, q, d), BF16),
            pltpu.VMEM((2, 4, 2, 2 * q, d), BF16),
            pltpu.VMEM((2, 3, 2 * q, d), BF16),
            pltpu.VMEM((2, 2, q, d), BF16),
            pltpu.VMEM((2, 2, 2 * q, d), BF16),
            pltpu.SemaphoreType.DMA,
            pltpu.SemaphoreType.DMA((Scatter.SEMS,)),
        ]

    def __init__(self, tor, part, bufs, order):
        self.tor, self.part, self.order = tor, part, order
        self.h1, self.f1, self.mid, self.h2, self.f2, self.ssem, self.rsem = bufs
        self.q = part.shape[1] // 4

    def copy(self, c, ph, bi, d, kind):
        q, first = self.q, c
        di = 0 if d == 1 else 1
        h = di if kind in (0, 2) else 1 - di
        step = 2 * d if kind == 0 else d
        if ph == 1:
            i = c * 8 + bi * 2 + di if kind == 0 else 16 + c * 4 + bi
            src = self.part.at[self.tor.slot(first, step, self.order[bi]), pl.ds(c * 2 * q + h * q, q)]
            dst = self.h1.at[c, bi, di] if kind == 0 else self.f1.at[c, bi, di, pl.ds(h * q, q)]
            to = self.tor.slot(first, d, 0)
        else:
            i = 24 + c * 2 + di if kind == 0 else 28 + c
            src = self.mid.at[c, self.order.index(2 if kind == 0 else d), pl.ds(h * q, q)]
            dst = self.h2.at[c, di] if kind == 0 else self.f2.at[c, di, pl.ds(h * q, q)]
            to = self.tor.slot(first, 0, d)
        return remote(src, dst, self.ssem, self.rsem.at[i], {"ty": to})

    def all_of(self, view, i):
        remote(view, view, self.ssem, self.rsem.at[i], {"ty": self.tor.me}).wait_recv()

    def issue(self, bi):
        for kind in (0, 1):
            for c in (0, 1):
                for d in (1, -1):
                    self.copy(c, 1, bi, d, kind).start()

    def augment(self, bi):
        q = self.q
        for c in (0, 1):
            for d in (1, -1):
                di = 0 if d == 1 else 1
                self.copy(c, 1, bi, d, 0).wait_recv()
                mine = self.part.at[self.tor.slot(c, d, self.order[bi]), pl.ds(c * 2 * q + di * q, q)]
                add_rows(mine, [mine, self.h1.at[c, bi, di]])
                self.copy(c, 1, bi, d, 2).start()

    def arrived(self, bi):
        q = self.q
        for c in (0, 1):
            self.all_of(self.f1.at[c, bi], 16 + c * 4 + bi)
            off = self.order[bi]
            if off == 0:
                continue
            own = self.part.at[self.tor.slot(c, 0, off), pl.ds(c * 2 * q, 2 * q)]
            add_rows(self.mid.at[c, bi], [own, self.f1.at[c, bi, 0], self.f1.at[c, bi, 1]])
            if off == 2:
                for d in (1, -1):
                    self.copy(c, 2, 0, d, 0).start()
            else:
                self.copy(c, 2, 0, off, 1).start()

    def augment2(self, d):
        q = self.q
        di = 0 if d == 1 else 1
        for c in (0, 1):
            self.copy(c, 2, 0, d, 0).wait_recv()
            mine = self.mid.at[c, self.order.index(d), pl.ds(di * q, q)]
            add_rows(mine, [mine, self.h2.at[c, di]])
            self.copy(c, 2, 0, d, 2).start()

    def last(self):
        for c in (0, 1):
            self.all_of(self.f2.at[c], 28 + c)

    def finish(self, resid, out):
        q, d = self.q, out.shape[-1]
        width = min(512, d)
        for c in (0, 1):
            rows = pl.ds(c * 2 * q, 2 * q)

            @pl.loop(0, d // width)
            def _(i):
                cols = pl.ds(pl.multiple_of(i * width, width), width)
                tot = self.part[self.tor.me, rows, cols].astype(F32)
                for di in (0, 1):
                    tot += self.f1[c, self.order.index(0), di, :, cols].astype(F32)
                for di in (0, 1):
                    tot += self.f2[c, di, :, cols].astype(F32)
                tot = tot.astype(BF16).astype(F32)
                out[rows, cols] = (resid[rows, cols].astype(F32) + tot).astype(BF16)

    def drain(self):
        view = self.part.at[pl.ds(0, self.part.shape[0] - 1)]
        remote(view, view, self.ssem, self.rsem.at[0], {"ty": self.tor.me}).wait_send()


class Exchange:
    def __init__(self, tx_count, src, dst, whole, ssem, rsem):
        self.n, self.src, self.dst, self.whole, self.ssem, self.rsem = tx_count, src, dst, whole, ssem, rsem
        self.me = lax.axis_index("tx")

    def start(self):
        for k in range(1, self.n):
            p = lax.rem(self.me + k, self.n)
            remote(self.src(p), self.dst(self.me), self.ssem, self.rsem, {"tx": p}).start()
        pltpu.make_async_copy(self.src(self.me), self.dst(self.me), self.rsem).start()

    def wait(self):
        view = self.whole(self.n)
        remote(view, view, self.ssem, self.rsem, {"tx": self.me}).wait_recv()

    def drain(self):
        view = self.whole(self.n - 1)
        remote(view, view, self.ssem, self.rsem, {"tx": self.me}).wait_send()


def norm_rows(src, dst):
    tok, d = src.shape
    step = 16

    @pl.loop(0, tok // step)
    def _(i):
        rows = pl.ds(pl.multiple_of(i * step, step), step)
        v = src[rows, :].astype(F32)
        mean = jnp.sum(v, axis=-1, keepdims=True) * (1.0 / d)
        var = jnp.sum(v * v, axis=-1, keepdims=True) * (1.0 / d) - mean * mean
        dst[rows, :] = ((v - mean) * lax.rsqrt(var + EPS)).astype(BF16)


class Ring:
    SEMS = 5

    def __init__(self, tx_count, rows, src, slot, whole, ssem, rsem):
        self.nx, self.rows, self.src, self.slot, self.whole, self.ssem, self.rsem = tx_count // 2, rows, src, slot, whole, ssem, rsem
        me = lax.axis_index("tx")
        self.me, self.x, self.core = me, lax.div(me, 2), lax.rem(me, 2)
        self.split = (rows // 2 + 15) // 16 * 16

    def tx(self, dx, other=False):
        return wrap(self.x + dx, self.nx) * 2 + (1 - self.core if other else self.core)

    def half(self, view, d):
        return view.at[pl.ds(0, self.split)] if d == 1 else view.at[pl.ds(self.split, self.rows - self.split)]

    def copy(self, i, src, dst, to):
        return remote(src, dst, self.ssem, self.rsem.at[i], {"tx": to})

    def pass_on(self, d, recv=False):
        view = self.slot(self.tx(-d if recv else 0))
        return self.copy(0 if d == 1 else 1, view if recv else self.src, view, self.tx(d))

    def relay(self, d, recv=False):
        view = self.half(self.slot(self.tx(-2 * d if recv else -d)), d)
        return self.copy(2 if d == 1 else 3, view, view, self.tx(d))

    def across(self, which, recv=False):
        view = self.slot(self.tx(which, recv))
        if abs(which) == 2:
            view = self.half(view, which // 2)
        src = self.src if which == 0 and not recv else view
        return self.copy(4, src, view, self.tx(0, True))

    def all_across(self):
        return (0, 1, -1, 2, -2) if self.nx > 1 else (0,)

    def own(self):
        return pltpu.make_async_copy(self.src, self.slot(self.me), self.rsem.at[4])

    def start(self, place=True):
        if self.nx > 1:
            for d in (1, -1):
                self.pass_on(d).start()
        self.across(0).start()
        if place:
            self.own().start()

    def step(self):
        if self.nx > 1:
            for d in (1, -1):
                self.pass_on(d, True).wait_recv()
                self.relay(d).start()
                self.across(-d).start()

    def step2(self):
        if self.nx > 1:
            for d in (1, -1):
                self.relay(d, True).wait_recv()
                self.across(2 * d).start()

    def finish(self, place=True):
        view = self.whole(self.nx + (1 if place else 0))
        remote(view, view, self.ssem, self.rsem.at[4], {"tx": self.me}).wait_recv()

    def drain(self):
        view = self.whole(2 * self.nx - 1)
        remote(view, view, self.ssem, self.rsem.at[4], {"tx": self.me}).wait_send()


def layer_kernel(tx_count, x_ref, wq_ref, wk_ref, wv_ref, wo_ref, wg_ref, wu_ref, wd_ref, cos_hbm, sin_hbm, y_ref,
                 xp, x2, wqkv, wo, wg, wu, wd, xs, os_, act, kv, xt, h, yr, cos_ref, sin_ref,
                 load_sem, a2a_s, a2a_r, qkv_s, qkv_r, gs, gr, ws, wr, *rs_bufs):
    n_dev, tok, d = xp.shape
    dx = x_ref.shape[1]
    hc = wq_ref.shape[1]
    f, fp = wg_ref.shape[0], wg.shape[2]
    seq = tok * tx_count
    spd = n_dev // tx_count
    heads = hc // HEAD_DIM
    q2 = tok // 2
    c3 = 3 * hc
    tor = Torus()
    me_tx = lax.axis_index("tx")

    def exchange(i, src, dst, whole):
        return Exchange(tx_count, src, dst, whole, a2a_s.at[i], a2a_r.at[i])

    def col(start, width):
        return pl.ds(pl.multiple_of(start, width), width)

    def ring(i, src, buf, inner):
        return Ring(tx_count, src.shape[0], src, lambda o: buf.at[(o, *inner)], lambda n: buf.at[(pl.ds(0, n), *inner)], ws.at[i], wr.at[i])

    every = pl.ds(0, dx)
    rings = [ring(i, src, wqkv, (every, pl.ds(i * hc, hc))) for i, src in enumerate((wq_ref, wk_ref, wv_ref))]
    r_o = ring(3, wo_ref, wo, ())
    r_gate = ring(4, wg.at[me_tx], wg, ())
    r_up = ring(5, wu.at[me_tx], wu, ())
    r_down = ring(6, wd_ref, wd, (pl.ds(0, f),))

    x_in = pltpu.make_async_copy(x_ref, yr, load_sem.at[2])
    x_in.start()
    raw = [pltpu.make_async_copy(src, wd.at[i, pl.ds(0, f)], load_sem.at[i]) for i, src in enumerate((wg_ref, wu_ref))]
    raw += [pltpu.make_async_copy(cos_hbm, cos_ref, load_sem.at[3]), pltpu.make_async_copy(sin_hbm, sin_ref, load_sem.at[4])]
    for cp in raw:
        cp.start()
    entry_barrier(tor, tx_count)
    x_in.wait()
    xe = exchange(
        0,
        lambda p: yr.at[pl.ds(pl.multiple_of(p * tok, tok), tok)],
        lambda o: xt.at[:, col(o * dx, dx)],
        lambda n: yr.at[pl.ds(0, n * tok)],
    )
    xe.start()
    if fp > f:
        wd[:, pl.ds(f, fp - f), :] = jnp.zeros((tx_count, fp - f, dx), BF16)
    xe.wait()
    norm_rows(xt, xp.at[tor.me])
    g1 = Gather(tor, xp, gs, gr)
    g1.start()
    for r in rings:
        r.start()
    for cp in raw:
        cp.wait()
    for i, dst in enumerate((wg, wu)):
        for j in range(fp // 128):
            dst[me_tx, :, pl.ds(j * 128, 128)] = wd[i, pl.ds(j * 128, 128), :].T

    def pieces(off):
        return [(c, tor.slot(1 - c, off, n), (c * 4 + n) * q2) for c in (0, 1) for n in range(RING)]

    def stage(src, off, dst, cols):
        for c, s, at in pieces(off):
            dst[pl.ds(at, q2), :] = src[s, pl.ds(c * q2, q2), cols]

    def qkv_group(off):
        stage(xp, off, xs, pl.ds(0, d))

        @pl.loop(0, 3)
        def _(n):
            cols = col(n * hc, hc)
            out = jnp.dot(xs[...], wqkv[:, :, cols].reshape(d, hc), preferred_element_type=F32).astype(BF16)
            for c, s, at in pieces(off):
                x2[s, pl.ds(c * q2, q2), cols] = out[at : at + q2]

        for c, s, _ in pieces(off):
            p, sl = lax.div(s, spd), lax.rem(s, spd)
            rows = pl.ds(c * q2, q2)
            src = x2.at[s, rows, pl.ds(0, c3)]
            dst = x2.at[sl * tx_count + me_tx, rows, pl.ds(c3, c3)]

            @pl.when(p == me_tx)
            def _():
                pltpu.make_async_copy(src, dst, qkv_r.at[sl]).start()

            @pl.when(p != me_tx)
            def _():
                remote(src, dst, qkv_s, qkv_r.at[sl], {"tx": p}).start()

    xe.drain()
    wq_r, wk_r, wv_r = rings
    g1.near()
    wq_r.step()
    g1.relay(0)
    g1.spread(-1)
    g1.spread(1)
    wk_r.step()
    wv_r.step()
    g1.halves(0)
    wq_r.step2()
    wk_r.step2()
    g1.relay(-1)
    g1.far()
    wv_r.step2()
    g1.relay(1)
    for r in rings:
        r.finish()
    qkv_group(0)
    g1.halves(-1)
    qkv_group(-1)
    g1.relay(2)
    g1.halves(1)
    qkv_group(1)
    g1.halves(2)
    qkv_group(2)

    block = min(seq, 128)
    sends = []
    for s in range(spd):
        view = x2.at[pl.ds(s * tx_count, tx_count), :, pl.ds(c3, c3)]
        remote(view, view, qkv_s, qkv_r.at[s], {"tx": me_tx}).wait_recv()
        if s == spd - 1:
            r_o.start()

        @pl.loop(0, heads)
        def _(hd):
            def part(which):
                return x2[pl.ds(s * tx_count, tx_count), :, col(c3 + which * hc + hd * HEAD_DIM, HEAD_DIM)].reshape(seq, HEAD_DIM)

            for which in (0, 1):
                v = part(which).astype(F32)
                rot = v * cos_ref[...] + pltpu.roll(v, HEAD_DIM // 2, 1) * sin_ref[...]
                kv[which] = rot.astype(BF16)
            kv[2] = part(2)
            for b in range(seq // block):
                keys = (b + 1) * block
                sc = lax.dot_general(kv[0, pl.ds(b * block, block)], kv[1, pl.ds(0, keys)], (((1,), (1,)), ((), ())), preferred_element_type=F32)
                sc = sc * HEAD_DIM ** -0.5
                q_pos = b * block + lax.broadcasted_iota(jnp.int32, (block, keys), 0)
                k_pos = lax.broadcasted_iota(jnp.int32, (block, keys), 1)
                sc = jnp.where(q_pos >= k_pos, sc, -1e30)
                e = jnp.exp(sc - jnp.max(sc, axis=-1, keepdims=True))
                prob = (e / jnp.sum(e, axis=-1, keepdims=True)).astype(BF16)
                o = jnp.dot(prob, kv[2, pl.ds(0, keys)], preferred_element_type=F32).astype(BF16)
                for n in range(block // tok):
                    at = (b * (block // tok) + n) * spd + s
                    x2[at, :, col(2 * c3 + hd * HEAD_DIM, HEAD_DIM)] = o[n * tok : (n + 1) * tok]

        oe = exchange(
            1 + s,
            lambda p, s=s: x2.at[p * spd + s, :, pl.ds(2 * c3, hc)],
            lambda o, s=s: x2.at[o * spd + s, :, pl.ds(2 * c3 + hc, hc)],
            lambda n: x2.at[pl.ds(0, n), :, pl.ds(2 * c3, hc)],
        )
        oe.start()
        sends.append(oe)

    r_o.step()
    g1.drain()
    view = x2.at[pl.ds(0, (tx_count - 1) * spd), :, pl.ds(0, c3)]
    remote(view, view, qkv_s, qkv_r.at[0], {"tx": me_tx}).wait_send()
    for oe in sends:
        oe.wait()
        oe.drain()
    r_o.step2()
    r_gate.start(place=False)
    r_up.start(place=False)
    r_down.start()
    r_o.finish()

    def put(off, x, out):
        for c, s, at in pieces(off):
            xp[s, pl.ds(c * q2, q2), col(x * dx, dx)] = out[at : at + q2]

    def o_group(off):
        stage(x2, off, os_, pl.ds(2 * c3 + hc, hc))

        @pl.loop(0, tx_count)
        def _(x):
            put(off, x, jnp.dot(os_[...], wo[x], preferred_element_type=F32).astype(BF16))

    order = (2, -1, 1, 0)
    sc1 = Scatter(tor, xp, rs_bufs, order)
    o_group(order[0])
    sc1.issue(0)
    o_group(order[1])
    sc1.issue(1)
    o_group(order[2])
    sc1.augment(0)
    sc1.issue(2)
    o_group(order[3])
    sc1.augment(1)
    sc1.issue(3)
    sc1.arrived(0)
    r_gate.step()
    sc1.augment(2)
    sc1.arrived(1)
    sc1.augment2(-1)
    sc1.augment(3)
    sc1.arrived(2)
    sc1.augment2(1)
    r_up.step()
    sc1.arrived(3)
    sc1.last()
    sc1.finish(xt, h)
    norm_rows(h, x2.at[tor.me])
    g2 = Gather(tor, x2, gs, gr)
    g2.start()
    sc1.drain()

    def mlp_group(off, between):
        stage(x2, off, xs, pl.ds(0, d))
        width = 256 if fp % 256 == 0 else 128

        @pl.loop(0, fp // width)
        def _(n):
            cols = col(n * width, width)
            gate = jnp.dot(xs[...], wg[:, :, cols].reshape(d, width), preferred_element_type=F32).astype(BF16).astype(F32)
            up = jnp.dot(xs[...], wu[:, :, cols].reshape(d, width), preferred_element_type=F32).astype(BF16).astype(F32)
            act[:, cols] = (gate * jax.nn.sigmoid(gate) * up).astype(BF16)

        between()

        @pl.loop(0, tx_count)
        def _(x):
            put(off, x, jnp.dot(act[...], wd[x], preferred_element_type=F32).astype(BF16))

    sc2 = Scatter(tor, xp, rs_bufs, (-1, 1, 2, 0))
    g2.near()
    r_down.step()
    g2.relay(0)
    g2.spread(-1)
    g2.spread(1)
    r_gate.step2()
    r_up.step2()
    g2.halves(0)
    r_gate.finish(place=False)
    r_up.finish(place=False)

    def rest():
        g2.relay(-1)
        g2.far()
        r_down.step2()
        r_down.finish()

    mlp_group(0, rest)
    g2.relay(1)
    g2.halves(-1)
    mlp_group(-1, lambda: g2.relay(2))
    sc2.issue(0)
    g2.halves(1)
    mlp_group(1, lambda: None)
    sc2.issue(1)
    g2.halves(2)
    mlp_group(2, lambda: None)
    sc2.issue(2)
    sc2.augment(0)
    sc2.augment(1)
    sc2.issue(3)
    sc2.arrived(0)
    sc2.augment(2)
    sc2.arrived(1)
    sc2.arrived(2)
    sc2.augment(3)
    sc2.augment2(-1)
    sc2.augment2(1)
    sc2.arrived(3)
    sc2.last()
    sc2.finish(h, xt)
    ye = exchange(
        1 + spd,
        lambda p: xt.at[:, col(p * dx, dx)],
        lambda o: yr.at[pl.ds(pl.multiple_of(o * tok, tok), tok)],
        lambda n: yr.at[pl.ds(0, n * tok)],
    )
    ye.start()
    g2.drain()
    sc2.drain()
    for r in rings + [r_o, r_gate, r_up, r_down]:
        r.drain()
    ye.wait()
    out = pltpu.make_async_copy(yr, y_ref, load_sem.at[0])
    out.start()
    ye.drain()
    out.wait()


ANY_SPEC = pl.BlockSpec(memory_space=pl.ANY)


def rotary_tables(seq_len):
    half = HEAD_DIM // 2
    inv_freq = (THETA ** (-2.0 * np.arange(half) / HEAD_DIM)).astype(np.float32)
    angles = np.arange(seq_len, dtype=np.float32)[:, None] * inv_freq[None, :]
    cos_t, sin_t = np.cos(angles), np.sin(angles)
    return np.concatenate([cos_t, cos_t], -1), np.concatenate([-sin_t, sin_t], -1)


def solution(mesh):
    tx_count, n_dev = mesh.shape["tx"], mesh.shape["ty"]
    act_spec = P(("dp", "ty"), None, "tx")
    col_spec = P("tx", "ty")
    row_spec = P("ty", "tx")
    dma = pltpu.SemaphoreType.DMA

    def layer_fn(x_blk, w_q, w_k, w_v, w_o, w_gate, w_up, w_down):
        seq, dx = x_blk.shape[1:]
        hc, f = w_q.shape[1], w_gate.shape[1]
        tok, d = seq // tx_count, dx * tx_count
        fp = -(-f // 128) * 128
        rows, spd = 4 * tok, n_dev // tx_count
        cos_t, sin_t = rotary_tables(seq)
        bf = lambda *shape: pltpu.VMEM(shape, BF16)
        scratch = [
            bf(n_dev, tok, d), bf(n_dev, tok, d), bf(tx_count, dx, 3 * hc), bf(tx_count, hc, dx),
            bf(tx_count, dx, fp), bf(tx_count, dx, fp), bf(tx_count, fp, dx),
            bf(rows, d), bf(rows, hc), bf(rows, fp), bf(3, seq, HEAD_DIM), bf(tok, d), bf(tok, d), bf(seq, dx),
            pltpu.VMEM((seq, HEAD_DIM), F32), pltpu.VMEM((seq, HEAD_DIM), F32),
            dma((5,)), dma((spd + 2,)), dma((spd + 2,)), dma, dma((spd,)),
            dma, dma((Gather.SEMS,)), dma((7,)), dma((7, Ring.SEMS)),
        ] + Scatter.buffers(tok, d)
        y = pl.pallas_call(
            functools.partial(layer_kernel, tx_count),
            name="layer",
            out_shape=jax.ShapeDtypeStruct((seq, dx), BF16),
            in_specs=[ANY_SPEC] * 10,
            out_specs=ANY_SPEC,
            scratch_shapes=scratch,
            compiler_params=pltpu.CompilerParams(collective_id=1, has_side_effects=True, vmem_limit_bytes=67043328),
        )(x_blk[0], w_q, w_k, w_v, w_o, w_gate.T, w_up.T, w_down, cos_t, sin_t)
        return y[None]

    return jax.shard_map(layer_fn, mesh=mesh, in_specs=(act_spec, col_spec, col_spec, col_spec, row_spec, col_spec, col_spec, row_spec), out_specs=act_spec, check_vma=False)
```

```python
import functools

import numpy as np
import jax
import jax.numpy as jnp
from jax import lax
from jax.experimental import pallas as pl
from jax.experimental.pallas import tpu as pltpu
from jax.sharding import PartitionSpec as P

HEAD_DIM = 128
EPS = 1e-5
THETA = 10000.0
RING = 4
MESH = pl.DeviceIdType.MESH
BF16 = jnp.bfloat16
F32 = jnp.float32
AWAY = (0, -1, 1, 2)


def wrap(v, n):
    return lax.rem(v + 2 * n, n)


class Torus:
    def __init__(self):
        t = lax.axis_index("ty")
        self.me = t
        self.pos = (lax.div(t, RING), lax.rem(t, RING))

    def slot(self, first, a_off, b_off):
        a = wrap(self.pos[first] + a_off, RING)
        b = wrap(self.pos[1 - first] + b_off, RING)
        return a * RING + b if first == 0 else b * RING + a


def entry_barrier(tor, tx_count):
    sem = pltpu.get_barrier_semaphore()
    for first in (0, 1):
        for d in (1, -1):
            pl.semaphore_signal(sem, inc=1, device_id={"ty": tor.slot(first, d, 0)}, device_id_type=MESH)
    me = lax.axis_index("tx")
    for k in range(1, tx_count):
        pl.semaphore_signal(sem, inc=1, device_id={"tx": lax.rem(me + k, tx_count)}, device_id_type=MESH)
    pl.semaphore_wait(sem, 4 + tx_count - 1)


def remote(src, dst, ssem, rsem, device):
    return pltpu.make_async_remote_copy(src_ref=src, dst_ref=dst, send_sem=ssem, recv_sem=rsem, device_id=device, device_id_type=MESH)


class Gather:
    SEMS = 25

    def __init__(self, tor, buf, ssem, rsem):
        self.tor, self.buf, self.ssem, self.rsem = tor, buf, ssem, rsem
        self.q = buf.shape[1] // 4

    def first(self, c):
        return 1 if c == 0 else 0

    def rows(self, c, d, half):
        if not half:
            return pl.ds(c * 2 * self.q, 2 * self.q)
        return pl.ds(c * 2 * self.q + (0 if d == 1 else self.q), self.q)

    def sem(self, c, ph, off, d, half):
        if half:
            return 20 + (0 if ph == 1 else 1 + AWAY.index(off))
        return (0 if ph == 1 else 4 + 4 * AWAY.index(off)) + c * 2 + (0 if d == 1 else 1)

    def copy(self, c, ph, off, d, half, hops):
        first = self.first(c)
        back = -d * hops
        s = self.tor.slot(first, back, 0) if ph == 1 else self.tor.slot(first, off, back)
        to = self.tor.slot(first, d, 0) if ph == 1 else self.tor.slot(first, 0, d)
        view = self.buf.at[s, self.rows(c, d, half)]
        return remote(view, view, self.ssem, self.rsem.at[self.sem(c, ph, off, d, half)], {"ty": to})

    def send(self, c, ph, off, d, half=False):
        self.copy(c, ph, off, d, half, 1 if half else 0).start()

    def recv(self, c, ph, off, d):
        self.copy(c, ph, off, d, False, 1).wait_recv()

    def recv_halves(self, ph, off):
        view = self.buf.at[0]
        remote(view, view, self.ssem, self.rsem.at[self.sem(0, ph, off, 1, True)], {"ty": self.tor.me}).wait_recv()

    def start(self):
        for ph in (1, 2):
            for c in (0, 1):
                for d in (1, -1):
                    self.send(c, ph, 0, d)

    def near(self):
        for d in (1, -1):
            for c in (0, 1):
                self.recv(c, 1, 0, d)
                self.send(c, 1, 0, d, True)

    def spread(self, off):
        for c in (0, 1):
            for d in (1, -1):
                self.send(c, 2, off, d)

    def relay(self, off):
        for d in (1, -1):
            for c in (0, 1):
                self.recv(c, 2, off, d)
                self.send(c, 2, off, d, True)

    def far(self):
        self.recv_halves(1, 0)
        self.spread(2)

    def halves(self, off):
        self.recv_halves(2, off)

    def drain(self):
        view = self.buf.at[pl.ds(0, self.buf.shape[0] - 1)]
        remote(view, view, self.ssem, self.rsem.at[0], {"ty": self.tor.me}).wait_send()


def add_rows(dst, srcs, width=512):
    d = dst.shape[-1]
    width = min(width, d)

    @pl.loop(0, d // width)
    def _(i):
        cols = pl.ds(pl.multiple_of(i * width, width), width)
        tot = srcs[0][:, cols].astype(F32)
        for s in srcs[1:]:
            tot += s[:, cols].astype(F32)
        dst[:, cols] = tot.astype(dst.dtype)


class Scatter:
    SEMS = 30

    @staticmethod
    def buffers(tok, d):
        q = tok // 4
        return [
            pltpu.VMEM((2, 4, 2, q, d), BF16),
            pltpu.VMEM((2, 4, 2, 2 * q, d), BF16),
            pltpu.VMEM((2, 3, 2 * q, d), BF16),
            pltpu.VMEM((2, 2, q, d), BF16),
            pltpu.VMEM((2, 2, 2 * q, d), BF16),
            pltpu.SemaphoreType.DMA,
            pltpu.SemaphoreType.DMA((Scatter.SEMS,)),
        ]

    def __init__(self, tor, part, bufs, order):
        self.tor, self.part, self.order = tor, part, order
        self.h1, self.f1, self.mid, self.h2, self.f2, self.ssem, self.rsem = bufs
        self.q = part.shape[1] // 4

    def copy(self, c, ph, bi, d, kind):
        q, first = self.q, c
        di = 0 if d == 1 else 1
        h = di if kind in (0, 2) else 1 - di
        step = 2 * d if kind == 0 else d
        if ph == 1:
            i = c * 8 + bi * 2 + di if kind == 0 else 16 + c * 4 + bi
            src = self.part.at[self.tor.slot(first, step, self.order[bi]), pl.ds(c * 2 * q + h * q, q)]
            dst = self.h1.at[c, bi, di] if kind == 0 else self.f1.at[c, bi, di, pl.ds(h * q, q)]
            to = self.tor.slot(first, d, 0)
        else:
            i = 24 + c * 2 + di if kind == 0 else 28 + c
            src = self.mid.at[c, self.order.index(2 if kind == 0 else d), pl.ds(h * q, q)]
            dst = self.h2.at[c, di] if kind == 0 else self.f2.at[c, di, pl.ds(h * q, q)]
            to = self.tor.slot(first, 0, d)
        return remote(src, dst, self.ssem, self.rsem.at[i], {"ty": to})

    def all_of(self, view, i):
        remote(view, view, self.ssem, self.rsem.at[i], {"ty": self.tor.me}).wait_recv()

    def issue(self, bi):
        for kind in (0, 1):
            for c in (0, 1):
                for d in (1, -1):
                    self.copy(c, 1, bi, d, kind).start()

    def augment(self, bi):
        q = self.q
        for c in (0, 1):
            for d in (1, -1):
                di = 0 if d == 1 else 1
                self.copy(c, 1, bi, d, 0).wait_recv()
                mine = self.part.at[self.tor.slot(c, d, self.order[bi]), pl.ds(c * 2 * q + di * q, q)]
                add_rows(mine, [mine, self.h1.at[c, bi, di]])
                self.copy(c, 1, bi, d, 2).start()

    def arrived(self, bi):
        q = self.q
        for c in (0, 1):
            self.all_of(self.f1.at[c, bi], 16 + c * 4 + bi)
            off = self.order[bi]
            if off == 0:
                continue
            own = self.part.at[self.tor.slot(c, 0, off), pl.ds(c * 2 * q, 2 * q)]
            add_rows(self.mid.at[c, bi], [own, self.f1.at[c, bi, 0], self.f1.at[c, bi, 1]])
            if off == 2:
                for d in (1, -1):
                    self.copy(c, 2, 0, d, 0).start()
            else:
                self.copy(c, 2, 0, off, 1).start()

    def augment2(self, d):
        q = self.q
        di = 0 if d == 1 else 1
        for c in (0, 1):
            self.copy(c, 2, 0, d, 0).wait_recv()
            mine = self.mid.at[c, self.order.index(d), pl.ds(di * q, q)]
            add_rows(mine, [mine, self.h2.at[c, di]])
            self.copy(c, 2, 0, d, 2).start()

    def last(self):
        for c in (0, 1):
            self.all_of(self.f2.at[c], 28 + c)

    def finish(self, resid, out):
        q, d = self.q, out.shape[-1]
        width = min(512, d)
        for c in (0, 1):
            rows = pl.ds(c * 2 * q, 2 * q)

            @pl.loop(0, d // width)
            def _(i):
                cols = pl.ds(pl.multiple_of(i * width, width), width)
                tot = self.part[self.tor.me, rows, cols].astype(F32)
                for di in (0, 1):
                    tot += self.f1[c, self.order.index(0), di, :, cols].astype(F32)
                for di in (0, 1):
                    tot += self.f2[c, di, :, cols].astype(F32)
                tot = tot.astype(BF16).astype(F32)
                out[rows, cols] = (resid[rows, cols].astype(F32) + tot).astype(BF16)

    def drain(self):
        view = self.part.at[pl.ds(0, self.part.shape[0] - 1)]
        remote(view, view, self.ssem, self.rsem.at[0], {"ty": self.tor.me}).wait_send()


class Exchange:
    def __init__(self, tx_count, src, dst, whole, ssem, rsem):
        self.n, self.src, self.dst, self.whole, self.ssem, self.rsem = tx_count, src, dst, whole, ssem, rsem
        self.me = lax.axis_index("tx")

    def start(self):
        for k in range(1, self.n):
            p = lax.rem(self.me + k, self.n)
            remote(self.src(p), self.dst(self.me), self.ssem, self.rsem, {"tx": p}).start()
        pltpu.make_async_copy(self.src(self.me), self.dst(self.me), self.rsem).start()

    def wait(self):
        view = self.whole(self.n)
        remote(view, view, self.ssem, self.rsem, {"tx": self.me}).wait_recv()

    def drain(self):
        view = self.whole(self.n - 1)
        remote(view, view, self.ssem, self.rsem, {"tx": self.me}).wait_send()


def norm_rows(src, dst):
    tok, d = src.shape
    step = 16

    @pl.loop(0, tok // step)
    def _(i):
        rows = pl.ds(pl.multiple_of(i * step, step), step)
        v = src[rows, :].astype(F32)
        mean = jnp.sum(v, axis=-1, keepdims=True) * (1.0 / d)
        var = jnp.sum(v * v, axis=-1, keepdims=True) * (1.0 / d) - mean * mean
        dst[rows, :] = ((v - mean) * lax.rsqrt(var + EPS)).astype(BF16)


class Ring:
    SEMS = 5

    def __init__(self, tx_count, rows, src, slot, whole, ssem, rsem):
        self.nx, self.rows, self.src, self.slot, self.whole, self.ssem, self.rsem = tx_count // 2, rows, src, slot, whole, ssem, rsem
        me = lax.axis_index("tx")
        self.me, self.x, self.core = me, lax.div(me, 2), lax.rem(me, 2)
        self.split = (rows // 2 + 15) // 16 * 16

    def tx(self, dx, other=False):
        return wrap(self.x + dx, self.nx) * 2 + (1 - self.core if other else self.core)

    def half(self, view, d):
        return view.at[pl.ds(0, self.split)] if d == 1 else view.at[pl.ds(self.split, self.rows - self.split)]

    def copy(self, i, src, dst, to):
        return remote(src, dst, self.ssem, self.rsem.at[i], {"tx": to})

    def pass_on(self, d, recv=False):
        view = self.slot(self.tx(-d if recv else 0))
        return self.copy(0 if d == 1 else 1, view if recv else self.src, view, self.tx(d))

    def relay(self, d, recv=False):
        view = self.half(self.slot(self.tx(-2 * d if recv else -d)), d)
        return self.copy(2 if d == 1 else 3, view, view, self.tx(d))

    def across(self, which, recv=False):
        view = self.slot(self.tx(which, recv))
        if abs(which) == 2:
            view = self.half(view, which // 2)
        src = self.src if which == 0 and not recv else view
        return self.copy(4, src, view, self.tx(0, True))

    def all_across(self):
        return (0, 1, -1, 2, -2) if self.nx > 1 else (0,)

    def own(self):
        return pltpu.make_async_copy(self.src, self.slot(self.me), self.rsem.at[4])

    def start(self, place=True):
        if self.nx > 1:
            for d in (1, -1):
                self.pass_on(d).start()
        self.across(0).start()
        if place:
            self.own().start()

    def step(self):
        if self.nx > 1:
            for d in (1, -1):
                self.pass_on(d, True).wait_recv()
                self.relay(d).start()
                self.across(-d).start()

    def step2(self):
        if self.nx > 1:
            for d in (1, -1):
                self.relay(d, True).wait_recv()
                self.across(2 * d).start()

    def finish(self, place=True):
        view = self.whole(self.nx + (1 if place else 0))
        remote(view, view, self.ssem, self.rsem.at[4], {"tx": self.me}).wait_recv()

    def drain(self):
        view = self.whole(2 * self.nx - 1)
        remote(view, view, self.ssem, self.rsem.at[4], {"tx": self.me}).wait_send()


def layer_kernel(tx_count, x_ref, wq_ref, wk_ref, wv_ref, wo_ref, wg_ref, wu_ref, wd_ref, cos_hbm, sin_hbm, y_ref,
                 xp, x2, wqkv, wo, wg, wu, wd, xs, os_, act, kv, xt, h, yr, cos_ref, sin_ref,
                 load_sem, a2a_s, a2a_r, qkv_s, qkv_r, via_s, via_r, gs, gr, ws, wr, *rs_bufs):
    n_dev, tok, d = xp.shape
    dx = x_ref.shape[1]
    hc = wq_ref.shape[1]
    f, fp = wg_ref.shape[0], wg.shape[2]
    seq = tok * tx_count
    spd = n_dev // tx_count
    heads = hc // HEAD_DIM
    q2 = tok // 2
    c3 = 3 * hc
    tor = Torus()
    me_tx = lax.axis_index("tx")

    def exchange(i, src, dst, whole):
        return Exchange(tx_count, src, dst, whole, a2a_s.at[i], a2a_r.at[i])

    def col(start, width):
        return pl.ds(pl.multiple_of(start, width), width)

    def ring(i, src, buf, inner):
        return Ring(tx_count, src.shape[0], src, lambda o: buf.at[(o, *inner)], lambda n: buf.at[(pl.ds(0, n), *inner)], ws.at[i], wr.at[i])

    every = pl.ds(0, dx)
    rings = [ring(i, src, wqkv, (every, pl.ds(i * hc, hc))) for i, src in enumerate((wq_ref, wk_ref, wv_ref))]
    r_o = ring(3, wo_ref, wo, ())
    r_gate = ring(4, wg.at[me_tx], wg, ())
    r_up = ring(5, wu.at[me_tx], wu, ())
    r_down = ring(6, wd_ref, wd, (pl.ds(0, f),))

    x_in = pltpu.make_async_copy(x_ref, yr, load_sem.at[2])
    x_in.start()
    raw = [pltpu.make_async_copy(src, wd.at[i, pl.ds(0, f)], load_sem.at[i]) for i, src in enumerate((wg_ref, wu_ref))]
    raw += [pltpu.make_async_copy(cos_hbm, cos_ref, load_sem.at[3]), pltpu.make_async_copy(sin_hbm, sin_ref, load_sem.at[4])]
    for cp in raw:
        cp.start()
    entry_barrier(tor, tx_count)
    x_in.wait()
    xe = exchange(
        0,
        lambda p: yr.at[pl.ds(pl.multiple_of(p * tok, tok), tok)],
        lambda o: xt.at[:, col(o * dx, dx)],
        lambda n: yr.at[pl.ds(0, n * tok)],
    )
    xe.start()
    if fp > f:
        wd[:, pl.ds(f, fp - f), :] = jnp.zeros((tx_count, fp - f, dx), BF16)
    xe.wait()
    norm_rows(xt, xp.at[tor.me])
    g1 = Gather(tor, xp, gs, gr)
    g1.start()
    for r in rings:
        r.start()
    for cp in raw:
        cp.wait()
    for i, dst in enumerate((wg, wu)):
        for j in range(fp // 128):
            dst[me_tx, :, pl.ds(j * 128, 128)] = wd[i, pl.ds(j * 128, 128), :].T

    def pieces(off):
        return [(c, tor.slot(1 - c, off, n), (c * 4 + n) * q2) for c in (0, 1) for n in range(RING)]

    def stage(src, off, dst, cols):
        for c, s, at in pieces(off):
            dst[pl.ds(at, q2), :] = src[s, pl.ds(c * q2, q2), cols]

    detours = tx_count == 8
    x_pos = lax.div(me_tx, 2)
    edge = (x_pos == 0) | (x_pos == 3)
    opposite = jnp.where(x_pos == 0, 2, 1)
    inner = jnp.where(x_pos == 0, 1, 2)
    over = (3 - x_pos) * 2 + lax.rem(me_tx, 2)
    via = pl.ds(2 * c3 + 2 * hc, c3)

    def qkv_group(off):
        stage(xp, off, xs, pl.ds(0, d))

        @pl.loop(0, 3)
        def _(n):
            cols = col(n * hc, hc)
            out = jnp.dot(xs[...], wqkv[:, :, cols].reshape(d, hc), preferred_element_type=F32).astype(BF16)
            for c, s, at in pieces(off):
                x2[s, pl.ds(c * q2, q2), cols] = out[at : at + q2]

        for c, s, _ in pieces(off):
            p, sl = lax.div(s, spd), lax.rem(s, spd)
            rows = pl.ds(c * q2, q2)
            src = x2.at[s, rows, pl.ds(0, c3)]
            dst = x2.at[sl * tx_count + me_tx, rows, pl.ds(c3, c3)]

            detour = (p != p) if off == 2 or not detours else edge & (lax.div(p, 2) == opposite)

            @pl.when(p == me_tx)
            def _():
                pltpu.make_async_copy(src, dst, qkv_r.at[sl]).start()

            @pl.when(detour)
            def _():
                remote(src, x2.at[s, rows, via], qkv_s, via_r.at[2 * AWAY.index(off) + c], {"tx": over}).start()

            @pl.when((p != me_tx) & jnp.logical_not(detour))
            def _():
                remote(src, dst, qkv_s, qkv_r.at[sl], {"tx": p}).start()

    def detour_rows(off, c):
        rows = pl.ds(c * q2, q2)
        return [(s, rows) for s in ([inner * RING + wrap(tor.pos[1] + off, RING)] if c == 0 else [inner * RING + y for y in range(RING)])]

    def pass_detour(off):
        if not detours:
            return
        for c in (0, 1):

            @pl.when(edge if c == 0 else edge & (wrap(tor.pos[0] + off, RING) == inner))
            def _():
                for s, rows in detour_rows(off, c):
                    view = x2.at[s, rows, via]
                    if c == 0:
                        remote(view, view, via_s, via_r.at[2 * AWAY.index(off) + c], {"tx": me_tx}).wait_recv()
                if c == 1:
                    view = x2.at[pl.ds(inner * RING, 2), :, via]
                    remote(view, view, via_s, via_r.at[2 * AWAY.index(off) + c], {"tx": me_tx}).wait_recv()
                for s, rows in detour_rows(off, c):
                    p, sl = lax.div(s, spd), lax.rem(s, spd)
                    remote(x2.at[s, rows, via], x2.at[sl * tx_count + over, rows, pl.ds(c3, c3)], via_s, qkv_r.at[sl], {"tx": p}).start()

    def drain_detours():
        if not detours:
            return
        for off in (0, -1, 1):
            for c in (0, 1):

                @pl.when(edge if c == 0 else edge & (wrap(tor.pos[0] + off, RING) == inner))
                def _():
                    view = x2.at[0, pl.ds(0, q2), via] if c == 0 else x2.at[pl.ds(0, 2), :, via]
                    remote(view, view, via_s, via_r.at[0], {"tx": me_tx}).wait_send()

    xe.drain()
    wq_r, wk_r, wv_r = rings
    g1.near()
    wq_r.step()
    g1.relay(0)
    g1.spread(-1)
    g1.spread(1)
    wk_r.step()
    wv_r.step()
    r_o.start()
    g1.halves(0)
    wq_r.step2()
    wk_r.step2()
    g1.relay(-1)
    wv_r.step2()
    for r in rings:
        r.finish()
    qkv_group(0)
    g1.relay(1)
    g1.far()
    r_o.step()
    g1.halves(-1)
    qkv_group(-1)
    g1.halves(1)
    qkv_group(1)
    pass_detour(0)
    g1.relay(2)
    r_o.step2()
    pass_detour(-1)
    g1.halves(2)
    qkv_group(2)
    pass_detour(1)

    block = min(seq, 128)
    sends = []
    for s in range(spd):
        view = x2.at[pl.ds(s * tx_count, tx_count), :, pl.ds(c3, c3)]
        remote(view, view, qkv_s, qkv_r.at[s], {"tx": me_tx}).wait_recv()

        @pl.loop(0, heads)
        def _(hd):
            def part(which):
                return x2[pl.ds(s * tx_count, tx_count), :, col(c3 + which * hc + hd * HEAD_DIM, HEAD_DIM)].reshape(seq, HEAD_DIM)

            for which in (0, 1):
                v = part(which).astype(F32)
                rot = v * cos_ref[...] + pltpu.roll(v, HEAD_DIM // 2, 1) * sin_ref[...]
                kv[which] = rot.astype(BF16)
            kv[2] = part(2)
            for b in range(seq // block):
                keys = (b + 1) * block
                sc = lax.dot_general(kv[0, pl.ds(b * block, block)], kv[1, pl.ds(0, keys)], (((1,), (1,)), ((), ())), preferred_element_type=F32)
                sc = sc * HEAD_DIM ** -0.5
                q_pos = b * block + lax.broadcasted_iota(jnp.int32, (block, keys), 0)
                k_pos = lax.broadcasted_iota(jnp.int32, (block, keys), 1)
                sc = jnp.where(q_pos >= k_pos, sc, -1e30)
                e = jnp.exp(sc - jnp.max(sc, axis=-1, keepdims=True))
                prob = (e / jnp.sum(e, axis=-1, keepdims=True)).astype(BF16)
                o = jnp.dot(prob, kv[2, pl.ds(0, keys)], preferred_element_type=F32).astype(BF16)
                for n in range(block // tok):
                    at = (b * (block // tok) + n) * spd + s
                    x2[at, :, col(2 * c3 + hd * HEAD_DIM, HEAD_DIM)] = o[n * tok : (n + 1) * tok]

        oe = exchange(
            1 + s,
            lambda p, s=s: x2.at[p * spd + s, :, pl.ds(2 * c3, hc)],
            lambda o, s=s: x2.at[o * spd + s, :, pl.ds(2 * c3 + hc, hc)],
            lambda n: x2.at[pl.ds(0, n), :, pl.ds(2 * c3, hc)],
        )
        oe.start()
        sends.append(oe)

    g1.drain()
    drain_detours()
    view = x2.at[pl.ds(0, (tx_count - 1) * spd), :, pl.ds(0, c3)]
    remote(view, view, qkv_s, qkv_r.at[0], {"tx": me_tx}).wait_send()
    for oe in sends:
        oe.wait()
        oe.drain()
    r_gate.start(place=False)
    r_up.start(place=False)
    r_down.start()
    r_o.finish()

    def put(off, x, out):
        for c, s, at in pieces(off):
            xp[s, pl.ds(c * q2, q2), col(x * dx, dx)] = out[at : at + q2]

    def o_group(off):
        stage(x2, off, os_, pl.ds(2 * c3 + hc, hc))

        @pl.loop(0, tx_count)
        def _(x):
            put(off, x, jnp.dot(os_[...], wo[x], preferred_element_type=F32).astype(BF16))

    order = (2, -1, 1, 0)
    sc1 = Scatter(tor, xp, rs_bufs, order)
    o_group(order[0])
    sc1.issue(0)
    o_group(order[1])
    sc1.issue(1)
    o_group(order[2])
    sc1.augment(0)
    sc1.issue(2)
    o_group(order[3])
    sc1.augment(1)
    sc1.issue(3)
    sc1.arrived(0)
    r_gate.step()
    sc1.augment(2)
    sc1.arrived(1)
    sc1.augment2(-1)
    sc1.augment(3)
    sc1.arrived(2)
    sc1.augment2(1)
    r_up.step()
    sc1.arrived(3)
    sc1.last()
    sc1.finish(xt, h)
    norm_rows(h, x2.at[tor.me])
    g2 = Gather(tor, x2, gs, gr)
    g2.start()
    sc1.drain()

    def mlp_group(off, between):
        stage(x2, off, xs, pl.ds(0, d))
        width = 256 if fp % 256 == 0 else 128

        @pl.loop(0, fp // width)
        def _(n):
            cols = col(n * width, width)
            gate = jnp.dot(xs[...], wg[:, :, cols].reshape(d, width), preferred_element_type=F32).astype(BF16).astype(F32)
            up = jnp.dot(xs[...], wu[:, :, cols].reshape(d, width), preferred_element_type=F32).astype(BF16).astype(F32)
            act[:, cols] = (gate * jax.nn.sigmoid(gate) * up).astype(BF16)

        between()

        @pl.loop(0, tx_count)
        def _(x):
            put(off, x, jnp.dot(act[...], wd[x], preferred_element_type=F32).astype(BF16))

    sc2 = Scatter(tor, xp, rs_bufs, (-1, 1, 2, 0))
    g2.near()
    r_down.step()
    g2.relay(0)
    g2.spread(-1)
    g2.spread(1)
    r_gate.step2()
    r_up.step2()
    g2.halves(0)
    r_gate.finish(place=False)
    r_up.finish(place=False)

    def rest():
        g2.relay(-1)
        g2.far()
        r_down.step2()
        r_down.finish()

    mlp_group(0, rest)
    g2.relay(1)
    g2.halves(-1)
    mlp_group(-1, lambda: g2.relay(2))
    sc2.issue(0)
    g2.halves(1)
    mlp_group(1, lambda: None)
    sc2.issue(1)
    g2.halves(2)
    mlp_group(2, lambda: None)
    sc2.issue(2)
    sc2.augment(0)
    sc2.augment(1)
    sc2.issue(3)
    sc2.arrived(0)
    sc2.augment(2)
    sc2.arrived(1)
    sc2.arrived(2)
    sc2.augment(3)
    sc2.augment2(-1)
    sc2.augment2(1)
    sc2.arrived(3)
    sc2.last()
    sc2.finish(h, xt)
    ye = exchange(
        1 + spd,
        lambda p: xt.at[:, col(p * dx, dx)],
        lambda o: yr.at[pl.ds(pl.multiple_of(o * tok, tok), tok)],
        lambda n: yr.at[pl.ds(0, n * tok)],
    )
    ye.start()
    g2.drain()
    sc2.drain()
    for r in rings + [r_o, r_gate, r_up, r_down]:
        r.drain()
    ye.wait()
    out = pltpu.make_async_copy(yr, y_ref, load_sem.at[0])
    out.start()
    ye.drain()
    out.wait()


ANY_SPEC = pl.BlockSpec(memory_space=pl.ANY)


def rotary_tables(seq_len):
    half = HEAD_DIM // 2
    inv_freq = (THETA ** (-2.0 * np.arange(half) / HEAD_DIM)).astype(np.float32)
    angles = np.arange(seq_len, dtype=np.float32)[:, None] * inv_freq[None, :]
    cos_t, sin_t = np.cos(angles), np.sin(angles)
    return np.concatenate([cos_t, cos_t], -1), np.concatenate([-sin_t, sin_t], -1)


def solution(mesh):
    tx_count, n_dev = mesh.shape["tx"], mesh.shape["ty"]
    act_spec = P(("dp", "ty"), None, "tx")
    col_spec = P("tx", "ty")
    row_spec = P("ty", "tx")
    dma = pltpu.SemaphoreType.DMA

    def layer_fn(x_blk, w_q, w_k, w_v, w_o, w_gate, w_up, w_down):
        seq, dx = x_blk.shape[1:]
        hc, f = w_q.shape[1], w_gate.shape[1]
        tok, d = seq // tx_count, dx * tx_count
        fp = -(-f // 128) * 128
        rows, spd = 4 * tok, n_dev // tx_count
        cos_t, sin_t = rotary_tables(seq)
        bf = lambda *shape: pltpu.VMEM(shape, BF16)
        scratch = [
            bf(n_dev, tok, d), bf(n_dev, tok, d), bf(tx_count, dx, 3 * hc), bf(tx_count, hc, dx),
            bf(tx_count, dx, fp), bf(tx_count, dx, fp), bf(tx_count, fp, dx),
            bf(rows, d), bf(rows, hc), bf(rows, fp), bf(3, seq, HEAD_DIM), bf(tok, d), bf(tok, d), bf(seq, dx),
            pltpu.VMEM((seq, HEAD_DIM), F32), pltpu.VMEM((seq, HEAD_DIM), F32),
            dma((5,)), dma((spd + 2,)), dma((spd + 2,)), dma, dma((spd,)), dma, dma((6,)),
            dma, dma((Gather.SEMS,)), dma((7,)), dma((7, Ring.SEMS)),
        ] + Scatter.buffers(tok, d)
        y = pl.pallas_call(
            functools.partial(layer_kernel, tx_count),
            name="layer",
            out_shape=jax.ShapeDtypeStruct((seq, dx), BF16),
            in_specs=[ANY_SPEC] * 10,
            out_specs=ANY_SPEC,
            scratch_shapes=scratch,
            compiler_params=pltpu.CompilerParams(collective_id=1, has_side_effects=True, vmem_limit_bytes=67043328),
        )(x_blk[0], w_q, w_k, w_v, w_o, w_gate.T, w_up.T, w_down, cos_t, sin_t)
        return y[None]

    return jax.shard_map(layer_fn, mesh=mesh, in_specs=(act_spec, col_spec, col_spec, col_spec, row_spec, col_spec, col_spec, row_spec), out_specs=act_spec, check_vma=False)
```

```python
import functools

import numpy as np
import jax
import jax.numpy as jnp
from jax import lax
from jax.experimental import pallas as pl
from jax.experimental.pallas import tpu as pltpu
from jax.sharding import PartitionSpec as P

HEAD_DIM = 128
EPS = 1e-5
THETA = 10000.0
RING = 4
BOTH = (0, 1)
DIRS = (1, -1)
MESH = pl.DeviceIdType.MESH
BF16 = jnp.bfloat16
F32 = jnp.float32
AWAY = (0, -1, 1, 2)


def nothing():
    pass


def wrap(v, n):
    return lax.rem(v + 2 * n, n)


class Torus:
    def __init__(self):
        t = lax.axis_index("ty")
        self.me = t
        self.pos = (lax.div(t, RING), lax.rem(t, RING))

    def slot(self, first, a_off, b_off):
        a = wrap(self.pos[first] + a_off, RING)
        b = wrap(self.pos[1 - first] + b_off, RING)
        return a * RING + b if first == 0 else b * RING + a


def entry_barrier(tor, tx_count):
    sem = pltpu.get_barrier_semaphore()
    for first in (0, 1):
        for d in DIRS:
            pl.semaphore_signal(sem, inc=1, device_id={"ty": tor.slot(first, d, 0)}, device_id_type=MESH)
    me = lax.axis_index("tx")
    for k in range(1, tx_count):
        pl.semaphore_signal(sem, inc=1, device_id={"tx": lax.rem(me + k, tx_count)}, device_id_type=MESH)
    pl.semaphore_wait(sem, 4 + tx_count - 1)


def remote(src, dst, ssem, rsem, device):
    return pltpu.make_async_remote_copy(src_ref=src, dst_ref=dst, send_sem=ssem, recv_sem=rsem, device_id=device, device_id_type=MESH)


class Gather:
    SEMS = 25

    def __init__(self, tor, buf, ssem, rsem):
        self.tor, self.buf, self.ssem, self.rsem = tor, buf, ssem, rsem
        self.q = buf.shape[1] // 4

    def first(self, c):
        return 1 if c == 0 else 0

    def rows(self, c, d, half):
        if not half:
            return pl.ds(c * 2 * self.q, 2 * self.q)
        return pl.ds(c * 2 * self.q + (0 if d == 1 else self.q), self.q)

    def sem(self, c, ph, off, d, half):
        if half:
            return 20 + (0 if ph == 1 else 1 + AWAY.index(off))
        return (0 if ph == 1 else 4 + 4 * AWAY.index(off)) + c * 2 + (0 if d == 1 else 1)

    def copy(self, c, ph, off, d, half, hops):
        first = self.first(c)
        back = -d * hops
        s = self.tor.slot(first, back, 0) if ph == 1 else self.tor.slot(first, off, back)
        to = self.tor.slot(first, d, 0) if ph == 1 else self.tor.slot(first, 0, d)
        view = self.buf.at[s, self.rows(c, d, half)]
        return remote(view, view, self.ssem, self.rsem.at[self.sem(c, ph, off, d, half)], {"ty": to})

    def send(self, c, ph, off, d, half=False):
        self.copy(c, ph, off, d, half, 1 if half else 0).start()

    def recv(self, c, ph, off, d):
        self.copy(c, ph, off, d, False, 1).wait_recv()

    def recv_halves(self, ph, off):
        view = self.buf.at[0]
        remote(view, view, self.ssem, self.rsem.at[self.sem(0, ph, off, 1, True)], {"ty": self.tor.me}).wait_recv()

    def start(self):
        for ph in (1, 2):
            for c in BOTH:
                for d in DIRS:
                    self.send(c, ph, 0, d)

    def near(self):
        for d in DIRS:
            for c in BOTH:
                self.recv(c, 1, 0, d)
                self.send(c, 1, 0, d, True)

    def spread(self, off):
        for c in BOTH:
            for d in DIRS:
                self.send(c, 2, off, d)

    def relay(self, off):
        for d in DIRS:
            for c in BOTH:
                self.recv(c, 2, off, d)
                self.send(c, 2, off, d, True)

    def far(self):
        self.recv_halves(1, 0)
        self.spread(2)

    def halves(self, off):
        self.recv_halves(2, off)

    def drain(self):
        view = self.buf.at[pl.ds(0, self.buf.shape[0] - 1)]
        remote(view, view, self.ssem, self.rsem.at[0], {"ty": self.tor.me}).wait_send()


def add_rows(dst, srcs, width=512):
    d = dst.shape[-1]
    width = min(width, d)

    @pl.loop(0, d // width)
    def _(i):
        cols = pl.ds(pl.multiple_of(i * width, width), width)
        tot = srcs[0][:, cols].astype(F32)
        for s in srcs[1:]:
            tot += s[:, cols].astype(F32)
        dst[:, cols] = tot.astype(dst.dtype)


class Scatter:
    SEMS = 30

    @staticmethod
    def buffers(tok, d):
        q = tok // 4
        return [
            pltpu.VMEM((2, 4, 2, q, d), BF16),
            pltpu.VMEM((2, 4, 2, 2 * q, d), BF16),
            pltpu.VMEM((2, 3, 2 * q, d), BF16),
            pltpu.VMEM((2, 2, q, d), BF16),
            pltpu.VMEM((2, 2, 2 * q, d), BF16),
            pltpu.SemaphoreType.DMA,
            pltpu.SemaphoreType.DMA((Scatter.SEMS,)),
        ]

    def __init__(self, tor, part, bufs, order):
        self.tor, self.part, self.order = tor, part, order
        self.h1, self.f1, self.mid, self.h2, self.f2, self.ssem, self.rsem = bufs
        self.q = part.shape[1] // 4

    def copy(self, c, ph, bi, d, kind):
        q, first = self.q, c
        di = 0 if d == 1 else 1
        h = di if kind in (0, 2) else 1 - di
        step = 2 * d if kind == 0 else d
        if ph == 1:
            i = c * 8 + bi * 2 + di if kind == 0 else 16 + c * 4 + bi
            src = self.part.at[self.tor.slot(first, step, self.order[bi]), pl.ds(c * 2 * q + h * q, q)]
            dst = self.h1.at[c, bi, di] if kind == 0 else self.f1.at[c, bi, di, pl.ds(h * q, q)]
            to = self.tor.slot(first, d, 0)
        else:
            i = 24 + c * 2 + di if kind == 0 else 28 + c
            src = self.mid.at[c, self.order.index(2 if kind == 0 else d), pl.ds(h * q, q)]
            dst = self.h2.at[c, di] if kind == 0 else self.f2.at[c, di, pl.ds(h * q, q)]
            to = self.tor.slot(first, 0, d)
        return remote(src, dst, self.ssem, self.rsem.at[i], {"ty": to})

    def all_of(self, view, i):
        remote(view, view, self.ssem, self.rsem.at[i], {"ty": self.tor.me}).wait_recv()

    def issue(self, bi):
        for kind in BOTH:
            for c in BOTH:
                for d in DIRS:
                    self.copy(c, 1, bi, d, kind).start()

    def augment(self, bi):
        q = self.q
        for c in BOTH:
            for d in DIRS:
                di = 0 if d == 1 else 1
                self.copy(c, 1, bi, d, 0).wait_recv()
                mine = self.part.at[self.tor.slot(c, d, self.order[bi]), pl.ds(c * 2 * q + di * q, q)]
                add_rows(mine, [mine, self.h1.at[c, bi, di]])
                self.copy(c, 1, bi, d, 2).start()

    def arrived(self, bi):
        q = self.q
        for c in BOTH:
            self.all_of(self.f1.at[c, bi], 16 + c * 4 + bi)
            off = self.order[bi]
            if off == 0:
                continue
            own = self.part.at[self.tor.slot(c, 0, off), pl.ds(c * 2 * q, 2 * q)]
            add_rows(self.mid.at[c, bi], [own, self.f1.at[c, bi, 0], self.f1.at[c, bi, 1]])
            if off == 2:
                for d in DIRS:
                    self.copy(c, 2, 0, d, 0).start()
            else:
                self.copy(c, 2, 0, off, 1).start()

    def augment2(self, d):
        q = self.q
        di = 0 if d == 1 else 1
        for c in BOTH:
            self.copy(c, 2, 0, d, 0).wait_recv()
            mine = self.mid.at[c, self.order.index(d), pl.ds(di * q, q)]
            add_rows(mine, [mine, self.h2.at[c, di]])
            self.copy(c, 2, 0, d, 2).start()

    def last(self):
        for c in BOTH:
            self.all_of(self.f2.at[c], 28 + c)

    def finish(self, resid, out):
        q, d = self.q, out.shape[-1]
        width = min(512, d)
        for c in BOTH:
            rows = pl.ds(c * 2 * q, 2 * q)

            @pl.loop(0, d // width)
            def _(i):
                cols = pl.ds(pl.multiple_of(i * width, width), width)
                tot = self.part[self.tor.me, rows, cols].astype(F32)
                for di in BOTH:
                    tot += self.f1[c, self.order.index(0), di, :, cols].astype(F32)
                for di in BOTH:
                    tot += self.f2[c, di, :, cols].astype(F32)
                tot = tot.astype(BF16).astype(F32)
                out[rows, cols] = (resid[rows, cols].astype(F32) + tot).astype(BF16)

    def drain(self):
        view = self.part.at[pl.ds(0, self.part.shape[0] - 1)]
        remote(view, view, self.ssem, self.rsem.at[0], {"ty": self.tor.me}).wait_send()


class Exchange:
    def __init__(self, tx_count, src, dst, whole, ssem, rsem):
        self.n, self.src, self.dst, self.whole, self.ssem, self.rsem = tx_count, src, dst, whole, ssem, rsem
        self.me = lax.axis_index("tx")

    def start(self):
        for k in range(1, self.n):
            p = lax.rem(self.me + k, self.n)
            remote(self.src(p), self.dst(self.me), self.ssem, self.rsem, {"tx": p}).start()
        pltpu.make_async_copy(self.src(self.me), self.dst(self.me), self.rsem).start()

    def wait(self):
        view = self.whole(self.n)
        remote(view, view, self.ssem, self.rsem, {"tx": self.me}).wait_recv()

    def drain(self):
        view = self.whole(self.n - 1)
        remote(view, view, self.ssem, self.rsem, {"tx": self.me}).wait_send()


def norm_rows(src, dst):
    tok, d = src.shape
    step = 16

    @pl.loop(0, tok // step)
    def _(i):
        rows = pl.ds(pl.multiple_of(i * step, step), step)
        v = src[rows, :].astype(F32)
        mean = jnp.sum(v, axis=-1, keepdims=True) * (1.0 / d)
        var = jnp.sum(v * v, axis=-1, keepdims=True) * (1.0 / d) - mean * mean
        dst[rows, :] = ((v - mean) * lax.rsqrt(var + EPS)).astype(BF16)


class Ring:
    SEMS = 5

    def __init__(self, tx_count, rows, src, slot, whole, ssem, rsem):
        self.nx, self.rows, self.src, self.slot, self.whole, self.ssem, self.rsem = tx_count // 2, rows, src, slot, whole, ssem, rsem
        me = lax.axis_index("tx")
        self.me, self.x, self.core = me, lax.div(me, 2), lax.rem(me, 2)
        self.split = (rows // 2 + 15) // 16 * 16

    def tx(self, dx, other=False):
        return wrap(self.x + dx, self.nx) * 2 + (1 - self.core if other else self.core)

    def half(self, view, d):
        return view.at[pl.ds(0, self.split)] if d == 1 else view.at[pl.ds(self.split, self.rows - self.split)]

    def copy(self, i, src, dst, to):
        return remote(src, dst, self.ssem, self.rsem.at[i], {"tx": to})

    def pass_on(self, d, recv=False):
        view = self.slot(self.tx(-d if recv else 0))
        return self.copy(0 if d == 1 else 1, view if recv else self.src, view, self.tx(d))

    def relay(self, d, recv=False):
        view = self.half(self.slot(self.tx(-2 * d if recv else -d)), d)
        return self.copy(2 if d == 1 else 3, view, view, self.tx(d))

    def across(self, which, recv=False):
        view = self.slot(self.tx(which, recv))
        if abs(which) == 2:
            view = self.half(view, which // 2)
        src = self.src if which == 0 and not recv else view
        return self.copy(4, src, view, self.tx(0, True))

    def all_across(self):
        return (0, 1, -1, 2, -2) if self.nx > 1 else (0,)

    def own(self):
        return pltpu.make_async_copy(self.src, self.slot(self.me), self.rsem.at[4])

    def start(self, place=True):
        if self.nx > 1:
            for d in DIRS:
                self.pass_on(d).start()
        self.across(0).start()
        if place:
            self.own().start()

    def step(self):
        if self.nx > 1:
            for d in DIRS:
                self.pass_on(d, True).wait_recv()
                self.relay(d).start()
                self.across(-d).start()

    def step2(self):
        if self.nx > 1:
            for d in DIRS:
                self.relay(d, True).wait_recv()
                self.across(2 * d).start()

    def finish(self, place=True):
        view = self.whole(self.nx + (1 if place else 0))
        remote(view, view, self.ssem, self.rsem.at[4], {"tx": self.me}).wait_recv()

    def drain(self):
        view = self.whole(2 * self.nx - 1)
        remote(view, view, self.ssem, self.rsem.at[4], {"tx": self.me}).wait_send()


def layer_kernel(tx_count, x_ref, wq_ref, wk_ref, wv_ref, wo_ref, wg_ref, wu_ref, wd_ref, cos_hbm, sin_hbm, y_ref,
                 xp, x2, wqkv, wo, wg, wu, wd, xs, os_, act, kv, xt, h, yr, cos_ref, sin_ref,
                 load_sem, a2a_s, a2a_r, qkv_s, qkv_r, via_s, via_r, gs, gr, ws, wr, *rs_bufs):
    n_dev, tok, d = xp.shape
    dx = x_ref.shape[1]
    hc = wq_ref.shape[1]
    f, fp = wg_ref.shape[0], wg.shape[2]
    seq = tok * tx_count
    spd = n_dev // tx_count
    heads = hc // HEAD_DIM
    q2 = tok // 2
    c3 = 3 * hc
    tor = Torus()
    me_tx = lax.axis_index("tx")

    def exchange(i, src, dst, whole):
        return Exchange(tx_count, src, dst, whole, a2a_s.at[i], a2a_r.at[i])

    def col(start, width):
        return pl.ds(pl.multiple_of(start, width), width)

    def ring(i, src, buf, inner):
        return Ring(tx_count, src.shape[0], src, lambda o: buf.at[(o, *inner)], lambda n: buf.at[(pl.ds(0, n), *inner)], ws.at[i], wr.at[i])

    every = pl.ds(0, dx)
    rings = [ring(i, src, wqkv, (every, pl.ds(i * hc, hc))) for i, src in enumerate((wq_ref, wk_ref, wv_ref))]
    r_o = ring(3, wo_ref, wo, ())
    r_gate = ring(4, wg.at[me_tx], wg, ())
    r_up = ring(5, wu.at[me_tx], wu, ())
    r_down = ring(6, wd_ref, wd, (pl.ds(0, f),))

    x_in = pltpu.make_async_copy(x_ref, yr, load_sem.at[2])
    x_in.start()
    raw = [pltpu.make_async_copy(src, wd.at[i, pl.ds(0, f)], load_sem.at[i]) for i, src in enumerate((wg_ref, wu_ref))]
    raw += [pltpu.make_async_copy(cos_hbm, cos_ref, load_sem.at[3]), pltpu.make_async_copy(sin_hbm, sin_ref, load_sem.at[4])]
    for cp in raw:
        cp.start()
    entry_barrier(tor, tx_count)
    x_in.wait()
    xe = exchange(
        0,
        lambda p: yr.at[pl.ds(pl.multiple_of(p * tok, tok), tok)],
        lambda o: xt.at[:, col(o * dx, dx)],
        lambda n: yr.at[pl.ds(0, n * tok)],
    )
    xe.start()
    if fp > f:
        wd[:, pl.ds(f, fp - f), :] = jnp.zeros((tx_count, fp - f, dx), BF16)
    xe.wait()
    norm_rows(xt, xp.at[tor.me])
    g1 = Gather(tor, xp, gs, gr)
    g1.start()
    for r in rings:
        r.start()
    for cp in raw:
        cp.wait()
    for i, dst in enumerate((wg, wu)):
        for j in range(fp // 128):
            dst[me_tx, :, pl.ds(j * 128, 128)] = wd[i, pl.ds(j * 128, 128), :].T

    def pieces(off):
        return [(c, tor.slot(1 - c, off, n), (c * 4 + n) * q2) for c in BOTH for n in range(RING)]

    def stage(src, off, dst, cols):
        for c, s, at in pieces(off):
            dst[pl.ds(at, q2), :] = src[s, pl.ds(c * q2, q2), cols]

    detours = tx_count == 8
    x_pos = lax.div(me_tx, 2)
    edge = (x_pos == 0) | (x_pos == 3)
    opposite = jnp.where(x_pos == 0, 2, 1)
    inner = jnp.where(x_pos == 0, 1, 2)
    over = (3 - x_pos) * 2 + lax.rem(me_tx, 2)
    via = pl.ds(2 * c3 + 2 * hc, c3)

    def qkv_group(off):
        stage(xp, off, xs, pl.ds(0, d))

        @pl.loop(0, 3)
        def _(n):
            cols = col(n * hc, hc)
            out = jnp.dot(xs[...], wqkv[:, :, cols].reshape(d, hc), preferred_element_type=F32).astype(BF16)
            for c, s, at in pieces(off):
                x2[s, pl.ds(c * q2, q2), cols] = out[at : at + q2]

        for c, s, _ in pieces(off):
            p, sl = lax.div(s, spd), lax.rem(s, spd)
            rows = pl.ds(c * q2, q2)
            src = x2.at[s, rows, pl.ds(0, c3)]
            dst = x2.at[sl * tx_count + me_tx, rows, pl.ds(c3, c3)]

            detour = (p != p) if off > 0 or not detours else edge & (lax.div(p, 2) == opposite)

            @pl.when(p == me_tx)
            def _():
                pltpu.make_async_copy(src, dst, qkv_r.at[sl]).start()

            @pl.when(detour)
            def _():
                remote(src, x2.at[s, rows, via], qkv_s, via_r.at[2 * AWAY.index(off) + c], {"tx": over}).start()

            @pl.when((p != me_tx) & jnp.logical_not(detour))
            def _():
                remote(src, dst, qkv_s, qkv_r.at[sl], {"tx": p}).start()

    def detour_rows(off, c):
        rows = pl.ds(c * q2, q2)
        return [(s, rows) for s in ([inner * RING + wrap(tor.pos[1] + off, RING)] if c == 0 else [inner * RING + y for y in range(RING)])]

    def pass_detour(off):
        if not detours:
            return
        for c in BOTH:

            @pl.when(edge if c == 0 else edge & (wrap(tor.pos[0] + off, RING) == inner))
            def _():
                for s, rows in detour_rows(off, c):
                    view = x2.at[s, rows, via]
                    if c == 0:
                        remote(view, view, via_s, via_r.at[2 * AWAY.index(off) + c], {"tx": me_tx}).wait_recv()
                if c == 1:
                    view = x2.at[pl.ds(inner * RING, 2), :, via]
                    remote(view, view, via_s, via_r.at[2 * AWAY.index(off) + c], {"tx": me_tx}).wait_recv()
                for s, rows in detour_rows(off, c):
                    p, sl = lax.div(s, spd), lax.rem(s, spd)
                    remote(x2.at[s, rows, via], x2.at[sl * tx_count + over, rows, pl.ds(c3, c3)], via_s, qkv_r.at[sl], {"tx": p}).start()

    def drain_detours():
        if not detours:
            return
        for off in (0, -1):
            for c in BOTH:

                @pl.when(edge if c == 0 else edge & (wrap(tor.pos[0] + off, RING) == inner))
                def _():
                    view = x2.at[0, pl.ds(0, q2), via] if c == 0 else x2.at[pl.ds(0, 2), :, via]
                    remote(view, view, via_s, via_r.at[0], {"tx": me_tx}).wait_send()

    xe.drain()
    wq_r, wk_r, wv_r = rings
    g1.near()
    wq_r.step()
    g1.relay(0)
    g1.spread(-1)
    g1.spread(1)
    wk_r.step()
    wv_r.step()
    g1.halves(0)
    wq_r.step2()
    wk_r.step2()
    g1.relay(-1)
    wv_r.step2()
    for r in rings:
        r.finish()
    qkv_group(0)
    g1.relay(1)
    g1.far()
    g1.halves(-1)
    qkv_group(-1)
    g1.halves(1)
    qkv_group(1)
    pass_detour(0)
    g1.relay(2)
    g1.halves(2)
    qkv_group(2)
    pass_detour(-1)
    r_o.start()

    block = min(seq, 128)
    sends = []
    for s in range(spd):
        view = x2.at[pl.ds(s * tx_count, tx_count), :, pl.ds(c3, c3)]
        remote(view, view, qkv_s, qkv_r.at[s], {"tx": me_tx}).wait_recv()

        @pl.loop(0, heads)
        def _(hd):
            def part(which):
                return x2[pl.ds(s * tx_count, tx_count), :, col(c3 + which * hc + hd * HEAD_DIM, HEAD_DIM)].reshape(seq, HEAD_DIM)

            for which in BOTH:
                v = part(which).astype(F32)
                rot = v * cos_ref[...] + pltpu.roll(v, HEAD_DIM // 2, 1) * sin_ref[...]
                kv[which] = rot.astype(BF16)
            kv[2] = part(2)
            for b in range(seq // block):
                keys = (b + 1) * block
                sc = lax.dot_general(kv[0, pl.ds(b * block, block)], kv[1, pl.ds(0, keys)], (((1,), (1,)), ((), ())), preferred_element_type=F32)
                sc = sc * HEAD_DIM ** -0.5
                q_pos = b * block + lax.broadcasted_iota(jnp.int32, (block, keys), 0)
                k_pos = lax.broadcasted_iota(jnp.int32, (block, keys), 1)
                sc = jnp.where(q_pos >= k_pos, sc, -1e30)
                e = jnp.exp(sc - jnp.max(sc, axis=-1, keepdims=True))
                prob = (e / jnp.sum(e, axis=-1, keepdims=True)).astype(BF16)
                o = jnp.dot(prob, kv[2, pl.ds(0, keys)], preferred_element_type=F32).astype(BF16)
                for n in range(block // tok):
                    at = (b * (block // tok) + n) * spd + s
                    x2[at, :, col(2 * c3 + hd * HEAD_DIM, HEAD_DIM)] = o[n * tok : (n + 1) * tok]

        oe = exchange(
            1 + s,
            lambda p, s=s: x2.at[p * spd + s, :, pl.ds(2 * c3, hc)],
            lambda o, s=s: x2.at[o * spd + s, :, pl.ds(2 * c3 + hc, hc)],
            lambda n: x2.at[pl.ds(0, n), :, pl.ds(2 * c3, hc)],
        )
        oe.start()
        sends.append(oe)

    r_o.step()
    g1.drain()
    drain_detours()
    view = x2.at[pl.ds(0, (tx_count - 1) * spd), :, pl.ds(0, c3)]
    remote(view, view, qkv_s, qkv_r.at[0], {"tx": me_tx}).wait_send()
    for oe in sends:
        oe.wait()
        oe.drain()
    r_o.step2()
    r_gate.start(place=False)
    r_up.start(place=False)
    r_down.start()
    r_o.finish()

    def put(off, x, out):
        for c, s, at in pieces(off):
            xp[s, pl.ds(c * q2, q2), col(x * dx, dx)] = out[at : at + q2]

    def o_group(off):
        stage(x2, off, os_, pl.ds(2 * c3 + hc, hc))

        @pl.loop(0, tx_count)
        def _(x):
            put(off, x, jnp.dot(os_[...], wo[x], preferred_element_type=F32).astype(BF16))

    order = (2, -1, 1, 0)
    sc1 = Scatter(tor, xp, rs_bufs, order)
    o_group(order[0])
    sc1.issue(0)
    o_group(order[1])
    sc1.issue(1)
    o_group(order[2])
    sc1.augment(0)
    sc1.issue(2)
    o_group(order[3])
    sc1.augment(1)
    sc1.issue(3)
    sc1.arrived(0)
    r_gate.step()
    sc1.augment(2)
    sc1.arrived(1)
    sc1.augment2(-1)
    sc1.augment(3)
    sc1.arrived(2)
    sc1.augment2(1)
    r_up.step()
    sc1.arrived(3)
    sc1.last()
    sc1.finish(xt, h)
    norm_rows(h, x2.at[tor.me])
    g2 = Gather(tor, x2, gs, gr)
    g2.start()
    sc1.drain()

    def mlp_group(off, between, mid):
        stage(x2, off, xs, pl.ds(0, d))
        width = 256 if fp % 256 == 0 else 128

        @pl.loop(0, fp // width)
        def _(n):
            cols = col(n * width, width)
            gate = jnp.dot(xs[...], wg[:, :, cols].reshape(d, width), preferred_element_type=F32).astype(BF16).astype(F32)
            up = jnp.dot(xs[...], wu[:, :, cols].reshape(d, width), preferred_element_type=F32).astype(BF16).astype(F32)
            act[:, cols] = (gate * jax.nn.sigmoid(gate) * up).astype(BF16)

        between()
        half = tx_count // 2
        for lo, then in ((0, mid), (half, nothing)):

            @pl.loop(lo, lo + half)
            def _(x):
                put(off, x, jnp.dot(act[...], wd[x], preferred_element_type=F32).astype(BF16))

            then()

    sc2 = Scatter(tor, xp, rs_bufs, (-1, 1, 2, 0))
    g2.near()
    r_down.step()
    g2.relay(0)
    g2.spread(-1)
    g2.spread(1)
    r_gate.step2()
    r_up.step2()
    g2.halves(0)
    r_gate.finish(place=False)
    r_up.finish(place=False)

    def weights_in():
        r_down.step2()
        r_down.finish()

    def onward():
        g2.relay(-1)
        g2.far()

    mlp_group(0, weights_in, onward)
    g2.relay(1)
    g2.halves(-1)
    mlp_group(-1, nothing, lambda: g2.relay(2))
    sc2.issue(0)
    g2.halves(1)
    mlp_group(1, nothing, nothing)
    sc2.issue(1)
    g2.halves(2)
    mlp_group(2, nothing, nothing)
    sc2.issue(2)
    sc2.augment(0)
    sc2.augment(1)
    sc2.issue(3)
    sc2.arrived(0)
    sc2.augment(2)
    sc2.arrived(1)
    sc2.arrived(2)
    sc2.augment(3)
    sc2.augment2(-1)
    sc2.augment2(1)
    sc2.arrived(3)
    sc2.last()
    sc2.finish(h, xt)
    ye = exchange(
        1 + spd,
        lambda p: xt.at[:, col(p * dx, dx)],
        lambda o: yr.at[pl.ds(pl.multiple_of(o * tok, tok), tok)],
        lambda n: yr.at[pl.ds(0, n * tok)],
    )
    ye.start()
    g2.drain()
    sc2.drain()
    for r in rings + [r_o, r_gate, r_up, r_down]:
        r.drain()
    ye.wait()
    out = pltpu.make_async_copy(yr, y_ref, load_sem.at[0])
    out.start()
    ye.drain()
    out.wait()


ANY_SPEC = pl.BlockSpec(memory_space=pl.ANY)


def rotary_tables(seq_len):
    half = HEAD_DIM // 2
    inv_freq = (THETA ** (-2.0 * np.arange(half) / HEAD_DIM)).astype(np.float32)
    angles = np.arange(seq_len, dtype=np.float32)[:, None] * inv_freq[None, :]
    cos_t, sin_t = np.cos(angles), np.sin(angles)
    return np.concatenate([cos_t, cos_t], -1), np.concatenate([-sin_t, sin_t], -1)


def solution(mesh):
    tx_count, n_dev = mesh.shape["tx"], mesh.shape["ty"]
    act_spec = P(("dp", "ty"), None, "tx")
    col_spec = P("tx", "ty")
    row_spec = P("ty", "tx")
    dma = pltpu.SemaphoreType.DMA

    def layer_fn(x_blk, w_q, w_k, w_v, w_o, w_gate, w_up, w_down):
        seq, dx = x_blk.shape[1:]
        hc, f = w_q.shape[1], w_gate.shape[1]
        tok, d = seq // tx_count, dx * tx_count
        fp = -(-f // 128) * 128
        rows, spd = 4 * tok, n_dev // tx_count
        cos_t, sin_t = rotary_tables(seq)
        bf = lambda *shape: pltpu.VMEM(shape, BF16)
        scratch = [
            bf(n_dev, tok, d), bf(n_dev, tok, d), bf(tx_count, dx, 3 * hc), bf(tx_count, hc, dx),
            bf(tx_count, dx, fp), bf(tx_count, dx, fp), bf(tx_count, fp, dx),
            bf(rows, d), bf(rows, hc), bf(rows, fp), bf(3, seq, HEAD_DIM), bf(tok, d), bf(tok, d), bf(seq, dx),
            pltpu.VMEM((seq, HEAD_DIM), F32), pltpu.VMEM((seq, HEAD_DIM), F32),
            dma((5,)), dma((spd + 2,)), dma((spd + 2,)), dma, dma((spd,)), dma, dma((6,)),
            dma, dma((Gather.SEMS,)), dma((7,)), dma((7, Ring.SEMS)),
        ] + Scatter.buffers(tok, d)
        y = pl.pallas_call(
            functools.partial(layer_kernel, tx_count),
            name="layer",
            out_shape=jax.ShapeDtypeStruct((seq, dx), BF16),
            in_specs=[ANY_SPEC] * 10,
            out_specs=ANY_SPEC,
            scratch_shapes=scratch,
            compiler_params=pltpu.CompilerParams(collective_id=1, has_side_effects=True, vmem_limit_bytes=67043328),
        )(x_blk[0], w_q, w_k, w_v, w_o, w_gate.T, w_up.T, w_down, cos_t, sin_t)
        return y[None]

    return jax.shard_map(layer_fn, mesh=mesh, in_specs=(act_spec, col_spec, col_spec, col_spec, row_spec, col_spec, col_spec, row_spec), out_specs=act_spec, check_vma=False)
```

```python
import functools

import numpy as np
import jax
import jax.numpy as jnp
from jax import lax
from jax.experimental import pallas as pl
from jax.experimental.pallas import tpu as pltpu
from jax.sharding import PartitionSpec as P

HEAD_DIM = 128
EPS = 1e-5
THETA = 10000.0
RING = 4
BOTH = (0, 1)
DIRS = (1, -1)
MESH = pl.DeviceIdType.MESH
BF16 = jnp.bfloat16
F32 = jnp.float32
AWAY = (0, -1, 1, 2)


def nothing():
    pass


def wrap(v, n):
    return lax.rem(v + 2 * n, n)


class Torus:
    def __init__(self):
        t = lax.axis_index("ty")
        self.me = t
        self.pos = (lax.div(t, RING), lax.rem(t, RING))

    def slot(self, first, a_off, b_off):
        a = wrap(self.pos[first] + a_off, RING)
        b = wrap(self.pos[1 - first] + b_off, RING)
        return a * RING + b if first == 0 else b * RING + a


def entry_barrier(tor, tx_count):
    sem = pltpu.get_barrier_semaphore()
    for first in (0, 1):
        for d in DIRS:
            pl.semaphore_signal(sem, inc=1, device_id={"ty": tor.slot(first, d, 0)}, device_id_type=MESH)
    me = lax.axis_index("tx")
    for k in range(1, tx_count):
        pl.semaphore_signal(sem, inc=1, device_id={"tx": lax.rem(me + k, tx_count)}, device_id_type=MESH)
    pl.semaphore_wait(sem, 4 + tx_count - 1)


def remote(src, dst, ssem, rsem, device):
    return pltpu.make_async_remote_copy(src_ref=src, dst_ref=dst, send_sem=ssem, recv_sem=rsem, device_id=device, device_id_type=MESH)


class Gather:
    SEMS = 25

    def __init__(self, tor, buf, ssem, rsem):
        self.tor, self.buf, self.ssem, self.rsem = tor, buf, ssem, rsem
        self.q = buf.shape[1] // 4

    def first(self, c):
        return 1 if c == 0 else 0

    def rows(self, c, d, half):
        if not half:
            return pl.ds(c * 2 * self.q, 2 * self.q)
        return pl.ds(c * 2 * self.q + (0 if d == 1 else self.q), self.q)

    def sem(self, c, ph, off, d, half):
        if half:
            return 20 + (0 if ph == 1 else 1 + AWAY.index(off))
        return (0 if ph == 1 else 4 + 4 * AWAY.index(off)) + c * 2 + (0 if d == 1 else 1)

    def copy(self, c, ph, off, d, half, hops):
        first = self.first(c)
        back = -d * hops
        s = self.tor.slot(first, back, 0) if ph == 1 else self.tor.slot(first, off, back)
        to = self.tor.slot(first, d, 0) if ph == 1 else self.tor.slot(first, 0, d)
        view = self.buf.at[s, self.rows(c, d, half)]
        return remote(view, view, self.ssem, self.rsem.at[self.sem(c, ph, off, d, half)], {"ty": to})

    def send(self, c, ph, off, d, half=False):
        self.copy(c, ph, off, d, half, 1 if half else 0).start()

    def recv(self, c, ph, off, d):
        self.copy(c, ph, off, d, False, 1).wait_recv()

    def far_copy(self, c, d, second, hops):
        s = self.tor.slot(self.first(c), 2, -d * hops)
        view = self.buf.at[s, self.rows(c, -d if second else d, True)]
        i = self.sem(c, 2, 2, d, second)
        return remote(view, view, self.ssem, self.rsem.at[i], {"ty": self.tor.slot(self.first(c), 0, d)})

    def recv_halves(self, ph, off):
        view = self.buf.at[pl.ds(0, 2)] if ph == off == 2 else self.buf.at[0]
        remote(view, view, self.ssem, self.rsem.at[self.sem(0, ph, off, 1, True)], {"ty": self.tor.me}).wait_recv()

    def start(self):
        for ph in (1, 2):
            for c in BOTH:
                for d in DIRS:
                    self.send(c, ph, 0, d)

    def near(self):
        for d in DIRS:
            for c in BOTH:
                self.recv(c, 1, 0, d)
                self.send(c, 1, 0, d, True)

    def spread(self, off):
        for c in BOTH:
            for d in DIRS:
                self.send(c, 2, off, d)

    def relay(self, off):
        for d in DIRS:
            for c in BOTH:
                if off == 2:
                    self.far_copy(c, d, False, 1).wait_recv()
                else:
                    self.recv(c, 2, off, d)
                self.send(c, 2, off, d, True)

    def far(self, second):
        if not second:
            self.recv_halves(1, 0)
        for c in BOTH:
            for d in DIRS:
                self.far_copy(c, d, second, 0).start()

    def halves(self, off):
        self.recv_halves(2, off)

    def drain(self):
        view = self.buf.at[pl.ds(0, self.buf.shape[0] - 1)]
        remote(view, view, self.ssem, self.rsem.at[0], {"ty": self.tor.me}).wait_send()


def add_rows(dst, srcs, width=512):
    d = dst.shape[-1]
    width = min(width, d)

    @pl.loop(0, d // width)
    def _(i):
        cols = pl.ds(pl.multiple_of(i * width, width), width)
        tot = srcs[0][:, cols].astype(F32)
        for s in srcs[1:]:
            tot += s[:, cols].astype(F32)
        dst[:, cols] = tot.astype(dst.dtype)


class Scatter:
    SEMS = 30

    @staticmethod
    def buffers(tok, d):
        q = tok // 4
        return [
            pltpu.VMEM((2, 4, 2, q, d), BF16),
            pltpu.VMEM((2, 4, 2, 2 * q, d), BF16),
            pltpu.VMEM((2, 3, 2 * q, d), BF16),
            pltpu.VMEM((2, 2, q, d), BF16),
            pltpu.VMEM((2, 2, 2 * q, d), BF16),
            pltpu.SemaphoreType.DMA,
            pltpu.SemaphoreType.DMA((Scatter.SEMS,)),
        ]

    def __init__(self, tor, part, bufs, order):
        self.tor, self.part, self.order = tor, part, order
        self.h1, self.f1, self.mid, self.h2, self.f2, self.ssem, self.rsem = bufs
        self.q = part.shape[1] // 4

    def copy(self, c, ph, bi, d, kind):
        q, first = self.q, c
        di = 0 if d == 1 else 1
        h = di if kind in (0, 2) else 1 - di
        step = 2 * d if kind == 0 else d
        if ph == 1:
            i = c * 8 + bi * 2 + di if kind == 0 else 16 + c * 4 + bi
            src = self.part.at[self.tor.slot(first, step, self.order[bi]), pl.ds(c * 2 * q + h * q, q)]
            dst = self.h1.at[c, bi, di] if kind == 0 else self.f1.at[c, bi, di, pl.ds(h * q, q)]
            to = self.tor.slot(first, d, 0)
        else:
            i = 24 + c * 2 + di if kind == 0 else 28 + c
            src = self.mid.at[c, self.order.index(2 if kind == 0 else d), pl.ds(h * q, q)]
            dst = self.h2.at[c, di] if kind == 0 else self.f2.at[c, di, pl.ds(h * q, q)]
            to = self.tor.slot(first, 0, d)
        return remote(src, dst, self.ssem, self.rsem.at[i], {"ty": to})

    def all_of(self, view, i):
        remote(view, view, self.ssem, self.rsem.at[i], {"ty": self.tor.me}).wait_recv()

    def issue(self, bi):
        for kind in BOTH:
            for c in BOTH:
                for d in DIRS:
                    self.copy(c, 1, bi, d, kind).start()

    def augment(self, bi):
        q = self.q
        for c in BOTH:
            for d in DIRS:
                di = 0 if d == 1 else 1
                self.copy(c, 1, bi, d, 0).wait_recv()
                mine = self.part.at[self.tor.slot(c, d, self.order[bi]), pl.ds(c * 2 * q + di * q, q)]
                add_rows(mine, [mine, self.h1.at[c, bi, di]])
                self.copy(c, 1, bi, d, 2).start()

    def arrived(self, bi):
        q = self.q
        for c in BOTH:
            self.all_of(self.f1.at[c, bi], 16 + c * 4 + bi)
            off = self.order[bi]
            if off == 0:
                continue
            own = self.part.at[self.tor.slot(c, 0, off), pl.ds(c * 2 * q, 2 * q)]
            add_rows(self.mid.at[c, bi], [own, self.f1.at[c, bi, 0], self.f1.at[c, bi, 1]])
            if off == 2:
                for d in DIRS:
                    self.copy(c, 2, 0, d, 0).start()
            else:
                self.copy(c, 2, 0, off, 1).start()

    def augment2(self, d):
        q = self.q
        di = 0 if d == 1 else 1
        for c in BOTH:
            self.copy(c, 2, 0, d, 0).wait_recv()
            mine = self.mid.at[c, self.order.index(d), pl.ds(di * q, q)]
            add_rows(mine, [mine, self.h2.at[c, di]])
            self.copy(c, 2, 0, d, 2).start()

    def last(self):
        for c in BOTH:
            self.all_of(self.f2.at[c], 28 + c)

    def finish(self, resid, out):
        q, d = self.q, out.shape[-1]
        width = min(512, d)
        for c in BOTH:
            rows = pl.ds(c * 2 * q, 2 * q)

            @pl.loop(0, d // width)
            def _(i):
                cols = pl.ds(pl.multiple_of(i * width, width), width)
                tot = self.part[self.tor.me, rows, cols].astype(F32)
                for di in BOTH:
                    tot += self.f1[c, self.order.index(0), di, :, cols].astype(F32)
                for di in BOTH:
                    tot += self.f2[c, di, :, cols].astype(F32)
                tot = tot.astype(BF16).astype(F32)
                out[rows, cols] = (resid[rows, cols].astype(F32) + tot).astype(BF16)

    def drain(self):
        view = self.part.at[pl.ds(0, self.part.shape[0] - 1)]
        remote(view, view, self.ssem, self.rsem.at[0], {"ty": self.tor.me}).wait_send()


class Exchange:
    def __init__(self, tx_count, src, dst, whole, ssem, rsem):
        self.n, self.src, self.dst, self.whole, self.ssem, self.rsem = tx_count, src, dst, whole, ssem, rsem
        self.me = lax.axis_index("tx")

    def start(self):
        for k in range(1, self.n):
            p = lax.rem(self.me + k, self.n)
            remote(self.src(p), self.dst(self.me), self.ssem, self.rsem, {"tx": p}).start()
        pltpu.make_async_copy(self.src(self.me), self.dst(self.me), self.rsem).start()

    def wait(self):
        view = self.whole(self.n)
        remote(view, view, self.ssem, self.rsem, {"tx": self.me}).wait_recv()

    def drain(self):
        view = self.whole(self.n - 1)
        remote(view, view, self.ssem, self.rsem, {"tx": self.me}).wait_send()


def norm_rows(src, dst):
    tok, d = src.shape
    step = 16

    @pl.loop(0, tok // step)
    def _(i):
        rows = pl.ds(pl.multiple_of(i * step, step), step)
        v = src[rows, :].astype(F32)
        mean = jnp.sum(v, axis=-1, keepdims=True) * (1.0 / d)
        var = jnp.sum(v * v, axis=-1, keepdims=True) * (1.0 / d) - mean * mean
        dst[rows, :] = ((v - mean) * lax.rsqrt(var + EPS)).astype(BF16)


class Ring:
    SEMS = 5

    def __init__(self, tx_count, rows, src, slot, whole, ssem, rsem):
        self.nx, self.rows, self.src, self.slot, self.whole, self.ssem, self.rsem = tx_count // 2, rows, src, slot, whole, ssem, rsem
        me = lax.axis_index("tx")
        self.me, self.x, self.core = me, lax.div(me, 2), lax.rem(me, 2)
        self.split = (rows // 2 + 15) // 16 * 16

    def tx(self, dx, other=False):
        return wrap(self.x + dx, self.nx) * 2 + (1 - self.core if other else self.core)

    def half(self, view, d):
        return view.at[pl.ds(0, self.split)] if d == 1 else view.at[pl.ds(self.split, self.rows - self.split)]

    def copy(self, i, src, dst, to):
        return remote(src, dst, self.ssem, self.rsem.at[i], {"tx": to})

    def pass_on(self, d, recv=False):
        view = self.slot(self.tx(-d if recv else 0))
        return self.copy(0 if d == 1 else 1, view if recv else self.src, view, self.tx(d))

    def relay(self, d, recv=False):
        view = self.half(self.slot(self.tx(-2 * d if recv else -d)), d)
        return self.copy(2 if d == 1 else 3, view, view, self.tx(d))

    def across(self, which, recv=False):
        view = self.slot(self.tx(which, recv))
        if abs(which) == 2:
            view = self.half(view, which // 2)
        src = self.src if which == 0 and not recv else view
        return self.copy(4, src, view, self.tx(0, True))

    def all_across(self):
        return (0, 1, -1, 2, -2) if self.nx > 1 else (0,)

    def own(self):
        return pltpu.make_async_copy(self.src, self.slot(self.me), self.rsem.at[4])

    def start(self, place=True):
        if self.nx > 1:
            for d in DIRS:
                self.pass_on(d).start()
        self.across(0).start()
        if place:
            self.own().start()

    def step(self):
        if self.nx > 1:
            for d in DIRS:
                self.pass_on(d, True).wait_recv()
                self.relay(d).start()
                self.across(-d).start()

    def step2(self):
        if self.nx > 1:
            for d in DIRS:
                self.relay(d, True).wait_recv()
                self.across(2 * d).start()

    def finish(self, place=True):
        view = self.whole(self.nx + (1 if place else 0))
        remote(view, view, self.ssem, self.rsem.at[4], {"tx": self.me}).wait_recv()

    def drain(self):
        view = self.whole(2 * self.nx - 1)
        remote(view, view, self.ssem, self.rsem.at[4], {"tx": self.me}).wait_send()


def layer_kernel(tx_count, x_ref, wq_ref, wk_ref, wv_ref, wo_ref, wg_ref, wu_ref, wd_ref, cos_hbm, sin_hbm, y_ref,
                 xp, x2, wqkv, wo, wg, wu, wd, xs, os_, act, kv, xt, h, yr, cos_ref, sin_ref,
                 load_sem, a2a_s, a2a_r, qkv_s, qkv_r, via_s, via_r, gs, gr, ws, wr, *rs_bufs):
    n_dev, tok, d = xp.shape
    dx = x_ref.shape[1]
    hc = wq_ref.shape[1]
    f, fp = wg_ref.shape[0], wg.shape[2]
    seq = tok * tx_count
    spd = n_dev // tx_count
    heads = hc // HEAD_DIM
    q2 = tok // 2
    c3 = 3 * hc
    tor = Torus()
    me_tx = lax.axis_index("tx")

    def exchange(i, src, dst, whole):
        return Exchange(tx_count, src, dst, whole, a2a_s.at[i], a2a_r.at[i])

    def col(start, width):
        return pl.ds(pl.multiple_of(start, width), width)

    def ring(i, src, buf, inner):
        return Ring(tx_count, src.shape[0], src, lambda o: buf.at[(o, *inner)], lambda n: buf.at[(pl.ds(0, n), *inner)], ws.at[i], wr.at[i])

    every = pl.ds(0, dx)
    rings = [ring(i, src, wqkv, (every, pl.ds(i * hc, hc))) for i, src in enumerate((wq_ref, wk_ref, wv_ref))]
    r_o = ring(3, wo_ref, wo, ())
    r_gate = ring(4, wg.at[me_tx], wg, ())
    r_up = ring(5, wu.at[me_tx], wu, ())
    r_down = ring(6, wd_ref, wd, (pl.ds(0, f),))

    x_in = pltpu.make_async_copy(x_ref, yr, load_sem.at[2])
    x_in.start()
    raw = [pltpu.make_async_copy(src, wd.at[i, pl.ds(0, f)], load_sem.at[i]) for i, src in enumerate((wg_ref, wu_ref))]
    raw += [pltpu.make_async_copy(cos_hbm, cos_ref, load_sem.at[3]), pltpu.make_async_copy(sin_hbm, sin_ref, load_sem.at[4])]
    for cp in raw:
        cp.start()
    entry_barrier(tor, tx_count)
    x_in.wait()
    xe = exchange(
        0,
        lambda p: yr.at[pl.ds(pl.multiple_of(p * tok, tok), tok)],
        lambda o: xt.at[:, col(o * dx, dx)],
        lambda n: yr.at[pl.ds(0, n * tok)],
    )
    xe.start()
    if fp > f:
        wd[:, pl.ds(f, fp - f), :] = jnp.zeros((tx_count, fp - f, dx), BF16)
    xe.wait()
    norm_rows(xt, xp.at[tor.me])
    g1 = Gather(tor, xp, gs, gr)
    g1.start()
    for r in rings:
        r.start()
    for cp in raw:
        cp.wait()
    for i, dst in enumerate((wg, wu)):
        for j in range(fp // 128):
            dst[me_tx, :, pl.ds(j * 128, 128)] = wd[i, pl.ds(j * 128, 128), :].T

    def pieces(off):
        return [(c, tor.slot(1 - c, off, n), (c * 4 + n) * q2) for c in BOTH for n in range(RING)]

    def stage(src, off, dst, cols):
        for c, s, at in pieces(off):
            dst[pl.ds(at, q2), :] = src[s, pl.ds(c * q2, q2), cols]

    detours = tx_count == 8
    x_pos = lax.div(me_tx, 2)
    edge = (x_pos == 0) | (x_pos == 3)
    opposite = jnp.where(x_pos == 0, 2, 1)
    inner = jnp.where(x_pos == 0, 1, 2)
    over = (3 - x_pos) * 2 + lax.rem(me_tx, 2)
    via = pl.ds(2 * c3 + 2 * hc, c3)

    def qkv_group(off):
        stage(xp, off, xs, pl.ds(0, d))

        @pl.loop(0, 3)
        def _(n):
            cols = col(n * hc, hc)
            out = jnp.dot(xs[...], wqkv[:, :, cols].reshape(d, hc), preferred_element_type=F32).astype(BF16)
            for c, s, at in pieces(off):
                x2[s, pl.ds(c * q2, q2), cols] = out[at : at + q2]

        for c, s, _ in pieces(off):
            p, sl = lax.div(s, spd), lax.rem(s, spd)
            rows = pl.ds(c * q2, q2)
            src = x2.at[s, rows, pl.ds(0, c3)]
            dst = x2.at[sl * tx_count + me_tx, rows, pl.ds(c3, c3)]

            detour = (p != p) if off > 0 or not detours else edge & (lax.div(p, 2) == opposite)

            @pl.when(p == me_tx)
            def _():
                pltpu.make_async_copy(src, dst, qkv_r.at[sl]).start()

            @pl.when(detour)
            def _():
                remote(src, x2.at[s, rows, via], qkv_s, via_r.at[2 * AWAY.index(off) + c], {"tx": over}).start()

            @pl.when((p != me_tx) & jnp.logical_not(detour))
            def _():
                remote(src, dst, qkv_s, qkv_r.at[sl], {"tx": p}).start()

    def detour_rows(off, c):
        rows = pl.ds(c * q2, q2)
        return [(s, rows) for s in ([inner * RING + wrap(tor.pos[1] + off, RING)] if c == 0 else [inner * RING + y for y in range(RING)])]

    def pass_detour(off):
        if not detours:
            return
        for c in BOTH:

            @pl.when(edge if c == 0 else edge & (wrap(tor.pos[0] + off, RING) == inner))
            def _():
                for s, rows in detour_rows(off, c):
                    view = x2.at[s, rows, via]
                    if c == 0:
                        remote(view, view, via_s, via_r.at[2 * AWAY.index(off) + c], {"tx": me_tx}).wait_recv()
                if c == 1:
                    view = x2.at[pl.ds(inner * RING, 2), :, via]
                    remote(view, view, via_s, via_r.at[2 * AWAY.index(off) + c], {"tx": me_tx}).wait_recv()
                for s, rows in detour_rows(off, c):
                    p, sl = lax.div(s, spd), lax.rem(s, spd)
                    remote(x2.at[s, rows, via], x2.at[sl * tx_count + over, rows, pl.ds(c3, c3)], via_s, qkv_r.at[sl], {"tx": p}).start()

    def drain_detours():
        if not detours:
            return
        for off in (0, -1):
            for c in BOTH:

                @pl.when(edge if c == 0 else edge & (wrap(tor.pos[0] + off, RING) == inner))
                def _():
                    view = x2.at[0, pl.ds(0, q2), via] if c == 0 else x2.at[pl.ds(0, 2), :, via]
                    remote(view, view, via_s, via_r.at[0], {"tx": me_tx}).wait_send()

    xe.drain()
    wq_r, wk_r, wv_r = rings
    g1.near()
    wq_r.step()
    g1.relay(0)
    g1.spread(-1)
    g1.spread(1)
    wk_r.step()
    wv_r.step()
    g1.halves(0)
    wq_r.step2()
    wk_r.step2()
    g1.relay(-1)
    g1.far(False)
    wv_r.step2()
    for r in rings:
        r.finish()
    qkv_group(0)
    g1.relay(1)
    g1.far(True)
    g1.halves(-1)
    qkv_group(-1)
    g1.relay(2)
    g1.halves(1)
    qkv_group(1)
    pass_detour(0)
    g1.halves(2)
    qkv_group(2)
    pass_detour(-1)
    r_o.start()

    block = min(seq, 128)
    sends = []
    for s in range(spd):
        view = x2.at[pl.ds(s * tx_count, tx_count), :, pl.ds(c3, c3)]
        remote(view, view, qkv_s, qkv_r.at[s], {"tx": me_tx}).wait_recv()

        @pl.loop(0, heads)
        def _(hd):
            def part(which):
                return x2[pl.ds(s * tx_count, tx_count), :, col(c3 + which * hc + hd * HEAD_DIM, HEAD_DIM)].reshape(seq, HEAD_DIM)

            for which in BOTH:
                v = part(which).astype(F32)
                rot = v * cos_ref[...] + pltpu.roll(v, HEAD_DIM // 2, 1) * sin_ref[...]
                kv[which] = rot.astype(BF16)
            kv[2] = part(2)
            for b in range(seq // block):
                keys = (b + 1) * block
                sc = lax.dot_general(kv[0, pl.ds(b * block, block)], kv[1, pl.ds(0, keys)], (((1,), (1,)), ((), ())), preferred_element_type=F32)
                sc = sc * HEAD_DIM ** -0.5
                q_pos = b * block + lax.broadcasted_iota(jnp.int32, (block, keys), 0)
                k_pos = lax.broadcasted_iota(jnp.int32, (block, keys), 1)
                sc = jnp.where(q_pos >= k_pos, sc, -1e30)
                e = jnp.exp(sc - jnp.max(sc, axis=-1, keepdims=True))
                prob = (e / jnp.sum(e, axis=-1, keepdims=True)).astype(BF16)
                o = jnp.dot(prob, kv[2, pl.ds(0, keys)], preferred_element_type=F32).astype(BF16)
                for n in range(block // tok):
                    at = (b * (block // tok) + n) * spd + s
                    x2[at, :, col(2 * c3 + hd * HEAD_DIM, HEAD_DIM)] = o[n * tok : (n + 1) * tok]

        oe = exchange(
            1 + s,
            lambda p, s=s: x2.at[p * spd + s, :, pl.ds(2 * c3, hc)],
            lambda o, s=s: x2.at[o * spd + s, :, pl.ds(2 * c3 + hc, hc)],
            lambda n: x2.at[pl.ds(0, n), :, pl.ds(2 * c3, hc)],
        )
        oe.start()
        sends.append(oe)

    r_o.step()
    g1.drain()
    drain_detours()
    view = x2.at[pl.ds(0, (tx_count - 1) * spd), :, pl.ds(0, c3)]
    remote(view, view, qkv_s, qkv_r.at[0], {"tx": me_tx}).wait_send()
    for oe in sends:
        oe.wait()
        oe.drain()
    r_o.step2()
    r_gate.start(place=False)
    r_up.start(place=False)
    r_down.start()
    r_o.finish()

    def put(off, x, out):
        for c, s, at in pieces(off):
            xp[s, pl.ds(c * q2, q2), col(x * dx, dx)] = out[at : at + q2]

    def o_group(off):
        stage(x2, off, os_, pl.ds(2 * c3 + hc, hc))

        @pl.loop(0, tx_count)
        def _(x):
            put(off, x, jnp.dot(os_[...], wo[x], preferred_element_type=F32).astype(BF16))

    order = (2, -1, 1, 0)
    sc1 = Scatter(tor, xp, rs_bufs, order)
    o_group(order[0])
    sc1.issue(0)
    o_group(order[1])
    sc1.issue(1)
    o_group(order[2])
    sc1.augment(0)
    sc1.issue(2)
    o_group(order[3])
    sc1.augment(1)
    sc1.issue(3)
    sc1.arrived(0)
    r_gate.step()
    sc1.augment(2)
    sc1.arrived(1)
    sc1.augment2(-1)
    sc1.augment(3)
    sc1.arrived(2)
    sc1.augment2(1)
    r_up.step()
    sc1.arrived(3)
    sc1.last()
    sc1.finish(xt, h)
    norm_rows(h, x2.at[tor.me])
    g2 = Gather(tor, x2, gs, gr)
    g2.start()
    sc1.drain()

    def mlp_group(off, between, mid):
        stage(x2, off, xs, pl.ds(0, d))
        width = 256 if fp % 256 == 0 else 128

        @pl.loop(0, fp // width)
        def _(n):
            cols = col(n * width, width)
            gate = jnp.dot(xs[...], wg[:, :, cols].reshape(d, width), preferred_element_type=F32).astype(BF16).astype(F32)
            up = jnp.dot(xs[...], wu[:, :, cols].reshape(d, width), preferred_element_type=F32).astype(BF16).astype(F32)
            act[:, cols] = (gate * jax.nn.sigmoid(gate) * up).astype(BF16)

        between()
        half = tx_count // 2
        for lo, then in ((0, mid), (half, nothing)):

            @pl.loop(lo, lo + half)
            def _(x):
                put(off, x, jnp.dot(act[...], wd[x], preferred_element_type=F32).astype(BF16))

            then()

    sc2 = Scatter(tor, xp, rs_bufs, (-1, 1, 2, 0))
    g2.near()
    r_down.step()
    g2.relay(0)
    g2.spread(-1)
    g2.spread(1)
    r_gate.step2()
    r_up.step2()
    g2.halves(0)
    r_gate.finish(place=False)
    r_up.finish(place=False)

    def onward():
        g2.relay(-1)
        g2.far(False)
        r_down.step2()
        r_down.finish()

    mlp_group(0, onward, nothing)
    g2.relay(1)
    g2.far(True)
    g2.halves(-1)
    mlp_group(-1, nothing, lambda: g2.relay(2))
    sc2.issue(0)
    g2.halves(1)
    mlp_group(1, nothing, nothing)
    sc2.issue(1)
    g2.halves(2)
    mlp_group(2, nothing, nothing)
    sc2.issue(2)
    sc2.augment(0)
    sc2.augment(1)
    sc2.issue(3)
    sc2.arrived(0)
    sc2.augment(2)
    sc2.arrived(1)
    sc2.arrived(2)
    sc2.augment(3)
    sc2.augment2(-1)
    sc2.augment2(1)
    sc2.arrived(3)
    sc2.last()
    sc2.finish(h, xt)
    ye = exchange(
        1 + spd,
        lambda p: xt.at[:, col(p * dx, dx)],
        lambda o: yr.at[pl.ds(pl.multiple_of(o * tok, tok), tok)],
        lambda n: yr.at[pl.ds(0, n * tok)],
    )
    ye.start()
    g2.drain()
    sc2.drain()
    for r in rings + [r_o, r_gate, r_up, r_down]:
        r.drain()
    ye.wait()
    out = pltpu.make_async_copy(yr, y_ref, load_sem.at[0])
    out.start()
    ye.drain()
    out.wait()


ANY_SPEC = pl.BlockSpec(memory_space=pl.ANY)


def rotary_tables(seq_len):
    half = HEAD_DIM // 2
    inv_freq = (THETA ** (-2.0 * np.arange(half) / HEAD_DIM)).astype(np.float32)
    angles = np.arange(seq_len, dtype=np.float32)[:, None] * inv_freq[None, :]
    cos_t, sin_t = np.cos(angles), np.sin(angles)
    return np.concatenate([cos_t, cos_t], -1), np.concatenate([-sin_t, sin_t], -1)


def solution(mesh):
    tx_count, n_dev = mesh.shape["tx"], mesh.shape["ty"]
    act_spec = P(("dp", "ty"), None, "tx")
    col_spec = P("tx", "ty")
    row_spec = P("ty", "tx")
    dma = pltpu.SemaphoreType.DMA

    def layer_fn(x_blk, w_q, w_k, w_v, w_o, w_gate, w_up, w_down):
        seq, dx = x_blk.shape[1:]
        hc, f = w_q.shape[1], w_gate.shape[1]
        tok, d = seq // tx_count, dx * tx_count
        fp = -(-f // 128) * 128
        rows, spd = 4 * tok, n_dev // tx_count
        cos_t, sin_t = rotary_tables(seq)
        bf = lambda *shape: pltpu.VMEM(shape, BF16)
        scratch = [
            bf(n_dev, tok, d), bf(n_dev, tok, d), bf(tx_count, dx, 3 * hc), bf(tx_count, hc, dx),
            bf(tx_count, dx, fp), bf(tx_count, dx, fp), bf(tx_count, fp, dx),
            bf(rows, d), bf(rows, hc), bf(rows, fp), bf(3, seq, HEAD_DIM), bf(tok, d), bf(tok, d), bf(seq, dx),
            pltpu.VMEM((seq, HEAD_DIM), F32), pltpu.VMEM((seq, HEAD_DIM), F32),
            dma((5,)), dma((spd + 2,)), dma((spd + 2,)), dma, dma((spd,)), dma, dma((4,)),
            dma, dma((Gather.SEMS,)), dma((7,)), dma((7, Ring.SEMS)),
        ] + Scatter.buffers(tok, d)
        y = pl.pallas_call(
            functools.partial(layer_kernel, tx_count),
            name="layer",
            out_shape=jax.ShapeDtypeStruct((seq, dx), BF16),
            in_specs=[ANY_SPEC] * 10,
            out_specs=ANY_SPEC,
            scratch_shapes=scratch,
            compiler_params=pltpu.CompilerParams(collective_id=1, has_side_effects=True, vmem_limit_bytes=67043328),
        )(x_blk[0], w_q, w_k, w_v, w_o, w_gate.T, w_up.T, w_down, cos_t, sin_t)
        return y[None]

    return jax.shard_map(layer_fn, mesh=mesh, in_specs=(act_spec, col_spec, col_spec, col_spec, row_spec, col_spec, col_spec, row_spec), out_specs=act_spec, check_vma=False)
```

```python
import functools

import numpy as np
import jax
import jax.numpy as jnp
from jax import lax
from jax.experimental import pallas as pl
from jax.experimental.pallas import tpu as pltpu
from jax.sharding import PartitionSpec as P

HEAD_DIM = 128
EPS = 1e-5
THETA = 10000.0
RING = 4
BOTH = (0, 1)
DIRS = (1, -1)
MESH = pl.DeviceIdType.MESH
BF16 = jnp.bfloat16
F32 = jnp.float32
AWAY = (0, -1, 1, 2)


def nothing():
    pass


def wrap(v, n):
    return lax.rem(v + 2 * n, n)


class Torus:
    def __init__(self):
        t = lax.axis_index("ty")
        self.me = t
        self.pos = (lax.div(t, RING), lax.rem(t, RING))

    def slot(self, first, a_off, b_off):
        a = wrap(self.pos[first] + a_off, RING)
        b = wrap(self.pos[1 - first] + b_off, RING)
        return a * RING + b if first == 0 else b * RING + a


def entry_barrier(tor, tx_count):
    sem = pltpu.get_barrier_semaphore()
    for first in (0, 1):
        for d in DIRS:
            pl.semaphore_signal(sem, inc=1, device_id={"ty": tor.slot(first, d, 0)}, device_id_type=MESH)
    me = lax.axis_index("tx")
    for k in range(1, tx_count):
        pl.semaphore_signal(sem, inc=1, device_id={"tx": lax.rem(me + k, tx_count)}, device_id_type=MESH)
    pl.semaphore_wait(sem, 4 + tx_count - 1)


def remote(src, dst, ssem, rsem, device):
    return pltpu.make_async_remote_copy(src_ref=src, dst_ref=dst, send_sem=ssem, recv_sem=rsem, device_id=device, device_id_type=MESH)


class Gather:
    SEMS = 25

    def __init__(self, tor, buf, ssem, rsem):
        self.tor, self.buf, self.ssem, self.rsem = tor, buf, ssem, rsem
        self.q = buf.shape[1] // 4

    def first(self, c):
        return 1 if c == 0 else 0

    def rows(self, c, d, half):
        if not half:
            return pl.ds(c * 2 * self.q, 2 * self.q)
        return pl.ds(c * 2 * self.q + (0 if d == 1 else self.q), self.q)

    def sem(self, c, ph, off, d, half):
        if half:
            return 20 + (0 if ph == 1 else 1 + AWAY.index(off))
        return (0 if ph == 1 else 4 + 4 * AWAY.index(off)) + c * 2 + (0 if d == 1 else 1)

    def copy(self, c, ph, off, d, half, hops):
        first = self.first(c)
        back = -d * hops
        s = self.tor.slot(first, back, 0) if ph == 1 else self.tor.slot(first, off, back)
        to = self.tor.slot(first, d, 0) if ph == 1 else self.tor.slot(first, 0, d)
        view = self.buf.at[s, self.rows(c, d, half)]
        return remote(view, view, self.ssem, self.rsem.at[self.sem(c, ph, off, d, half)], {"ty": to})

    def send(self, c, ph, off, d, half=False):
        self.copy(c, ph, off, d, half, 1 if half else 0).start()

    def recv(self, c, ph, off, d):
        self.copy(c, ph, off, d, False, 1).wait_recv()

    def far_copy(self, c, d, second, hops):
        s = self.tor.slot(self.first(c), 2, -d * hops)
        view = self.buf.at[s, self.rows(c, -d if second else d, True)]
        i = self.sem(c, 2, 2, d, second)
        return remote(view, view, self.ssem, self.rsem.at[i], {"ty": self.tor.slot(self.first(c), 0, d)})

    def recv_halves(self, ph, off):
        view = self.buf.at[pl.ds(0, 2)] if ph == off == 2 else self.buf.at[0]
        remote(view, view, self.ssem, self.rsem.at[self.sem(0, ph, off, 1, True)], {"ty": self.tor.me}).wait_recv()

    def start(self):
        for ph in (1, 2):
            for c in BOTH:
                for d in DIRS:
                    self.send(c, ph, 0, d)

    def near(self):
        for d in DIRS:
            for c in BOTH:
                self.recv(c, 1, 0, d)
                self.send(c, 1, 0, d, True)

    def spread(self, off):
        for c in BOTH:
            for d in DIRS:
                self.send(c, 2, off, d)

    def relay(self, off):
        for d in DIRS:
            for c in BOTH:
                if off == 2:
                    self.far_copy(c, d, False, 1).wait_recv()
                else:
                    self.recv(c, 2, off, d)
                self.send(c, 2, off, d, True)

    def far(self, second):
        if not second:
            self.recv_halves(1, 0)
        for c in BOTH:
            for d in DIRS:
                self.far_copy(c, d, second, 0).start()

    def halves(self, off):
        self.recv_halves(2, off)

    def drain(self):
        view = self.buf.at[pl.ds(0, self.buf.shape[0] - 1)]
        remote(view, view, self.ssem, self.rsem.at[0], {"ty": self.tor.me}).wait_send()


def add_rows(dst, srcs, width=512):
    d = dst.shape[-1]
    width = min(width, d)

    @pl.loop(0, d // width)
    def _(i):
        cols = pl.ds(pl.multiple_of(i * width, width), width)
        tot = srcs[0][:, cols].astype(F32)
        for s in srcs[1:]:
            tot += s[:, cols].astype(F32)
        dst[:, cols] = tot.astype(dst.dtype)


class Scatter:
    SEMS = 30

    @staticmethod
    def buffers(tok, d):
        q = tok // 4
        return [
            pltpu.VMEM((2, 4, 2, q, d), BF16),
            pltpu.VMEM((2, 4, 2, 2 * q, d), BF16),
            pltpu.VMEM((2, 3, 2 * q, d), BF16),
            pltpu.VMEM((2, 2, q, d), BF16),
            pltpu.VMEM((2, 2, 2 * q, d), BF16),
            pltpu.SemaphoreType.DMA,
            pltpu.SemaphoreType.DMA((Scatter.SEMS,)),
        ]

    def __init__(self, tor, part, bufs, order):
        self.tor, self.part, self.order = tor, part, order
        self.h1, self.f1, self.mid, self.h2, self.f2, self.ssem, self.rsem = bufs
        self.q = part.shape[1] // 4

    def copy(self, c, ph, bi, d, kind):
        q, first = self.q, c
        di = 0 if d == 1 else 1
        h = di if kind in (0, 2) else 1 - di
        step = 2 * d if kind == 0 else d
        if ph == 1:
            i = c * 8 + bi * 2 + di if kind == 0 else 16 + c * 4 + bi
            src = self.part.at[self.tor.slot(first, step, self.order[bi]), pl.ds(c * 2 * q + h * q, q)]
            dst = self.h1.at[c, bi, di] if kind == 0 else self.f1.at[c, bi, di, pl.ds(h * q, q)]
            to = self.tor.slot(first, d, 0)
        else:
            i = 24 + c * 2 + di if kind == 0 else 28 + c
            src = self.mid.at[c, self.order.index(2 if kind == 0 else d), pl.ds(h * q, q)]
            dst = self.h2.at[c, di] if kind == 0 else self.f2.at[c, di, pl.ds(h * q, q)]
            to = self.tor.slot(first, 0, d)
        return remote(src, dst, self.ssem, self.rsem.at[i], {"ty": to})

    def all_of(self, view, i):
        remote(view, view, self.ssem, self.rsem.at[i], {"ty": self.tor.me}).wait_recv()

    def issue(self, bi):
        for kind in BOTH:
            for c in BOTH:
                for d in DIRS:
                    self.copy(c, 1, bi, d, kind).start()

    def augment(self, bi):
        q = self.q
        for c in BOTH:
            for d in DIRS:
                di = 0 if d == 1 else 1
                self.copy(c, 1, bi, d, 0).wait_recv()
                mine = self.part.at[self.tor.slot(c, d, self.order[bi]), pl.ds(c * 2 * q + di * q, q)]
                add_rows(mine, [mine, self.h1.at[c, bi, di]])
                self.copy(c, 1, bi, d, 2).start()

    def arrived(self, bi):
        q = self.q
        for c in BOTH:
            self.all_of(self.f1.at[c, bi], 16 + c * 4 + bi)
            off = self.order[bi]
            if off == 0:
                continue
            own = self.part.at[self.tor.slot(c, 0, off), pl.ds(c * 2 * q, 2 * q)]
            add_rows(self.mid.at[c, bi], [own, self.f1.at[c, bi, 0], self.f1.at[c, bi, 1]])
            if off == 2:
                for d in DIRS:
                    self.copy(c, 2, 0, d, 0).start()
            else:
                self.copy(c, 2, 0, off, 1).start()

    def augment2(self, d):
        q = self.q
        di = 0 if d == 1 else 1
        for c in BOTH:
            self.copy(c, 2, 0, d, 0).wait_recv()
            mine = self.mid.at[c, self.order.index(d), pl.ds(di * q, q)]
            add_rows(mine, [mine, self.h2.at[c, di]])
            self.copy(c, 2, 0, d, 2).start()

    def last(self):
        for c in BOTH:
            self.all_of(self.f2.at[c], 28 + c)

    def finish(self, resid, out):
        q, d = self.q, out.shape[-1]
        width = min(512, d)
        for c in BOTH:
            rows = pl.ds(c * 2 * q, 2 * q)

            @pl.loop(0, d // width)
            def _(i):
                cols = pl.ds(pl.multiple_of(i * width, width), width)
                tot = self.part[self.tor.me, rows, cols].astype(F32)
                for di in BOTH:
                    tot += self.f1[c, self.order.index(0), di, :, cols].astype(F32)
                for di in BOTH:
                    tot += self.f2[c, di, :, cols].astype(F32)
                tot = tot.astype(BF16).astype(F32)
                out[rows, cols] = (resid[rows, cols].astype(F32) + tot).astype(BF16)

    def drain(self):
        view = self.part.at[pl.ds(0, self.part.shape[0] - 1)]
        remote(view, view, self.ssem, self.rsem.at[0], {"ty": self.tor.me}).wait_send()


class Exchange:
    def __init__(self, tx_count, src, dst, whole, ssem, rsem):
        self.n, self.src, self.dst, self.whole, self.ssem, self.rsem = tx_count, src, dst, whole, ssem, rsem
        self.me = lax.axis_index("tx")

    def start(self):
        for k in range(1, self.n):
            p = lax.rem(self.me + k, self.n)
            remote(self.src(p), self.dst(self.me), self.ssem, self.rsem, {"tx": p}).start()
        pltpu.make_async_copy(self.src(self.me), self.dst(self.me), self.rsem).start()

    def wait(self):
        view = self.whole(self.n)
        remote(view, view, self.ssem, self.rsem, {"tx": self.me}).wait_recv()

    def drain(self):
        view = self.whole(self.n - 1)
        remote(view, view, self.ssem, self.rsem, {"tx": self.me}).wait_send()


def norm_rows(src, dst):
    tok, d = src.shape
    step = 16

    @pl.loop(0, tok // step)
    def _(i):
        rows = pl.ds(pl.multiple_of(i * step, step), step)
        v = src[rows, :].astype(F32)
        mean = jnp.sum(v, axis=-1, keepdims=True) * (1.0 / d)
        var = jnp.sum(v * v, axis=-1, keepdims=True) * (1.0 / d) - mean * mean
        dst[rows, :] = ((v - mean) * lax.rsqrt(var + EPS)).astype(BF16)


class Ring:
    SEMS = 5

    def __init__(self, tx_count, rows, src, slot, whole, ssem, rsem):
        self.nx, self.rows, self.src, self.slot, self.whole, self.ssem, self.rsem = tx_count // 2, rows, src, slot, whole, ssem, rsem
        me = lax.axis_index("tx")
        self.me, self.x, self.core = me, lax.div(me, 2), lax.rem(me, 2)
        self.split = (rows // 2 + 15) // 16 * 16

    def tx(self, dx, other=False):
        return wrap(self.x + dx, self.nx) * 2 + (1 - self.core if other else self.core)

    def half(self, view, d):
        return view.at[pl.ds(0, self.split)] if d == 1 else view.at[pl.ds(self.split, self.rows - self.split)]

    def copy(self, i, src, dst, to):
        return remote(src, dst, self.ssem, self.rsem.at[i], {"tx": to})

    def pass_on(self, d, recv=False):
        view = self.slot(self.tx(-d if recv else 0))
        return self.copy(0 if d == 1 else 1, view if recv else self.src, view, self.tx(d))

    def relay(self, d, recv=False):
        view = self.half(self.slot(self.tx(-2 * d if recv else -d)), d)
        return self.copy(2 if d == 1 else 3, view, view, self.tx(d))

    def across(self, which, recv=False):
        view = self.slot(self.tx(which, recv))
        if abs(which) == 2:
            view = self.half(view, which // 2)
        src = self.src if which == 0 and not recv else view
        return self.copy(4, src, view, self.tx(0, True))

    def all_across(self):
        return (0, 1, -1, 2, -2) if self.nx > 1 else (0,)

    def own(self):
        return pltpu.make_async_copy(self.src, self.slot(self.me), self.rsem.at[4])

    def start(self, place=True):
        if self.nx > 1:
            for d in DIRS:
                self.pass_on(d).start()
        self.across(0).start()
        if place:
            self.own().start()

    def step(self):
        if self.nx > 1:
            for d in DIRS:
                self.pass_on(d, True).wait_recv()
                self.relay(d).start()
                self.across(-d).start()

    def step2(self):
        if self.nx > 1:
            for d in DIRS:
                self.relay(d, True).wait_recv()
                self.across(2 * d).start()

    def finish(self, place=True):
        view = self.whole(self.nx + (1 if place else 0))
        remote(view, view, self.ssem, self.rsem.at[4], {"tx": self.me}).wait_recv()

    def drain(self):
        view = self.whole(2 * self.nx - 1)
        remote(view, view, self.ssem, self.rsem.at[4], {"tx": self.me}).wait_send()


def layer_kernel(tx_count, x_ref, wq_ref, wk_ref, wv_ref, wo_ref, wg_ref, wu_ref, wd_ref, cos_hbm, sin_hbm, y_ref,
                 xp, x2, wqkv, wo, wg, wu, wd, xs, os_, act, kv, xt, h, yr, cos_ref, sin_ref,
                 load_sem, a2a_s, a2a_r, qkv_s, qkv_r, via_s, via_r, gs, gr, ws, wr, *rs_bufs):
    n_dev, tok, d = xp.shape
    dx = x_ref.shape[1]
    hc = wq_ref.shape[1]
    f, fp = wg_ref.shape[0], wg.shape[2]
    seq = tok * tx_count
    spd = n_dev // tx_count
    heads = hc // HEAD_DIM
    q2 = tok // 2
    c3 = 3 * hc
    tor = Torus()
    me_tx = lax.axis_index("tx")

    def exchange(i, src, dst, whole):
        return Exchange(tx_count, src, dst, whole, a2a_s.at[i], a2a_r.at[i])

    def col(start, width):
        return pl.ds(pl.multiple_of(start, width), width)

    def ring(i, src, buf, inner):
        return Ring(tx_count, src.shape[0], src, lambda o: buf.at[(o, *inner)], lambda n: buf.at[(pl.ds(0, n), *inner)], ws.at[i], wr.at[i])

    every = pl.ds(0, dx)
    rings = [ring(i, src, wqkv, (every, pl.ds(i * hc, hc))) for i, src in enumerate((wq_ref, wk_ref, wv_ref))]
    r_o = ring(3, wo_ref, wo, ())
    r_gate = ring(4, wg.at[me_tx], wg, ())
    r_up = ring(5, wu.at[me_tx], wu, ())
    r_down = ring(6, wd_ref, wd, (pl.ds(0, f),))

    x_in = pltpu.make_async_copy(x_ref, yr, load_sem.at[2])
    x_in.start()
    raw = [pltpu.make_async_copy(src, wd.at[i, pl.ds(0, f)], load_sem.at[i]) for i, src in enumerate((wg_ref, wu_ref))]
    raw += [pltpu.make_async_copy(cos_hbm, cos_ref, load_sem.at[3]), pltpu.make_async_copy(sin_hbm, sin_ref, load_sem.at[4])]
    for cp in raw:
        cp.start()
    entry_barrier(tor, tx_count)
    x_in.wait()
    xe = exchange(
        0,
        lambda p: yr.at[pl.ds(pl.multiple_of(p * tok, tok), tok)],
        lambda o: xt.at[:, col(o * dx, dx)],
        lambda n: yr.at[pl.ds(0, n * tok)],
    )
    xe.start()
    if fp > f:
        wd[:, pl.ds(f, fp - f), :] = jnp.zeros((tx_count, fp - f, dx), BF16)
    xe.wait()
    norm_rows(xt, xp.at[tor.me])
    g1 = Gather(tor, xp, gs, gr)
    g1.start()
    for r in rings:
        r.start()
    for cp in raw:
        cp.wait()
    for i, dst in enumerate((wg, wu)):
        for j in range(fp // 128):
            dst[me_tx, :, pl.ds(j * 128, 128)] = wd[i, pl.ds(j * 128, 128), :].T

    def pieces(off):
        return [(c, tor.slot(1 - c, off, n), (c * 4 + n) * q2) for c in BOTH for n in range(RING)]

    def stage(src, off, dst, cols):
        for c, s, at in pieces(off):
            dst[pl.ds(at, q2), :] = src[s, pl.ds(c * q2, q2), cols]

    detours = tx_count == 8
    x_pos = lax.div(me_tx, 2)
    edge = (x_pos == 0) | (x_pos == 3)
    opposite = jnp.where(x_pos == 0, 2, 1)
    inner = jnp.where(x_pos == 0, 1, 2)
    over = (3 - x_pos) * 2 + lax.rem(me_tx, 2)
    via = pl.ds(2 * c3 + 2 * hc, c3)

    def qkv_group(off):
        stage(xp, off, xs, pl.ds(0, d))

        @pl.loop(0, 3)
        def _(n):
            cols = col(n * hc, hc)
            out = jnp.dot(xs[...], wqkv[:, :, cols].reshape(d, hc), preferred_element_type=F32).astype(BF16)
            for c, s, at in pieces(off):
                x2[s, pl.ds(c * q2, q2), cols] = out[at : at + q2]

        def hand_out(chosen):
            for c, s, _ in pieces(off):
                p, sl = lax.div(s, spd), lax.rem(s, spd)
                now = chosen(sl)
                rows = pl.ds(c * q2, q2)
                src = x2.at[s, rows, pl.ds(0, c3)]
                dst = x2.at[sl * tx_count + me_tx, rows, pl.ds(c3, c3)]
                detour = (p != p) if off > 0 or not detours else edge & (lax.div(p, 2) == opposite)

                @pl.when(now & (p == me_tx))
                def _():
                    pltpu.make_async_copy(src, dst, qkv_r.at[sl]).start()

                @pl.when(now & detour)
                def _():
                    remote(src, x2.at[s, rows, via], qkv_s, via_r.at[2 * AWAY.index(off) + c], {"tx": over}).start()

                @pl.when(now & (p != me_tx) & jnp.logical_not(detour))
                def _():
                    remote(src, dst, qkv_s, qkv_r.at[sl], {"tx": p}).start()

        if off == 2:
            hand_out(lambda sl: sl < spd // 2)
            hand_out(lambda sl: sl >= spd // 2)
        else:
            hand_out(lambda sl: sl >= 0)

    def detour_rows(off, c):
        rows = pl.ds(c * q2, q2)
        return [(s, rows) for s in ([inner * RING + wrap(tor.pos[1] + off, RING)] if c == 0 else [inner * RING + y for y in range(RING)])]

    def pass_detour(off):
        if not detours:
            return
        for c in BOTH:

            @pl.when(edge if c == 0 else edge & (wrap(tor.pos[0] + off, RING) == inner))
            def _():
                for s, rows in detour_rows(off, c):
                    view = x2.at[s, rows, via]
                    if c == 0:
                        remote(view, view, via_s, via_r.at[2 * AWAY.index(off) + c], {"tx": me_tx}).wait_recv()
                if c == 1:
                    view = x2.at[pl.ds(inner * RING, 2), :, via]
                    remote(view, view, via_s, via_r.at[2 * AWAY.index(off) + c], {"tx": me_tx}).wait_recv()
                for s, rows in detour_rows(off, c):
                    p, sl = lax.div(s, spd), lax.rem(s, spd)
                    remote(x2.at[s, rows, via], x2.at[sl * tx_count + over, rows, pl.ds(c3, c3)], via_s, qkv_r.at[sl], {"tx": p}).start()

    def drain_detours():
        if not detours:
            return
        for off in (0, -1):
            for c in BOTH:

                @pl.when(edge if c == 0 else edge & (wrap(tor.pos[0] + off, RING) == inner))
                def _():
                    view = x2.at[0, pl.ds(0, q2), via] if c == 0 else x2.at[pl.ds(0, 2), :, via]
                    remote(view, view, via_s, via_r.at[0], {"tx": me_tx}).wait_send()

    xe.drain()
    wq_r, wk_r, wv_r = rings
    g1.near()
    wq_r.step()
    g1.relay(0)
    g1.spread(-1)
    g1.spread(1)
    wk_r.step()
    wv_r.step()
    g1.halves(0)
    wq_r.step2()
    wk_r.step2()
    g1.relay(-1)
    g1.far(False)
    wv_r.step2()
    for r in rings:
        r.finish()
    qkv_group(0)
    r_o.start()
    g1.relay(1)
    g1.far(True)
    g1.halves(-1)
    qkv_group(-1)
    g1.relay(2)
    g1.halves(1)
    qkv_group(1)
    pass_detour(0)
    g1.halves(2)
    qkv_group(2)
    pass_detour(-1)
    r_o.step()

    block = min(seq, 128)
    sends = []
    for s in range(spd):
        view = x2.at[pl.ds(s * tx_count, tx_count), :, pl.ds(c3, c3)]
        remote(view, view, qkv_s, qkv_r.at[s], {"tx": me_tx}).wait_recv()

        @pl.loop(0, heads)
        def _(hd):
            def part(which):
                return x2[pl.ds(s * tx_count, tx_count), :, col(c3 + which * hc + hd * HEAD_DIM, HEAD_DIM)].reshape(seq, HEAD_DIM)

            for which in BOTH:
                v = part(which).astype(F32)
                rot = v * cos_ref[...] + pltpu.roll(v, HEAD_DIM // 2, 1) * sin_ref[...]
                kv[which] = rot.astype(BF16)
            kv[2] = part(2)
            for b in range(seq // block):
                keys = (b + 1) * block
                sc = lax.dot_general(kv[0, pl.ds(b * block, block)], kv[1, pl.ds(0, keys)], (((1,), (1,)), ((), ())), preferred_element_type=F32)
                sc = sc * HEAD_DIM ** -0.5
                q_pos = b * block + lax.broadcasted_iota(jnp.int32, (block, keys), 0)
                k_pos = lax.broadcasted_iota(jnp.int32, (block, keys), 1)
                sc = jnp.where(q_pos >= k_pos, sc, -1e30)
                e = jnp.exp(sc - jnp.max(sc, axis=-1, keepdims=True))
                prob = (e / jnp.sum(e, axis=-1, keepdims=True)).astype(BF16)
                o = jnp.dot(prob, kv[2, pl.ds(0, keys)], preferred_element_type=F32).astype(BF16)
                for n in range(block // tok):
                    at = (b * (block // tok) + n) * spd + s
                    x2[at, :, col(2 * c3 + hd * HEAD_DIM, HEAD_DIM)] = o[n * tok : (n + 1) * tok]

        oe = exchange(
            1 + s,
            lambda p, s=s: x2.at[p * spd + s, :, pl.ds(2 * c3, hc)],
            lambda o, s=s: x2.at[o * spd + s, :, pl.ds(2 * c3 + hc, hc)],
            lambda n: x2.at[pl.ds(0, n), :, pl.ds(2 * c3, hc)],
        )
        oe.start()
        sends.append(oe)

    g1.drain()
    drain_detours()
    view = x2.at[pl.ds(0, (tx_count - 1) * spd), :, pl.ds(0, c3)]
    remote(view, view, qkv_s, qkv_r.at[0], {"tx": me_tx}).wait_send()
    for oe in sends:
        oe.wait()
        oe.drain()
    r_o.step2()
    r_gate.start(place=False)
    r_up.start(place=False)
    r_down.start()
    r_o.finish()

    def put(off, x, out):
        for c, s, at in pieces(off):
            xp[s, pl.ds(c * q2, q2), col(x * dx, dx)] = out[at : at + q2]

    def o_group(off):
        stage(x2, off, os_, pl.ds(2 * c3 + hc, hc))

        @pl.loop(0, tx_count)
        def _(x):
            put(off, x, jnp.dot(os_[...], wo[x], preferred_element_type=F32).astype(BF16))

    order = (2, -1, 1, 0)
    sc1 = Scatter(tor, xp, rs_bufs, order)
    o_group(order[0])
    sc1.issue(0)
    o_group(order[1])
    sc1.issue(1)
    o_group(order[2])
    sc1.augment(0)
    sc1.issue(2)
    o_group(order[3])
    sc1.augment(1)
    sc1.issue(3)
    sc1.arrived(0)
    r_gate.step()
    sc1.augment(2)
    sc1.arrived(1)
    sc1.augment2(-1)
    sc1.augment(3)
    sc1.arrived(2)
    sc1.augment2(1)
    r_up.step()
    sc1.arrived(3)
    sc1.last()
    sc1.finish(xt, h)
    norm_rows(h, x2.at[tor.me])
    g2 = Gather(tor, x2, gs, gr)
    g2.start()
    sc1.drain()

    def mlp_group(off, between, mid):
        stage(x2, off, xs, pl.ds(0, d))
        width = 256 if fp % 256 == 0 else 128

        @pl.loop(0, fp // width)
        def _(n):
            cols = col(n * width, width)
            gate = jnp.dot(xs[...], wg[:, :, cols].reshape(d, width), preferred_element_type=F32).astype(BF16).astype(F32)
            up = jnp.dot(xs[...], wu[:, :, cols].reshape(d, width), preferred_element_type=F32).astype(BF16).astype(F32)
            act[:, cols] = (gate * jax.nn.sigmoid(gate) * up).astype(BF16)

        between()
        half = tx_count // 2
        for lo, then in ((0, mid), (half, nothing)):

            @pl.loop(lo, lo + half)
            def _(x):
                put(off, x, jnp.dot(act[...], wd[x], preferred_element_type=F32).astype(BF16))

            then()

    sc2 = Scatter(tor, xp, rs_bufs, (-1, 1, 2, 0))
    g2.near()
    r_down.step()
    g2.relay(0)
    g2.spread(-1)
    g2.spread(1)
    r_gate.step2()
    r_up.step2()
    g2.halves(0)
    r_gate.finish(place=False)
    r_up.finish(place=False)

    def onward():
        g2.relay(-1)
        g2.far(False)
        r_down.step2()
        r_down.finish()

    mlp_group(0, onward, nothing)
    g2.relay(1)
    g2.far(True)
    g2.halves(-1)
    mlp_group(-1, nothing, lambda: g2.relay(2))
    sc2.issue(0)
    g2.halves(1)
    mlp_group(1, nothing, nothing)
    sc2.issue(1)
    g2.halves(2)
    mlp_group(2, nothing, nothing)
    sc2.issue(2)
    sc2.augment(0)
    sc2.augment(1)
    sc2.issue(3)
    sc2.arrived(0)
    sc2.augment(2)
    sc2.arrived(1)
    sc2.arrived(2)
    sc2.augment(3)
    sc2.augment2(-1)
    sc2.augment2(1)
    sc2.arrived(3)
    sc2.last()
    sc2.finish(h, xt)
    ye = exchange(
        1 + spd,
        lambda p: xt.at[:, col(p * dx, dx)],
        lambda o: yr.at[pl.ds(pl.multiple_of(o * tok, tok), tok)],
        lambda n: yr.at[pl.ds(0, n * tok)],
    )
    ye.start()
    g2.drain()
    sc2.drain()
    for r in rings + [r_o, r_gate, r_up, r_down]:
        r.drain()
    ye.wait()
    out = pltpu.make_async_copy(yr, y_ref, load_sem.at[0])
    out.start()
    ye.drain()
    out.wait()


ANY_SPEC = pl.BlockSpec(memory_space=pl.ANY)


def rotary_tables(seq_len):
    half = HEAD_DIM // 2
    inv_freq = (THETA ** (-2.0 * np.arange(half) / HEAD_DIM)).astype(np.float32)
    angles = np.arange(seq_len, dtype=np.float32)[:, None] * inv_freq[None, :]
    cos_t, sin_t = np.cos(angles), np.sin(angles)
    return np.concatenate([cos_t, cos_t], -1), np.concatenate([-sin_t, sin_t], -1)


def solution(mesh):
    tx_count, n_dev = mesh.shape["tx"], mesh.shape["ty"]
    act_spec = P(("dp", "ty"), None, "tx")
    col_spec = P("tx", "ty")
    row_spec = P("ty", "tx")
    dma = pltpu.SemaphoreType.DMA

    def layer_fn(x_blk, w_q, w_k, w_v, w_o, w_gate, w_up, w_down):
        seq, dx = x_blk.shape[1:]
        hc, f = w_q.shape[1], w_gate.shape[1]
        tok, d = seq // tx_count, dx * tx_count
        fp = -(-f // 128) * 128
        rows, spd = 4 * tok, n_dev // tx_count
        cos_t, sin_t = rotary_tables(seq)
        bf = lambda *shape: pltpu.VMEM(shape, BF16)
        scratch = [
            bf(n_dev, tok, d), bf(n_dev, tok, d), bf(tx_count, dx, 3 * hc), bf(tx_count, hc, dx),
            bf(tx_count, dx, fp), bf(tx_count, dx, fp), bf(tx_count, fp, dx),
            bf(rows, d), bf(rows, hc), bf(rows, fp), bf(3, seq, HEAD_DIM), bf(tok, d), bf(tok, d), bf(seq, dx),
            pltpu.VMEM((seq, HEAD_DIM), F32), pltpu.VMEM((seq, HEAD_DIM), F32),
            dma((5,)), dma((spd + 2,)), dma((spd + 2,)), dma, dma((spd,)), dma, dma((4,)),
            dma, dma((Gather.SEMS,)), dma((7,)), dma((7, Ring.SEMS)),
        ] + Scatter.buffers(tok, d)
        y = pl.pallas_call(
            functools.partial(layer_kernel, tx_count),
            name="layer",
            out_shape=jax.ShapeDtypeStruct((seq, dx), BF16),
            in_specs=[ANY_SPEC] * 10,
            out_specs=ANY_SPEC,
            scratch_shapes=scratch,
            compiler_params=pltpu.CompilerParams(collective_id=1, has_side_effects=True, vmem_limit_bytes=67043328),
        )(x_blk[0], w_q, w_k, w_v, w_o, w_gate.T, w_up.T, w_down, cos_t, sin_t)
        return y[None]

    return jax.shard_map(layer_fn, mesh=mesh, in_specs=(act_spec, col_spec, col_spec, col_spec, row_spec, col_spec, col_spec, row_spec), out_specs=act_spec, check_vma=False)
```

```python
import functools

import numpy as np
import jax
import jax.numpy as jnp
from jax import lax
from jax.experimental import pallas as pl
from jax.experimental.pallas import tpu as pltpu
from jax.sharding import PartitionSpec as P

HEAD_DIM = 128
EPS = 1e-5
THETA = 10000.0
RING = 4
BOTH = (0, 1)
DIRS = (1, -1)
MESH = pl.DeviceIdType.MESH
BF16 = jnp.bfloat16
F32 = jnp.float32
AWAY = (0, -1, 1, 2)


def nothing():
    pass


def wrap(v, n):
    return lax.rem(v + 2 * n, n)


class Torus:
    def __init__(self):
        t = lax.axis_index("ty")
        self.me = t
        self.pos = (lax.div(t, RING), lax.rem(t, RING))

    def slot(self, first, a_off, b_off):
        a = wrap(self.pos[first] + a_off, RING)
        b = wrap(self.pos[1 - first] + b_off, RING)
        return a * RING + b if first == 0 else b * RING + a


def entry_barrier(tor, tx_count):
    sem = pltpu.get_barrier_semaphore()
    for first in (0, 1):
        for d in DIRS:
            pl.semaphore_signal(sem, inc=1, device_id={"ty": tor.slot(first, d, 0)}, device_id_type=MESH)
    me = lax.axis_index("tx")
    for k in range(1, tx_count):
        pl.semaphore_signal(sem, inc=1, device_id={"tx": lax.rem(me + k, tx_count)}, device_id_type=MESH)
    pl.semaphore_wait(sem, 4 + tx_count - 1)


def remote(src, dst, ssem, rsem, device):
    return pltpu.make_async_remote_copy(src_ref=src, dst_ref=dst, send_sem=ssem, recv_sem=rsem, device_id=device, device_id_type=MESH)


class Gather:
    SEMS = 25

    def __init__(self, tor, buf, ssem, rsem):
        self.tor, self.buf, self.ssem, self.rsem = tor, buf, ssem, rsem
        self.q = buf.shape[1] // 4

    def first(self, c):
        return 1 if c == 0 else 0

    def rows(self, c, d, half):
        if not half:
            return pl.ds(c * 2 * self.q, 2 * self.q)
        return pl.ds(c * 2 * self.q + (0 if d == 1 else self.q), self.q)

    def sem(self, c, ph, off, d, half):
        if half:
            return 20 + (0 if ph == 1 else 1 + AWAY.index(off))
        return (0 if ph == 1 else 4 + 4 * AWAY.index(off)) + c * 2 + (0 if d == 1 else 1)

    def copy(self, c, ph, off, d, half, hops):
        first = self.first(c)
        back = -d * hops
        s = self.tor.slot(first, back, 0) if ph == 1 else self.tor.slot(first, off, back)
        to = self.tor.slot(first, d, 0) if ph == 1 else self.tor.slot(first, 0, d)
        view = self.buf.at[s, self.rows(c, d, half)]
        return remote(view, view, self.ssem, self.rsem.at[self.sem(c, ph, off, d, half)], {"ty": to})

    def send(self, c, ph, off, d, half=False):
        self.copy(c, ph, off, d, half, 1 if half else 0).start()

    def recv(self, c, ph, off, d):
        self.copy(c, ph, off, d, False, 1).wait_recv()

    def far_copy(self, c, d, second, hops):
        s = self.tor.slot(self.first(c), 2, -d * hops)
        view = self.buf.at[s, self.rows(c, -d if second else d, True)]
        i = self.sem(c, 2, 2, d, second)
        return remote(view, view, self.ssem, self.rsem.at[i], {"ty": self.tor.slot(self.first(c), 0, d)})

    def recv_halves(self, ph, off):
        view = self.buf.at[pl.ds(0, 2)] if ph == off == 2 else self.buf.at[0]
        remote(view, view, self.ssem, self.rsem.at[self.sem(0, ph, off, 1, True)], {"ty": self.tor.me}).wait_recv()

    def start(self):
        for ph in (1, 2):
            for c in BOTH:
                for d in DIRS:
                    self.send(c, ph, 0, d)

    def near(self):
        for d in DIRS:
            for c in BOTH:
                self.recv(c, 1, 0, d)
                self.send(c, 1, 0, d, True)

    def spread(self, off):
        for c in BOTH:
            for d in DIRS:
                self.send(c, 2, off, d)

    def relay(self, off):
        for d in DIRS:
            for c in BOTH:
                if off == 2:
                    self.far_copy(c, d, False, 1).wait_recv()
                else:
                    self.recv(c, 2, off, d)
                self.send(c, 2, off, d, True)

    def far(self, second):
        if not second:
            self.recv_halves(1, 0)
        for c in BOTH:
            for d in DIRS:
                self.far_copy(c, d, second, 0).start()

    def halves(self, off):
        self.recv_halves(2, off)

    def drain(self):
        view = self.buf.at[pl.ds(0, self.buf.shape[0] - 1)]
        remote(view, view, self.ssem, self.rsem.at[0], {"ty": self.tor.me}).wait_send()


def add_rows(dst, srcs, width=512):
    d = dst.shape[-1]
    width = min(width, d)

    @pl.loop(0, d // width)
    def _(i):
        cols = pl.ds(pl.multiple_of(i * width, width), width)
        tot = srcs[0][:, cols].astype(F32)
        for s in srcs[1:]:
            tot += s[:, cols].astype(F32)
        dst[:, cols] = tot.astype(dst.dtype)


class Scatter:
    SEMS = 30

    @staticmethod
    def buffers(tok, d):
        q = tok // 4
        return [
            pltpu.VMEM((2, 4, 2, q, d), BF16),
            pltpu.VMEM((2, 4, 2, 2 * q, d), BF16),
            pltpu.VMEM((2, 3, 2 * q, d), BF16),
            pltpu.VMEM((2, 2, q, d), BF16),
            pltpu.VMEM((2, 2, 2 * q, d), BF16),
            pltpu.SemaphoreType.DMA,
            pltpu.SemaphoreType.DMA((Scatter.SEMS,)),
        ]

    def __init__(self, tor, part, bufs, order):
        self.tor, self.part, self.order = tor, part, order
        self.h1, self.f1, self.mid, self.h2, self.f2, self.ssem, self.rsem = bufs
        self.q = part.shape[1] // 4

    def copy(self, c, ph, bi, d, kind):
        q, first = self.q, c
        di = 0 if d == 1 else 1
        h = di if kind in (0, 2) else 1 - di
        step = 2 * d if kind == 0 else d
        if ph == 1:
            i = c * 8 + bi * 2 + di if kind == 0 else 16 + c * 4 + bi
            src = self.part.at[self.tor.slot(first, step, self.order[bi]), pl.ds(c * 2 * q + h * q, q)]
            dst = self.h1.at[c, bi, di] if kind == 0 else self.f1.at[c, bi, di, pl.ds(h * q, q)]
            to = self.tor.slot(first, d, 0)
        else:
            i = 24 + c * 2 + di if kind == 0 else 28 + c
            src = self.mid.at[c, self.order.index(2 if kind == 0 else d), pl.ds(h * q, q)]
            dst = self.h2.at[c, di] if kind == 0 else self.f2.at[c, di, pl.ds(h * q, q)]
            to = self.tor.slot(first, 0, d)
        return remote(src, dst, self.ssem, self.rsem.at[i], {"ty": to})

    def all_of(self, view, i):
        remote(view, view, self.ssem, self.rsem.at[i], {"ty": self.tor.me}).wait_recv()

    def issue(self, bi):
        for kind in BOTH:
            for c in BOTH:
                for d in DIRS:
                    self.copy(c, 1, bi, d, kind).start()

    def augment(self, bi):
        q = self.q
        for c in BOTH:
            for d in DIRS:
                di = 0 if d == 1 else 1
                self.copy(c, 1, bi, d, 0).wait_recv()
                mine = self.part.at[self.tor.slot(c, d, self.order[bi]), pl.ds(c * 2 * q + di * q, q)]
                add_rows(mine, [mine, self.h1.at[c, bi, di]])
                self.copy(c, 1, bi, d, 2).start()

    def arrived(self, bi):
        q = self.q
        for c in BOTH:
            self.all_of(self.f1.at[c, bi], 16 + c * 4 + bi)
            off = self.order[bi]
            if off == 0:
                continue
            own = self.part.at[self.tor.slot(c, 0, off), pl.ds(c * 2 * q, 2 * q)]
            add_rows(self.mid.at[c, bi], [own, self.f1.at[c, bi, 0], self.f1.at[c, bi, 1]])
            if off == 2:
                for d in DIRS:
                    self.copy(c, 2, 0, d, 0).start()
            else:
                self.copy(c, 2, 0, off, 1).start()

    def augment2(self, d):
        q = self.q
        di = 0 if d == 1 else 1
        for c in BOTH:
            self.copy(c, 2, 0, d, 0).wait_recv()
            mine = self.mid.at[c, self.order.index(d), pl.ds(di * q, q)]
            add_rows(mine, [mine, self.h2.at[c, di]])
            self.copy(c, 2, 0, d, 2).start()

    def last(self):
        for c in BOTH:
            self.all_of(self.f2.at[c], 28 + c)

    def finish(self, resid, out):
        q, d = self.q, out.shape[-1]
        width = min(512, d)
        for c in BOTH:
            rows = pl.ds(c * 2 * q, 2 * q)

            @pl.loop(0, d // width)
            def _(i):
                cols = pl.ds(pl.multiple_of(i * width, width), width)
                tot = self.part[self.tor.me, rows, cols].astype(F32)
                for di in BOTH:
                    tot += self.f1[c, self.order.index(0), di, :, cols].astype(F32)
                for di in BOTH:
                    tot += self.f2[c, di, :, cols].astype(F32)
                tot = tot.astype(BF16).astype(F32)
                out[rows, cols] = (resid[rows, cols].astype(F32) + tot).astype(BF16)

    def drain(self):
        view = self.part.at[pl.ds(0, self.part.shape[0] - 1)]
        remote(view, view, self.ssem, self.rsem.at[0], {"ty": self.tor.me}).wait_send()


class Exchange:
    def __init__(self, tx_count, src, dst, whole, ssem, rsem):
        self.n, self.src, self.dst, self.whole, self.ssem, self.rsem = tx_count, src, dst, whole, ssem, rsem
        self.me = lax.axis_index("tx")

    def start(self):
        for k in range(1, self.n):
            p = lax.rem(self.me + k, self.n)
            remote(self.src(p), self.dst(self.me), self.ssem, self.rsem, {"tx": p}).start()
        pltpu.make_async_copy(self.src(self.me), self.dst(self.me), self.rsem).start()

    def wait(self):
        view = self.whole(self.n)
        remote(view, view, self.ssem, self.rsem, {"tx": self.me}).wait_recv()

    def drain(self):
        view = self.whole(self.n - 1)
        remote(view, view, self.ssem, self.rsem, {"tx": self.me}).wait_send()


def norm_rows(src, dst):
    tok, d = src.shape
    step = 16

    @pl.loop(0, tok // step)
    def _(i):
        rows = pl.ds(pl.multiple_of(i * step, step), step)
        v = src[rows, :].astype(F32)
        mean = jnp.sum(v, axis=-1, keepdims=True) * (1.0 / d)
        var = jnp.sum(v * v, axis=-1, keepdims=True) * (1.0 / d) - mean * mean
        dst[rows, :] = ((v - mean) * lax.rsqrt(var + EPS)).astype(BF16)


class Ring:
    SEMS = 5

    def __init__(self, tx_count, rows, src, slot, whole, ssem, rsem):
        self.nx, self.rows, self.src, self.slot, self.whole, self.ssem, self.rsem = tx_count // 2, rows, src, slot, whole, ssem, rsem
        me = lax.axis_index("tx")
        self.me, self.x, self.core = me, lax.div(me, 2), lax.rem(me, 2)
        self.split = (rows // 2 + 15) // 16 * 16

    def tx(self, dx, other=False):
        return wrap(self.x + dx, self.nx) * 2 + (1 - self.core if other else self.core)

    def half(self, view, d):
        return view.at[pl.ds(0, self.split)] if d == 1 else view.at[pl.ds(self.split, self.rows - self.split)]

    def copy(self, i, src, dst, to):
        return remote(src, dst, self.ssem, self.rsem.at[i], {"tx": to})

    def pass_on(self, d, recv=False):
        view = self.slot(self.tx(-d if recv else 0))
        return self.copy(0 if d == 1 else 1, view if recv else self.src, view, self.tx(d))

    def relay(self, d, recv=False):
        view = self.half(self.slot(self.tx(-2 * d if recv else -d)), d)
        return self.copy(2 if d == 1 else 3, view, view, self.tx(d))

    def across(self, which, recv=False):
        view = self.slot(self.tx(which, recv))
        if abs(which) == 2:
            view = self.half(view, which // 2)
        src = self.src if which == 0 and not recv else view
        return self.copy(4, src, view, self.tx(0, True))

    def all_across(self):
        return (0, 1, -1, 2, -2) if self.nx > 1 else (0,)

    def own(self):
        return pltpu.make_async_copy(self.src, self.slot(self.me), self.rsem.at[4])

    def start(self, place=True):
        if self.nx > 1:
            for d in DIRS:
                self.pass_on(d).start()
        self.across(0).start()
        if place:
            self.own().start()

    def step(self):
        if self.nx > 1:
            for d in DIRS:
                self.pass_on(d, True).wait_recv()
                self.relay(d).start()
                self.across(-d).start()

    def step2(self):
        if self.nx > 1:
            for d in DIRS:
                self.relay(d, True).wait_recv()
                self.across(2 * d).start()

    def finish(self, place=True):
        view = self.whole(self.nx + (1 if place else 0))
        remote(view, view, self.ssem, self.rsem.at[4], {"tx": self.me}).wait_recv()

    def drain(self):
        view = self.whole(2 * self.nx - 1)
        remote(view, view, self.ssem, self.rsem.at[4], {"tx": self.me}).wait_send()


def layer_kernel(tx_count, x_ref, wq_ref, wk_ref, wv_ref, wo_ref, wg_ref, wu_ref, wd_ref, cos_hbm, sin_hbm, y_ref,
                 xp, x2, wqkv, wo, wg, wu, wd, xs, os_, act, kv, xt, h, yr, cos_ref, sin_ref,
                 load_sem, a2a_s, a2a_r, qkv_s, qkv_r, via_s, via_r, gs, gr, ws, wr, *rs_bufs):
    n_dev, tok, d = xp.shape
    dx = x_ref.shape[1]
    hc = wq_ref.shape[1]
    f, fp = wg_ref.shape[0], wg.shape[2]
    seq = tok * tx_count
    spd = n_dev // tx_count
    heads = hc // HEAD_DIM
    q2 = tok // 2
    c3 = 3 * hc
    tor = Torus()
    me_tx = lax.axis_index("tx")

    def exchange(i, src, dst, whole):
        return Exchange(tx_count, src, dst, whole, a2a_s.at[i], a2a_r.at[i])

    def col(start, width):
        return pl.ds(pl.multiple_of(start, width), width)

    def ring(i, src, buf, inner):
        return Ring(tx_count, src.shape[0], src, lambda o: buf.at[(o, *inner)], lambda n: buf.at[(pl.ds(0, n), *inner)], ws.at[i], wr.at[i])

    every = pl.ds(0, dx)
    rings = [ring(i, src, wqkv, (every, pl.ds(i * hc, hc))) for i, src in enumerate((wq_ref, wk_ref, wv_ref))]
    r_o = ring(3, wo_ref, wo, ())
    r_gate = ring(4, wg.at[me_tx], wg, ())
    r_up = ring(5, wu.at[me_tx], wu, ())
    r_down = ring(6, wd_ref, wd, (pl.ds(0, f),))

    x_in = pltpu.make_async_copy(x_ref, yr, load_sem.at[2])
    x_in.start()
    raw = [pltpu.make_async_copy(src, wd.at[i, pl.ds(0, f)], load_sem.at[i]) for i, src in enumerate((wg_ref, wu_ref))]
    raw += [pltpu.make_async_copy(cos_hbm, cos_ref, load_sem.at[3]), pltpu.make_async_copy(sin_hbm, sin_ref, load_sem.at[4])]
    for cp in raw:
        cp.start()
    entry_barrier(tor, tx_count)
    x_in.wait()
    xe = exchange(
        0,
        lambda p: yr.at[pl.ds(pl.multiple_of(p * tok, tok), tok)],
        lambda o: xt.at[:, col(o * dx, dx)],
        lambda n: yr.at[pl.ds(0, n * tok)],
    )
    xe.start()
    if fp > f:
        wd[:, pl.ds(f, fp - f), :] = jnp.zeros((tx_count, fp - f, dx), BF16)
    xe.wait()
    norm_rows(xt, xp.at[tor.me])
    g1 = Gather(tor, xp, gs, gr)
    g1.start()
    for r in rings:
        r.start()
    for cp in raw:
        cp.wait()
    for i, dst in enumerate((wg, wu)):
        for j in range(fp // 128):
            dst[me_tx, :, pl.ds(j * 128, 128)] = wd[i, pl.ds(j * 128, 128), :].T

    def pieces(off):
        return [(c, tor.slot(1 - c, off, n), (c * 4 + n) * q2) for c in BOTH for n in range(RING)]

    def stage(src, off, dst, cols):
        for c, s, at in pieces(off):
            dst[pl.ds(at, q2), :] = src[s, pl.ds(c * q2, q2), cols]

    detours = tx_count == 8
    x_pos = lax.div(me_tx, 2)
    edge = (x_pos == 0) | (x_pos == 3)
    opposite = jnp.where(x_pos == 0, 2, 1)
    inner = jnp.where(x_pos == 0, 1, 2)
    over = (3 - x_pos) * 2 + lax.rem(me_tx, 2)
    via = pl.ds(2 * c3 + 2 * hc, c3)

    def qkv_group(off):
        stage(xp, off, xs, pl.ds(0, d))

        @pl.loop(0, 3)
        def _(n):
            cols = col(n * hc, hc)
            out = jnp.dot(xs[...], wqkv[:, :, cols].reshape(d, hc), preferred_element_type=F32).astype(BF16)
            for c, s, at in pieces(off):
                x2[s, pl.ds(c * q2, q2), cols] = out[at : at + q2]

        def hand_out(chosen):
            for c, s, _ in pieces(off):
                p, sl = lax.div(s, spd), lax.rem(s, spd)
                now = chosen(sl)
                rows = pl.ds(c * q2, q2)
                src = x2.at[s, rows, pl.ds(0, c3)]
                dst = x2.at[sl * tx_count + me_tx, rows, pl.ds(c3, c3)]
                detour = (p != p) if off > 0 or not detours else edge & (lax.div(p, 2) == opposite)

                @pl.when(now & (p == me_tx))
                def _():
                    pltpu.make_async_copy(src, dst, qkv_r.at[sl]).start()

                @pl.when(now & detour)
                def _():
                    remote(src, x2.at[s, rows, via], qkv_s, via_r.at[2 * AWAY.index(off) + c], {"tx": over}).start()

                @pl.when(now & (p != me_tx) & jnp.logical_not(detour))
                def _():
                    remote(src, dst, qkv_s, qkv_r.at[sl], {"tx": p}).start()

        if off == 2:
            hand_out(lambda sl: sl < spd // 2)
            hand_out(lambda sl: sl >= spd // 2)
        else:
            hand_out(lambda sl: sl >= 0)

    def detour_rows(off, c):
        rows = pl.ds(c * q2, q2)
        return [(s, rows) for s in ([inner * RING + wrap(tor.pos[1] + off, RING)] if c == 0 else [inner * RING + y for y in range(RING)])]

    def pass_detour(off):
        if not detours:
            return
        for c in BOTH:

            @pl.when(edge if c == 0 else edge & (wrap(tor.pos[0] + off, RING) == inner))
            def _():
                for s, rows in detour_rows(off, c):
                    view = x2.at[s, rows, via]
                    if c == 0:
                        remote(view, view, via_s, via_r.at[2 * AWAY.index(off) + c], {"tx": me_tx}).wait_recv()
                if c == 1:
                    view = x2.at[pl.ds(inner * RING, 2), :, via]
                    remote(view, view, via_s, via_r.at[2 * AWAY.index(off) + c], {"tx": me_tx}).wait_recv()
                for s, rows in detour_rows(off, c):
                    p, sl = lax.div(s, spd), lax.rem(s, spd)
                    remote(x2.at[s, rows, via], x2.at[sl * tx_count + over, rows, pl.ds(c3, c3)], via_s, qkv_r.at[sl], {"tx": p}).start()

    def drain_detours():
        if not detours:
            return
        for off in (0, -1):
            for c in BOTH:

                @pl.when(edge if c == 0 else edge & (wrap(tor.pos[0] + off, RING) == inner))
                def _():
                    view = x2.at[0, pl.ds(0, q2), via] if c == 0 else x2.at[pl.ds(0, 2), :, via]
                    remote(view, view, via_s, via_r.at[0], {"tx": me_tx}).wait_send()

    xe.drain()
    wq_r, wk_r, wv_r = rings
    g1.near()
    wq_r.step()
    g1.relay(0)
    g1.spread(-1)
    g1.spread(1)
    wk_r.step()
    wv_r.step()
    g1.halves(0)
    wq_r.step2()
    wk_r.step2()
    g1.relay(-1)
    g1.far(False)
    wv_r.step2()
    for r in rings:
        r.finish()
    qkv_group(0)
    g1.relay(1)
    g1.far(True)
    g1.halves(-1)
    qkv_group(-1)
    g1.relay(2)
    g1.halves(1)
    qkv_group(1)
    pass_detour(0)
    g1.halves(2)
    qkv_group(2)
    pass_detour(-1)
    r_o.start()

    block = min(seq, 128)
    sends = []
    for s in range(spd):
        view = x2.at[pl.ds(s * tx_count, tx_count), :, pl.ds(c3, c3)]
        remote(view, view, qkv_s, qkv_r.at[s], {"tx": me_tx}).wait_recv()

        @pl.loop(0, heads)
        def _(hd):
            def part(which):
                return x2[pl.ds(s * tx_count, tx_count), :, col(c3 + which * hc + hd * HEAD_DIM, HEAD_DIM)].reshape(seq, HEAD_DIM)

            for which in BOTH:
                v = part(which).astype(F32)
                rot = v * cos_ref[...] + pltpu.roll(v, HEAD_DIM // 2, 1) * sin_ref[...]
                kv[which] = rot.astype(BF16)
            kv[2] = part(2)
            for b in range(seq // block):
                keys = (b + 1) * block
                sc = lax.dot_general(kv[0, pl.ds(b * block, block)], kv[1, pl.ds(0, keys)], (((1,), (1,)), ((), ())), preferred_element_type=F32)
                sc = sc * HEAD_DIM ** -0.5
                q_pos = b * block + lax.broadcasted_iota(jnp.int32, (block, keys), 0)
                k_pos = lax.broadcasted_iota(jnp.int32, (block, keys), 1)
                sc = jnp.where(q_pos >= k_pos, sc, -1e30)
                e = jnp.exp(sc - jnp.max(sc, axis=-1, keepdims=True))
                prob = (e / jnp.sum(e, axis=-1, keepdims=True)).astype(BF16)
                o = jnp.dot(prob, kv[2, pl.ds(0, keys)], preferred_element_type=F32).astype(BF16)
                for n in range(block // tok):
                    at = (b * (block // tok) + n) * spd + s
                    x2[at, :, col(2 * c3 + hd * HEAD_DIM, HEAD_DIM)] = o[n * tok : (n + 1) * tok]

        oe = exchange(
            1 + s,
            lambda p, s=s: x2.at[p * spd + s, :, pl.ds(2 * c3, hc)],
            lambda o, s=s: x2.at[o * spd + s, :, pl.ds(2 * c3 + hc, hc)],
            lambda n: x2.at[pl.ds(0, n), :, pl.ds(2 * c3, hc)],
        )
        oe.start()
        sends.append(oe)

    r_o.step()
    g1.drain()
    drain_detours()
    view = x2.at[pl.ds(0, (tx_count - 1) * spd), :, pl.ds(0, c3)]
    remote(view, view, qkv_s, qkv_r.at[0], {"tx": me_tx}).wait_send()
    for oe in sends:
        oe.wait()
        oe.drain()
    r_o.step2()
    r_gate.start(place=False)
    r_up.start(place=False)
    r_down.start()
    r_o.finish()

    def put(off, x, out):
        for c, s, at in pieces(off):
            xp[s, pl.ds(c * q2, q2), col(x * dx, dx)] = out[at : at + q2]

    def o_group(off):
        stage(x2, off, os_, pl.ds(2 * c3 + hc, hc))

        @pl.loop(0, tx_count)
        def _(x):
            put(off, x, jnp.dot(os_[...], wo[x], preferred_element_type=F32).astype(BF16))

    order = (2, -1, 1, 0)
    sc1 = Scatter(tor, xp, rs_bufs, order)
    o_group(order[0])
    sc1.issue(0)
    o_group(order[1])
    sc1.issue(1)
    o_group(order[2])
    sc1.augment(0)
    sc1.issue(2)
    o_group(order[3])
    sc1.augment(1)
    sc1.issue(3)
    sc1.arrived(0)
    r_gate.step()
    sc1.augment(2)
    sc1.arrived(1)
    sc1.augment2(-1)
    sc1.augment(3)
    sc1.arrived(2)
    sc1.augment2(1)
    r_up.step()
    sc1.arrived(3)
    sc1.last()
    sc1.finish(xt, h)
    norm_rows(h, x2.at[tor.me])
    g2 = Gather(tor, x2, gs, gr)
    g2.start()
    sc1.drain()

    def mlp_group(off, between, mid):
        stage(x2, off, xs, pl.ds(0, d))
        width = 256 if fp % 256 == 0 else 128

        @pl.loop(0, fp // width)
        def _(n):
            cols = col(n * width, width)
            gate = jnp.dot(xs[...], wg[:, :, cols].reshape(d, width), preferred_element_type=F32).astype(BF16).astype(F32)
            up = jnp.dot(xs[...], wu[:, :, cols].reshape(d, width), preferred_element_type=F32).astype(BF16).astype(F32)
            act[:, cols] = (gate * jax.nn.sigmoid(gate) * up).astype(BF16)

        between()
        half = tx_count // 2
        for lo, then in ((0, mid), (half, nothing)):

            @pl.loop(lo, lo + half)
            def _(x):
                put(off, x, jnp.dot(act[...], wd[x], preferred_element_type=F32).astype(BF16))

            then()

    sc2 = Scatter(tor, xp, rs_bufs, (-1, 1, 2, 0))
    g2.near()
    r_down.step()
    g2.relay(0)
    g2.spread(-1)
    g2.spread(1)
    r_gate.step2()
    r_up.step2()
    g2.halves(0)
    r_gate.finish(place=False)
    r_up.finish(place=False)

    def onward():
        g2.relay(-1)
        g2.far(False)
        r_down.step2()
        r_down.finish()

    mlp_group(0, onward, nothing)
    g2.relay(1)
    g2.far(True)
    g2.halves(-1)
    mlp_group(-1, nothing, lambda: g2.relay(2))
    sc2.issue(0)
    g2.halves(1)
    mlp_group(1, nothing, nothing)
    sc2.issue(1)
    g2.halves(2)
    mlp_group(2, nothing, nothing)
    sc2.issue(2)
    sc2.augment(0)
    sc2.augment(1)
    sc2.issue(3)
    sc2.arrived(0)
    sc2.augment(2)
    sc2.arrived(1)
    sc2.arrived(2)
    sc2.augment(3)
    sc2.augment2(-1)
    sc2.augment2(1)
    sc2.arrived(3)
    sc2.last()
    sc2.finish(h, xt)
    ye = exchange(
        1 + spd,
        lambda p: xt.at[:, col(p * dx, dx)],
        lambda o: yr.at[pl.ds(pl.multiple_of(o * tok, tok), tok)],
        lambda n: yr.at[pl.ds(0, n * tok)],
    )
    ye.start()
    g2.drain()
    sc2.drain()
    for r in rings + [r_o, r_gate, r_up, r_down]:
        r.drain()
    ye.wait()
    out = pltpu.make_async_copy(yr, y_ref, load_sem.at[0])
    out.start()
    ye.drain()
    out.wait()


ANY_SPEC = pl.BlockSpec(memory_space=pl.ANY)


def rotary_tables(seq_len):
    half = HEAD_DIM // 2
    inv_freq = (THETA ** (-2.0 * np.arange(half) / HEAD_DIM)).astype(np.float32)
    angles = np.arange(seq_len, dtype=np.float32)[:, None] * inv_freq[None, :]
    cos_t, sin_t = np.cos(angles), np.sin(angles)
    return np.concatenate([cos_t, cos_t], -1), np.concatenate([-sin_t, sin_t], -1)


def solution(mesh):
    tx_count, n_dev = mesh.shape["tx"], mesh.shape["ty"]
    act_spec = P(("dp", "ty"), None, "tx")
    col_spec = P("tx", "ty")
    row_spec = P("ty", "tx")
    dma = pltpu.SemaphoreType.DMA

    def layer_fn(x_blk, w_q, w_k, w_v, w_o, w_gate, w_up, w_down):
        seq, dx = x_blk.shape[1:]
        hc, f = w_q.shape[1], w_gate.shape[1]
        tok, d = seq // tx_count, dx * tx_count
        fp = -(-f // 128) * 128
        rows, spd = 4 * tok, n_dev // tx_count
        cos_t, sin_t = rotary_tables(seq)
        bf = lambda *shape: pltpu.VMEM(shape, BF16)
        scratch = [
            bf(n_dev, tok, d), bf(n_dev, tok, d), bf(tx_count, dx, 3 * hc), bf(tx_count, hc, dx),
            bf(tx_count, dx, fp), bf(tx_count, dx, fp), bf(tx_count, fp, dx),
            bf(rows, d), bf(rows, hc), bf(rows, fp), bf(3, seq, HEAD_DIM), bf(tok, d), bf(tok, d), bf(seq, dx),
            pltpu.VMEM((seq, HEAD_DIM), F32), pltpu.VMEM((seq, HEAD_DIM), F32),
            dma((5,)), dma((spd + 2,)), dma((spd + 2,)), dma, dma((spd,)), dma, dma((4,)),
            dma, dma((Gather.SEMS,)), dma((7,)), dma((7, Ring.SEMS)),
        ] + Scatter.buffers(tok, d)
        y = pl.pallas_call(
            functools.partial(layer_kernel, tx_count),
            name="layer",
            out_shape=jax.ShapeDtypeStruct((seq, dx), BF16),
            in_specs=[ANY_SPEC] * 10,
            out_specs=ANY_SPEC,
            scratch_shapes=scratch,
            compiler_params=pltpu.CompilerParams(collective_id=1, has_side_effects=True, vmem_limit_bytes=67043328),
        )(x_blk[0], w_q, w_k, w_v, w_o, w_gate.T, w_up.T, w_down, cos_t, sin_t)
        return y[None]

    return jax.shard_map(layer_fn, mesh=mesh, in_specs=(act_spec, col_spec, col_spec, col_spec, row_spec, col_spec, col_spec, row_spec), out_specs=act_spec, check_vma=False)
```

```python
import functools

import numpy as np
import jax
import jax.numpy as jnp
from jax import lax
from jax.experimental import pallas as pl
from jax.experimental.pallas import tpu as pltpu
from jax.sharding import PartitionSpec as P

HEAD_DIM = 128
EPS = 1e-5
THETA = 10000.0
RING = 4
BOTH = (0, 1)
DIRS = (1, -1)
MESH = pl.DeviceIdType.MESH
BF16 = jnp.bfloat16
F32 = jnp.float32
AWAY = (0, -1, 1, 2)


def nothing():
    pass


def wrap(v, n):
    return lax.rem(v + 2 * n, n)


class Torus:
    def __init__(self):
        t = lax.axis_index("ty")
        self.me = t
        self.pos = (lax.div(t, RING), lax.rem(t, RING))

    def slot(self, first, a_off, b_off):
        a = wrap(self.pos[first] + a_off, RING)
        b = wrap(self.pos[1 - first] + b_off, RING)
        return a * RING + b if first == 0 else b * RING + a


def entry_barrier(tor, tx_count):
    sem = pltpu.get_barrier_semaphore()
    for first in (0, 1):
        for d in DIRS:
            pl.semaphore_signal(sem, inc=1, device_id={"ty": tor.slot(first, d, 0)}, device_id_type=MESH)
    me = lax.axis_index("tx")
    for k in range(1, tx_count):
        pl.semaphore_signal(sem, inc=1, device_id={"tx": lax.rem(me + k, tx_count)}, device_id_type=MESH)
    pl.semaphore_wait(sem, 4 + tx_count - 1)


def remote(src, dst, ssem, rsem, device):
    return pltpu.make_async_remote_copy(src_ref=src, dst_ref=dst, send_sem=ssem, recv_sem=rsem, device_id=device, device_id_type=MESH)


class Gather:
    SEMS = 25

    def __init__(self, tor, buf, ssem, rsem):
        self.tor, self.buf, self.ssem, self.rsem = tor, buf, ssem, rsem
        self.q = buf.shape[1] // 4

    def first(self, c):
        return 1 if c == 0 else 0

    def rows(self, c, d, half):
        if not half:
            return pl.ds(c * 2 * self.q, 2 * self.q)
        return pl.ds(c * 2 * self.q + (0 if d == 1 else self.q), self.q)

    def sem(self, c, ph, off, d, half):
        if half:
            return 20 + (0 if ph == 1 else 1 + AWAY.index(off))
        return (0 if ph == 1 else 4 + 4 * AWAY.index(off)) + c * 2 + (0 if d == 1 else 1)

    def copy(self, c, ph, off, d, half, hops):
        first = self.first(c)
        back = -d * hops
        s = self.tor.slot(first, back, 0) if ph == 1 else self.tor.slot(first, off, back)
        to = self.tor.slot(first, d, 0) if ph == 1 else self.tor.slot(first, 0, d)
        view = self.buf.at[s, self.rows(c, d, half)]
        return remote(view, view, self.ssem, self.rsem.at[self.sem(c, ph, off, d, half)], {"ty": to})

    def send(self, c, ph, off, d, half=False):
        self.copy(c, ph, off, d, half, 1 if half else 0).start()

    def recv(self, c, ph, off, d):
        self.copy(c, ph, off, d, False, 1).wait_recv()

    def far_copy(self, c, d, second, hops):
        s = self.tor.slot(self.first(c), 2, -d * hops)
        view = self.buf.at[s, self.rows(c, -d if second else d, True)]
        i = self.sem(c, 2, 2, d, second)
        return remote(view, view, self.ssem, self.rsem.at[i], {"ty": self.tor.slot(self.first(c), 0, d)})

    def recv_halves(self, ph, off):
        view = self.buf.at[pl.ds(0, 2)] if ph == off == 2 else self.buf.at[0]
        remote(view, view, self.ssem, self.rsem.at[self.sem(0, ph, off, 1, True)], {"ty": self.tor.me}).wait_recv()

    def start(self):
        for ph in (1, 2):
            for c in BOTH:
                for d in DIRS:
                    self.send(c, ph, 0, d)

    def near(self):
        for d in DIRS:
            for c in BOTH:
                self.recv(c, 1, 0, d)
                self.send(c, 1, 0, d, True)

    def spread(self, off):
        for c in BOTH:
            for d in DIRS:
                self.send(c, 2, off, d)

    def relay(self, off):
        for d in DIRS:
            for c in BOTH:
                if off == 2:
                    self.far_copy(c, d, False, 1).wait_recv()
                else:
                    self.recv(c, 2, off, d)
                self.send(c, 2, off, d, True)

    def far(self, second):
        if not second:
            self.recv_halves(1, 0)
        for c in BOTH:
            for d in DIRS:
                self.far_copy(c, d, second, 0).start()

    def halves(self, off):
        self.recv_halves(2, off)

    def drain(self):
        view = self.buf.at[pl.ds(0, self.buf.shape[0] - 1)]
        remote(view, view, self.ssem, self.rsem.at[0], {"ty": self.tor.me}).wait_send()


def add_rows(dst, srcs, width=512):
    d = dst.shape[-1]
    width = min(width, d)

    @pl.loop(0, d // width)
    def _(i):
        cols = pl.ds(pl.multiple_of(i * width, width), width)
        tot = srcs[0][:, cols].astype(F32)
        for s in srcs[1:]:
            tot += s[:, cols].astype(F32)
        dst[:, cols] = tot.astype(dst.dtype)


class Scatter:
    SEMS = 30

    @staticmethod
    def buffers(tok, d):
        q = tok // 4
        return [
            pltpu.VMEM((2, 4, 2, q, d), BF16),
            pltpu.VMEM((2, 4, 2, 2 * q, d), BF16),
            pltpu.VMEM((2, 3, 2 * q, d), BF16),
            pltpu.VMEM((2, 2, q, d), BF16),
            pltpu.VMEM((2, 2, 2 * q, d), BF16),
            pltpu.SemaphoreType.DMA,
            pltpu.SemaphoreType.DMA((Scatter.SEMS,)),
        ]

    def __init__(self, tor, part, bufs, order):
        self.tor, self.part, self.order = tor, part, order
        self.h1, self.f1, self.mid, self.h2, self.f2, self.ssem, self.rsem = bufs
        self.q = part.shape[1] // 4

    def copy(self, c, ph, bi, d, kind):
        q, first = self.q, c
        di = 0 if d == 1 else 1
        h = di if kind in (0, 2) else 1 - di
        step = 2 * d if kind == 0 else d
        if ph == 1:
            i = c * 8 + bi * 2 + di if kind == 0 else 16 + c * 4 + bi
            src = self.part.at[self.tor.slot(first, step, self.order[bi]), pl.ds(c * 2 * q + h * q, q)]
            dst = self.h1.at[c, bi, di] if kind == 0 else self.f1.at[c, bi, di, pl.ds(h * q, q)]
            to = self.tor.slot(first, d, 0)
        else:
            i = 24 + c * 2 + di if kind == 0 else 28 + c
            src = self.mid.at[c, self.order.index(2 if kind == 0 else d), pl.ds(h * q, q)]
            dst = self.h2.at[c, di] if kind == 0 else self.f2.at[c, di, pl.ds(h * q, q)]
            to = self.tor.slot(first, 0, d)
        return remote(src, dst, self.ssem, self.rsem.at[i], {"ty": to})

    def all_of(self, view, i):
        remote(view, view, self.ssem, self.rsem.at[i], {"ty": self.tor.me}).wait_recv()

    def issue(self, bi):
        for kind in BOTH:
            for c in BOTH:
                for d in DIRS:
                    self.copy(c, 1, bi, d, kind).start()

    def augment(self, bi):
        q = self.q
        for c in BOTH:
            for d in DIRS:
                di = 0 if d == 1 else 1
                self.copy(c, 1, bi, d, 0).wait_recv()
                mine = self.part.at[self.tor.slot(c, d, self.order[bi]), pl.ds(c * 2 * q + di * q, q)]
                add_rows(mine, [mine, self.h1.at[c, bi, di]])
                self.copy(c, 1, bi, d, 2).start()

    def arrived(self, bi):
        q = self.q
        for c in BOTH:
            self.all_of(self.f1.at[c, bi], 16 + c * 4 + bi)
            off = self.order[bi]
            if off == 0:
                continue
            own = self.part.at[self.tor.slot(c, 0, off), pl.ds(c * 2 * q, 2 * q)]
            add_rows(self.mid.at[c, bi], [own, self.f1.at[c, bi, 0], self.f1.at[c, bi, 1]])
            if off == 2:
                for d in DIRS:
                    self.copy(c, 2, 0, d, 0).start()
            else:
                self.copy(c, 2, 0, off, 1).start()

    def augment2(self, d):
        q = self.q
        di = 0 if d == 1 else 1
        for c in BOTH:
            self.copy(c, 2, 0, d, 0).wait_recv()
            mine = self.mid.at[c, self.order.index(d), pl.ds(di * q, q)]
            add_rows(mine, [mine, self.h2.at[c, di]])
            self.copy(c, 2, 0, d, 2).start()

    def last(self):
        for c in BOTH:
            self.all_of(self.f2.at[c], 28 + c)

    def finish(self, resid, out):
        q, d = self.q, out.shape[-1]
        width = min(512, d)
        for c in BOTH:
            rows = pl.ds(c * 2 * q, 2 * q)

            @pl.loop(0, d // width)
            def _(i):
                cols = pl.ds(pl.multiple_of(i * width, width), width)
                tot = self.part[self.tor.me, rows, cols].astype(F32)
                for di in BOTH:
                    tot += self.f1[c, self.order.index(0), di, :, cols].astype(F32)
                for di in BOTH:
                    tot += self.f2[c, di, :, cols].astype(F32)
                tot = tot.astype(BF16).astype(F32)
                out[rows, cols] = (resid[rows, cols].astype(F32) + tot).astype(BF16)

    def drain(self):
        view = self.part.at[pl.ds(0, self.part.shape[0] - 1)]
        remote(view, view, self.ssem, self.rsem.at[0], {"ty": self.tor.me}).wait_send()


class Exchange:
    def __init__(self, tx_count, src, dst, whole, ssem, rsem):
        self.n, self.src, self.dst, self.whole, self.ssem, self.rsem = tx_count, src, dst, whole, ssem, rsem
        self.me = lax.axis_index("tx")

    def start(self):
        for k in range(1, self.n):
            p = lax.rem(self.me + k, self.n)
            remote(self.src(p), self.dst(self.me), self.ssem, self.rsem, {"tx": p}).start()
        pltpu.make_async_copy(self.src(self.me), self.dst(self.me), self.rsem).start()

    def wait(self):
        view = self.whole(self.n)
        remote(view, view, self.ssem, self.rsem, {"tx": self.me}).wait_recv()

    def drain(self):
        view = self.whole(self.n - 1)
        remote(view, view, self.ssem, self.rsem, {"tx": self.me}).wait_send()


def norm_rows(src, dst):
    tok, d = src.shape
    step = 16

    @pl.loop(0, tok // step)
    def _(i):
        rows = pl.ds(pl.multiple_of(i * step, step), step)
        v = src[rows, :].astype(F32)
        mean = jnp.sum(v, axis=-1, keepdims=True) * (1.0 / d)
        var = jnp.sum(v * v, axis=-1, keepdims=True) * (1.0 / d) - mean * mean
        dst[rows, :] = ((v - mean) * lax.rsqrt(var + EPS)).astype(BF16)


class Ring:
    SEMS = 5

    def __init__(self, tx_count, rows, src, slot, whole, ssem, rsem):
        self.nx, self.rows, self.src, self.slot, self.whole, self.ssem, self.rsem = tx_count // 2, rows, src, slot, whole, ssem, rsem
        me = lax.axis_index("tx")
        self.me, self.x, self.core = me, lax.div(me, 2), lax.rem(me, 2)
        self.split = (rows // 2 + 15) // 16 * 16

    def tx(self, dx, other=False):
        return wrap(self.x + dx, self.nx) * 2 + (1 - self.core if other else self.core)

    def half(self, view, d):
        return view.at[pl.ds(0, self.split)] if d == 1 else view.at[pl.ds(self.split, self.rows - self.split)]

    def copy(self, i, src, dst, to):
        return remote(src, dst, self.ssem, self.rsem.at[i], {"tx": to})

    def pass_on(self, d, recv=False):
        view = self.slot(self.tx(-d if recv else 0))
        return self.copy(0 if d == 1 else 1, view if recv else self.src, view, self.tx(d))

    def relay(self, d, recv=False):
        view = self.half(self.slot(self.tx(-2 * d if recv else -d)), d)
        return self.copy(2 if d == 1 else 3, view, view, self.tx(d))

    def across(self, which, recv=False):
        view = self.slot(self.tx(which, recv))
        if abs(which) == 2:
            view = self.half(view, which // 2)
        src = self.src if which == 0 and not recv else view
        return self.copy(4, src, view, self.tx(0, True))

    def all_across(self):
        return (0, 1, -1, 2, -2) if self.nx > 1 else (0,)

    def own(self):
        return pltpu.make_async_copy(self.src, self.slot(self.me), self.rsem.at[4])

    def start(self, place=True):
        if self.nx > 1:
            for d in DIRS:
                self.pass_on(d).start()
        self.across(0).start()
        if place:
            self.own().start()

    def step(self):
        if self.nx > 1:
            for d in DIRS:
                self.pass_on(d, True).wait_recv()
                self.relay(d).start()
                self.across(-d).start()

    def step2(self):
        if self.nx > 1:
            for d in DIRS:
                self.relay(d, True).wait_recv()
                self.across(2 * d).start()

    def finish(self, place=True):
        view = self.whole(self.nx + (1 if place else 0))
        remote(view, view, self.ssem, self.rsem.at[4], {"tx": self.me}).wait_recv()

    def drain(self):
        view = self.whole(2 * self.nx - 1)
        remote(view, view, self.ssem, self.rsem.at[4], {"tx": self.me}).wait_send()


def layer_kernel(tx_count, x_ref, wq_ref, wk_ref, wv_ref, wo_ref, wg_ref, wu_ref, wd_ref, cos_hbm, sin_hbm, y_ref,
                 xp, x2, wqkv, wo, wg, wu, wd, xs, os_, act, kv, xt, h, yr, cos_ref, sin_ref,
                 load_sem, a2a_s, a2a_r, qkv_s, qkv_r, via_s, via_r, gs, gr, ws, wr, *rs_bufs):
    n_dev, tok, d = xp.shape
    dx = x_ref.shape[1]
    hc = wq_ref.shape[1]
    f, fp = wg_ref.shape[0], wg.shape[2]
    seq = tok * tx_count
    spd = n_dev // tx_count
    heads = hc // HEAD_DIM
    q2 = tok // 2
    c3 = 3 * hc
    tor = Torus()
    me_tx = lax.axis_index("tx")

    def exchange(i, src, dst, whole):
        return Exchange(tx_count, src, dst, whole, a2a_s.at[i], a2a_r.at[i])

    def col(start, width):
        return pl.ds(pl.multiple_of(start, width), width)

    def ring(i, src, buf, inner):
        return Ring(tx_count, src.shape[0], src, lambda o: buf.at[(o, *inner)], lambda n: buf.at[(pl.ds(0, n), *inner)], ws.at[i], wr.at[i])

    every = pl.ds(0, dx)
    rings = [ring(i, src, wqkv, (every, pl.ds(i * hc, hc))) for i, src in enumerate((wq_ref, wk_ref, wv_ref))]
    r_o = ring(3, wo_ref, wo, ())
    r_gate = ring(4, wg.at[me_tx], wg, ())
    r_up = ring(5, wu.at[me_tx], wu, ())
    r_down = ring(6, wd_ref, wd, (pl.ds(0, f),))

    x_in = pltpu.make_async_copy(x_ref, yr, load_sem.at[2])
    x_in.start()
    raw = [pltpu.make_async_copy(src, wd.at[i, pl.ds(0, f)], load_sem.at[i]) for i, src in enumerate((wg_ref, wu_ref))]
    raw += [pltpu.make_async_copy(cos_hbm, cos_ref, load_sem.at[3]), pltpu.make_async_copy(sin_hbm, sin_ref, load_sem.at[4])]
    for cp in raw:
        cp.start()
    entry_barrier(tor, tx_count)
    x_in.wait()
    xe = exchange(
        0,
        lambda p: yr.at[pl.ds(pl.multiple_of(p * tok, tok), tok)],
        lambda o: xt.at[:, col(o * dx, dx)],
        lambda n: yr.at[pl.ds(0, n * tok)],
    )
    xe.start()
    if fp > f:
        wd[:, pl.ds(f, fp - f), :] = jnp.zeros((tx_count, fp - f, dx), BF16)
    xe.wait()
    norm_rows(xt, xp.at[tor.me])
    g1 = Gather(tor, xp, gs, gr)
    g1.start()
    for r in rings:
        r.start()
    for cp in raw:
        cp.wait()
    for i, dst in enumerate((wg, wu)):
        for j in range(fp // 128):
            dst[me_tx, :, pl.ds(j * 128, 128)] = wd[i, pl.ds(j * 128, 128), :].T

    def pieces(off):
        return [(c, tor.slot(1 - c, off, n), (c * 4 + n) * q2) for c in BOTH for n in range(RING)]

    def stage(src, off, dst, cols):
        for c, s, at in pieces(off):
            dst[pl.ds(at, q2), :] = src[s, pl.ds(c * q2, q2), cols]

    detours = tx_count == 8
    x_pos = lax.div(me_tx, 2)
    edge = (x_pos == 0) | (x_pos == 3)
    opposite = jnp.where(x_pos == 0, 2, 1)
    inner = jnp.where(x_pos == 0, 1, 2)
    over = (3 - x_pos) * 2 + lax.rem(me_tx, 2)
    via = pl.ds(2 * c3 + 2 * hc, c3)

    def qkv_group(off):
        stage(xp, off, xs, pl.ds(0, d))

        @pl.loop(0, 3)
        def _(n):
            cols = col(n * hc, hc)
            out = jnp.dot(xs[...], wqkv[:, :, cols].reshape(d, hc), preferred_element_type=F32).astype(BF16)
            for c, s, at in pieces(off):
                x2[s, pl.ds(c * q2, q2), cols] = out[at : at + q2]

        def hand_out(chosen):
            for c, s, _ in pieces(off):
                p, sl = lax.div(s, spd), lax.rem(s, spd)
                now = chosen(sl)
                rows = pl.ds(c * q2, q2)
                src = x2.at[s, rows, pl.ds(0, c3)]
                dst = x2.at[sl * tx_count + me_tx, rows, pl.ds(c3, c3)]
                detour = (p != p) if off > 0 or not detours else edge & (lax.div(p, 2) == opposite)

                @pl.when(now & (p == me_tx))
                def _():
                    pltpu.make_async_copy(src, dst, qkv_r.at[sl]).start()

                @pl.when(now & detour)
                def _():
                    remote(src, x2.at[s, rows, via], qkv_s, via_r.at[2 * AWAY.index(off) + c], {"tx": over}).start()

                @pl.when(now & (p != me_tx) & jnp.logical_not(detour))
                def _():
                    remote(src, dst, qkv_s, qkv_r.at[sl], {"tx": p}).start()

        if off == 2:
            hand_out(lambda sl: sl < spd // 2)
            hand_out(lambda sl: sl >= spd // 2)
        else:
            hand_out(lambda sl: sl >= 0)

    def detour_rows(off, c):
        rows = pl.ds(c * q2, q2)
        return [(s, rows) for s in ([inner * RING + wrap(tor.pos[1] + off, RING)] if c == 0 else [inner * RING + y for y in range(RING)])]

    def pass_detour(off):
        if not detours:
            return
        for c in BOTH:

            @pl.when(edge if c == 0 else edge & (wrap(tor.pos[0] + off, RING) == inner))
            def _():
                for s, rows in detour_rows(off, c):
                    view = x2.at[s, rows, via]
                    if c == 0:
                        remote(view, view, via_s, via_r.at[2 * AWAY.index(off) + c], {"tx": me_tx}).wait_recv()
                if c == 1:
                    view = x2.at[pl.ds(inner * RING, 2), :, via]
                    remote(view, view, via_s, via_r.at[2 * AWAY.index(off) + c], {"tx": me_tx}).wait_recv()
                for s, rows in detour_rows(off, c):
                    p, sl = lax.div(s, spd), lax.rem(s, spd)
                    remote(x2.at[s, rows, via], x2.at[sl * tx_count + over, rows, pl.ds(c3, c3)], via_s, qkv_r.at[sl], {"tx": p}).start()

    def drain_detours():
        if not detours:
            return
        for off in (0, -1):
            for c in BOTH:

                @pl.when(edge if c == 0 else edge & (wrap(tor.pos[0] + off, RING) == inner))
                def _():
                    view = x2.at[0, pl.ds(0, q2), via] if c == 0 else x2.at[pl.ds(0, 2), :, via]
                    remote(view, view, via_s, via_r.at[0], {"tx": me_tx}).wait_send()

    xe.drain()
    wq_r, wk_r, wv_r = rings
    g1.near()
    wq_r.step()
    g1.relay(0)
    g1.spread(-1)
    g1.spread(1)
    wk_r.step()
    wv_r.step()
    g1.halves(0)
    wq_r.step2()
    wk_r.step2()
    g1.relay(-1)
    g1.far(False)
    wv_r.step2()
    for r in rings:
        r.finish()
    qkv_group(0)
    g1.relay(1)
    g1.far(True)
    g1.halves(-1)
    qkv_group(-1)
    g1.relay(2)
    g1.halves(1)
    qkv_group(1)
    pass_detour(0)
    g1.halves(2)
    qkv_group(2)
    pass_detour(-1)
    r_o.start()

    block = min(seq, 128)
    sends = []
    for s in range(spd):
        view = x2.at[pl.ds(s * tx_count, tx_count), :, pl.ds(c3, c3)]
        remote(view, view, qkv_s, qkv_r.at[s], {"tx": me_tx}).wait_recv()

        for hd in range(heads):
            def part(which, s=s, hd=hd):
                return x2[pl.ds(s * tx_count, tx_count), :, pl.ds(c3 + which * hc + hd * HEAD_DIM, HEAD_DIM)].reshape(seq, HEAD_DIM)

            for which in BOTH:
                v = part(which).astype(F32)
                rot = v * cos_ref[...] + pltpu.roll(v, HEAD_DIM // 2, 1) * sin_ref[...]
                kv[hd, which] = rot.astype(BF16)
            kv[hd, 2] = part(2)
            for b in range(seq // block):
                keys = (b + 1) * block
                sc = lax.dot_general(kv[hd, 0, pl.ds(b * block, block)], kv[hd, 1, pl.ds(0, keys)], (((1,), (1,)), ((), ())), preferred_element_type=F32)
                sc = sc * HEAD_DIM ** -0.5
                q_pos = b * block + lax.broadcasted_iota(jnp.int32, (block, keys), 0)
                k_pos = lax.broadcasted_iota(jnp.int32, (block, keys), 1)
                sc = jnp.where(q_pos >= k_pos, sc, -1e30)
                e = jnp.exp(sc - jnp.max(sc, axis=-1, keepdims=True))
                prob = (e / jnp.sum(e, axis=-1, keepdims=True)).astype(BF16)
                o = jnp.dot(prob, kv[hd, 2, pl.ds(0, keys)], preferred_element_type=F32).astype(BF16)
                for n in range(block // tok):
                    at = (b * (block // tok) + n) * spd + s
                    x2[at, :, pl.ds(2 * c3 + hd * HEAD_DIM, HEAD_DIM)] = o[n * tok : (n + 1) * tok]

        oe = exchange(
            1 + s,
            lambda p, s=s: x2.at[p * spd + s, :, pl.ds(2 * c3, hc)],
            lambda o, s=s: x2.at[o * spd + s, :, pl.ds(2 * c3 + hc, hc)],
            lambda n: x2.at[pl.ds(0, n), :, pl.ds(2 * c3, hc)],
        )
        oe.start()
        sends.append(oe)

    r_o.step()
    g1.drain()
    drain_detours()
    view = x2.at[pl.ds(0, (tx_count - 1) * spd), :, pl.ds(0, c3)]
    remote(view, view, qkv_s, qkv_r.at[0], {"tx": me_tx}).wait_send()
    for oe in sends:
        oe.wait()
        oe.drain()
    r_o.step2()
    r_gate.start(place=False)
    r_up.start(place=False)
    r_down.start()
    r_o.finish()

    def put(off, x, out):
        for c, s, at in pieces(off):
            xp[s, pl.ds(c * q2, q2), col(x * dx, dx)] = out[at : at + q2]

    def o_group(off):
        stage(x2, off, os_, pl.ds(2 * c3 + hc, hc))

        @pl.loop(0, tx_count)
        def _(x):
            put(off, x, jnp.dot(os_[...], wo[x], preferred_element_type=F32).astype(BF16))

    order = (2, -1, 1, 0)
    sc1 = Scatter(tor, xp, rs_bufs, order)
    o_group(order[0])
    sc1.issue(0)
    o_group(order[1])
    sc1.issue(1)
    o_group(order[2])
    sc1.augment(0)
    sc1.issue(2)
    o_group(order[3])
    sc1.augment(1)
    sc1.issue(3)
    sc1.arrived(0)
    r_gate.step()
    sc1.augment(2)
    sc1.arrived(1)
    sc1.augment2(-1)
    sc1.augment(3)
    sc1.arrived(2)
    sc1.augment2(1)
    r_up.step()
    sc1.arrived(3)
    sc1.last()
    sc1.finish(xt, h)
    norm_rows(h, x2.at[tor.me])
    g2 = Gather(tor, x2, gs, gr)
    g2.start()
    sc1.drain()

    def mlp_group(off, between, mid):
        stage(x2, off, xs, pl.ds(0, d))
        width = 256 if fp % 256 == 0 else 128

        @pl.loop(0, fp // width)
        def _(n):
            cols = col(n * width, width)
            gate = jnp.dot(xs[...], wg[:, :, cols].reshape(d, width), preferred_element_type=F32).astype(BF16).astype(F32)
            up = jnp.dot(xs[...], wu[:, :, cols].reshape(d, width), preferred_element_type=F32).astype(BF16).astype(F32)
            act[:, cols] = (gate * jax.nn.sigmoid(gate) * up).astype(BF16)

        between()
        half = tx_count // 2
        for lo, then in ((0, mid), (half, nothing)):

            @pl.loop(lo, lo + half)
            def _(x):
                put(off, x, jnp.dot(act[...], wd[x], preferred_element_type=F32).astype(BF16))

            then()

    sc2 = Scatter(tor, xp, rs_bufs, (-1, 1, 2, 0))
    g2.near()
    r_down.step()
    g2.relay(0)
    g2.spread(-1)
    g2.spread(1)
    r_gate.step2()
    r_up.step2()
    g2.halves(0)
    r_gate.finish(place=False)
    r_up.finish(place=False)

    def onward():
        g2.relay(-1)
        g2.far(False)
        r_down.step2()
        r_down.finish()

    mlp_group(0, onward, nothing)
    g2.relay(1)
    g2.far(True)
    g2.halves(-1)
    mlp_group(-1, nothing, lambda: g2.relay(2))
    sc2.issue(0)
    g2.halves(1)
    mlp_group(1, nothing, nothing)
    sc2.issue(1)
    g2.halves(2)
    mlp_group(2, nothing, nothing)
    sc2.issue(2)
    sc2.augment(0)
    sc2.augment(1)
    sc2.issue(3)
    sc2.arrived(0)
    sc2.augment(2)
    sc2.arrived(1)
    sc2.arrived(2)
    sc2.augment(3)
    sc2.augment2(-1)
    sc2.augment2(1)
    sc2.arrived(3)
    sc2.last()
    sc2.finish(h, xt)
    ye = exchange(
        1 + spd,
        lambda p: xt.at[:, col(p * dx, dx)],
        lambda o: yr.at[pl.ds(pl.multiple_of(o * tok, tok), tok)],
        lambda n: yr.at[pl.ds(0, n * tok)],
    )
    ye.start()
    g2.drain()
    sc2.drain()
    for r in rings + [r_o, r_gate, r_up, r_down]:
        r.drain()
    ye.wait()
    out = pltpu.make_async_copy(yr, y_ref, load_sem.at[0])
    out.start()
    ye.drain()
    out.wait()


ANY_SPEC = pl.BlockSpec(memory_space=pl.ANY)


def rotary_tables(seq_len):
    half = HEAD_DIM // 2
    inv_freq = (THETA ** (-2.0 * np.arange(half) / HEAD_DIM)).astype(np.float32)
    angles = np.arange(seq_len, dtype=np.float32)[:, None] * inv_freq[None, :]
    cos_t, sin_t = np.cos(angles), np.sin(angles)
    return np.concatenate([cos_t, cos_t], -1), np.concatenate([-sin_t, sin_t], -1)


def solution(mesh):
    tx_count, n_dev = mesh.shape["tx"], mesh.shape["ty"]
    act_spec = P(("dp", "ty"), None, "tx")
    col_spec = P("tx", "ty")
    row_spec = P("ty", "tx")
    dma = pltpu.SemaphoreType.DMA

    def layer_fn(x_blk, w_q, w_k, w_v, w_o, w_gate, w_up, w_down):
        seq, dx = x_blk.shape[1:]
        hc, f = w_q.shape[1], w_gate.shape[1]
        tok, d = seq // tx_count, dx * tx_count
        fp = -(-f // 128) * 128
        rows, spd = 4 * tok, n_dev // tx_count
        cos_t, sin_t = rotary_tables(seq)
        bf = lambda *shape: pltpu.VMEM(shape, BF16)
        scratch = [
            bf(n_dev, tok, d), bf(n_dev, tok, d), bf(tx_count, dx, 3 * hc), bf(tx_count, hc, dx),
            bf(tx_count, dx, fp), bf(tx_count, dx, fp), bf(tx_count, fp, dx),
            bf(rows, d), bf(rows, hc), bf(rows, fp), bf(hc // HEAD_DIM, 3, seq, HEAD_DIM), bf(tok, d), bf(tok, d), bf(seq, dx),
            pltpu.VMEM((seq, HEAD_DIM), F32), pltpu.VMEM((seq, HEAD_DIM), F32),
            dma((5,)), dma((spd + 2,)), dma((spd + 2,)), dma, dma((spd,)), dma, dma((4,)),
            dma, dma((Gather.SEMS,)), dma((7,)), dma((7, Ring.SEMS)),
        ] + Scatter.buffers(tok, d)
        y = pl.pallas_call(
            functools.partial(layer_kernel, tx_count),
            name="layer",
            out_shape=jax.ShapeDtypeStruct((seq, dx), BF16),
            in_specs=[ANY_SPEC] * 10,
            out_specs=ANY_SPEC,
            scratch_shapes=scratch,
            compiler_params=pltpu.CompilerParams(collective_id=1, has_side_effects=True, vmem_limit_bytes=67043328),
        )(x_blk[0], w_q, w_k, w_v, w_o, w_gate.T, w_up.T, w_down, cos_t, sin_t)
        return y[None]

    return jax.shard_map(layer_fn, mesh=mesh, in_specs=(act_spec, col_spec, col_spec, col_spec, row_spec, col_spec, col_spec, row_spec), out_specs=act_spec, check_vma=False)
```

```python
import functools

import numpy as np
import jax
import jax.numpy as jnp
from jax import lax
from jax.experimental import pallas as pl
from jax.experimental.pallas import tpu as pltpu
from jax.sharding import PartitionSpec as P

HEAD_DIM = 128
EPS = 1e-5
THETA = 10000.0
RING = 4
BOTH = (0, 1)
DIRS = (1, -1)
MESH = pl.DeviceIdType.MESH
BF16 = jnp.bfloat16
F32 = jnp.float32
AWAY = (0, -1, 1, 2)


def nothing():
    pass


def wrap(v, n):
    return lax.rem(v + 2 * n, n)


class Torus:
    def __init__(self):
        t = lax.axis_index("ty")
        self.me = t
        self.pos = (lax.div(t, RING), lax.rem(t, RING))

    def slot(self, first, a_off, b_off):
        a = wrap(self.pos[first] + a_off, RING)
        b = wrap(self.pos[1 - first] + b_off, RING)
        return a * RING + b if first == 0 else b * RING + a


def entry_barrier(tor, tx_count):
    sem = pltpu.get_barrier_semaphore()
    for first in (0, 1):
        for d in DIRS:
            pl.semaphore_signal(sem, inc=1, device_id={"ty": tor.slot(first, d, 0)}, device_id_type=MESH)
    me = lax.axis_index("tx")
    for k in range(1, tx_count):
        pl.semaphore_signal(sem, inc=1, device_id={"tx": lax.rem(me + k, tx_count)}, device_id_type=MESH)
    pl.semaphore_wait(sem, 4 + tx_count - 1)


def remote(src, dst, ssem, rsem, device):
    return pltpu.make_async_remote_copy(src_ref=src, dst_ref=dst, send_sem=ssem, recv_sem=rsem, device_id=device, device_id_type=MESH)


class Gather:
    SEMS = 25

    def __init__(self, tor, buf, ssem, rsem):
        self.tor, self.buf, self.ssem, self.rsem = tor, buf, ssem, rsem
        self.q = buf.shape[1] // 4

    def first(self, c):
        return 1 if c == 0 else 0

    def rows(self, c, d, half):
        if not half:
            return pl.ds(c * 2 * self.q, 2 * self.q)
        return pl.ds(c * 2 * self.q + (0 if d == 1 else self.q), self.q)

    def sem(self, c, ph, off, d, half):
        if half:
            return 20 + (0 if ph == 1 else 1 + AWAY.index(off))
        return (0 if ph == 1 else 4 + 4 * AWAY.index(off)) + c * 2 + (0 if d == 1 else 1)

    def copy(self, c, ph, off, d, half, hops):
        first = self.first(c)
        back = -d * hops
        s = self.tor.slot(first, back, 0) if ph == 1 else self.tor.slot(first, off, back)
        to = self.tor.slot(first, d, 0) if ph == 1 else self.tor.slot(first, 0, d)
        view = self.buf.at[s, self.rows(c, d, half)]
        return remote(view, view, self.ssem, self.rsem.at[self.sem(c, ph, off, d, half)], {"ty": to})

    def send(self, c, ph, off, d, half=False):
        self.copy(c, ph, off, d, half, 1 if half else 0).start()

    def recv(self, c, ph, off, d):
        self.copy(c, ph, off, d, False, 1).wait_recv()

    def far_copy(self, c, d, second, hops):
        s = self.tor.slot(self.first(c), 2, -d * hops)
        view = self.buf.at[s, self.rows(c, -d if second else d, True)]
        i = self.sem(c, 2, 2, d, second)
        return remote(view, view, self.ssem, self.rsem.at[i], {"ty": self.tor.slot(self.first(c), 0, d)})

    def recv_halves(self, ph, off):
        view = self.buf.at[pl.ds(0, 2)] if ph == off == 2 else self.buf.at[0]
        remote(view, view, self.ssem, self.rsem.at[self.sem(0, ph, off, 1, True)], {"ty": self.tor.me}).wait_recv()

    def start(self):
        for ph in (1, 2):
            for c in BOTH:
                for d in DIRS:
                    self.send(c, ph, 0, d)

    def near(self):
        for d in DIRS:
            for c in BOTH:
                self.recv(c, 1, 0, d)
                self.send(c, 1, 0, d, True)

    def spread(self, off):
        for c in BOTH:
            for d in DIRS:
                self.send(c, 2, off, d)

    def relay(self, off):
        for d in DIRS:
            for c in BOTH:
                if off == 2:
                    self.far_copy(c, d, False, 1).wait_recv()
                else:
                    self.recv(c, 2, off, d)
                self.send(c, 2, off, d, True)

    def far(self, second):
        if not second:
            self.recv_halves(1, 0)
        for c in BOTH:
            for d in DIRS:
                self.far_copy(c, d, second, 0).start()

    def halves(self, off):
        self.recv_halves(2, off)

    def drain(self):
        view = self.buf.at[pl.ds(0, self.buf.shape[0] - 1)]
        remote(view, view, self.ssem, self.rsem.at[0], {"ty": self.tor.me}).wait_send()


def add_rows(dst, srcs, width=512):
    d = dst.shape[-1]
    width = min(width, d)

    @pl.loop(0, d // width)
    def _(i):
        cols = pl.ds(pl.multiple_of(i * width, width), width)
        tot = srcs[0][:, cols].astype(F32)
        for s in srcs[1:]:
            tot += s[:, cols].astype(F32)
        dst[:, cols] = tot.astype(dst.dtype)


class Scatter:
    SEMS = 30

    @staticmethod
    def buffers(tok, d):
        q = tok // 4
        return [
            pltpu.VMEM((2, 4, 2, q, d), BF16),
            pltpu.VMEM((2, 4, 2, 2 * q, d), BF16),
            pltpu.VMEM((2, 3, 2 * q, d), BF16),
            pltpu.VMEM((2, 2, q, d), BF16),
            pltpu.VMEM((2, 2, 2 * q, d), BF16),
            pltpu.SemaphoreType.DMA,
            pltpu.SemaphoreType.DMA((Scatter.SEMS,)),
        ]

    def __init__(self, tor, part, bufs, order):
        self.tor, self.part, self.order = tor, part, order
        self.h1, self.f1, self.mid, self.h2, self.f2, self.ssem, self.rsem = bufs
        self.q = part.shape[1] // 4

    def copy(self, c, ph, bi, d, kind):
        q, first = self.q, c
        di = 0 if d == 1 else 1
        h = di if kind in (0, 2) else 1 - di
        step = 2 * d if kind == 0 else d
        if ph == 1:
            i = c * 8 + bi * 2 + di if kind == 0 else 16 + c * 4 + bi
            src = self.part.at[self.tor.slot(first, step, self.order[bi]), pl.ds(c * 2 * q + h * q, q)]
            dst = self.h1.at[c, bi, di] if kind == 0 else self.f1.at[c, bi, di, pl.ds(h * q, q)]
            to = self.tor.slot(first, d, 0)
        else:
            i = 24 + c * 2 + di if kind == 0 else 28 + c
            src = self.mid.at[c, self.order.index(2 if kind == 0 else d), pl.ds(h * q, q)]
            dst = self.h2.at[c, di] if kind == 0 else self.f2.at[c, di, pl.ds(h * q, q)]
            to = self.tor.slot(first, 0, d)
        return remote(src, dst, self.ssem, self.rsem.at[i], {"ty": to})

    def all_of(self, view, i):
        remote(view, view, self.ssem, self.rsem.at[i], {"ty": self.tor.me}).wait_recv()

    def issue(self, bi):
        for kind in BOTH:
            for c in BOTH:
                for d in DIRS:
                    self.copy(c, 1, bi, d, kind).start()

    def augment(self, bi):
        q = self.q
        for c in BOTH:
            for d in DIRS:
                di = 0 if d == 1 else 1
                self.copy(c, 1, bi, d, 0).wait_recv()
                mine = self.part.at[self.tor.slot(c, d, self.order[bi]), pl.ds(c * 2 * q + di * q, q)]
                add_rows(mine, [mine, self.h1.at[c, bi, di]])
                self.copy(c, 1, bi, d, 2).start()

    def arrived(self, bi):
        q = self.q
        for c in BOTH:
            self.all_of(self.f1.at[c, bi], 16 + c * 4 + bi)
            off = self.order[bi]
            if off == 0:
                continue
            own = self.part.at[self.tor.slot(c, 0, off), pl.ds(c * 2 * q, 2 * q)]
            add_rows(self.mid.at[c, bi], [own, self.f1.at[c, bi, 0], self.f1.at[c, bi, 1]])
            if off == 2:
                for d in DIRS:
                    self.copy(c, 2, 0, d, 0).start()
            else:
                self.copy(c, 2, 0, off, 1).start()

    def augment2(self, d):
        q = self.q
        di = 0 if d == 1 else 1
        for c in BOTH:
            self.copy(c, 2, 0, d, 0).wait_recv()
            mine = self.mid.at[c, self.order.index(d), pl.ds(di * q, q)]
            add_rows(mine, [mine, self.h2.at[c, di]])
            self.copy(c, 2, 0, d, 2).start()

    def last(self):
        for c in BOTH:
            self.all_of(self.f2.at[c], 28 + c)

    def finish(self, resid, out):
        q, d = self.q, out.shape[-1]
        width = min(512, d)
        for c in BOTH:
            rows = pl.ds(c * 2 * q, 2 * q)

            @pl.loop(0, d // width)
            def _(i):
                cols = pl.ds(pl.multiple_of(i * width, width), width)
                tot = self.part[self.tor.me, rows, cols].astype(F32)
                for di in BOTH:
                    tot += self.f1[c, self.order.index(0), di, :, cols].astype(F32)
                for di in BOTH:
                    tot += self.f2[c, di, :, cols].astype(F32)
                tot = tot.astype(BF16).astype(F32)
                out[rows, cols] = (resid[rows, cols].astype(F32) + tot).astype(BF16)

    def drain(self):
        view = self.part.at[pl.ds(0, self.part.shape[0] - 1)]
        remote(view, view, self.ssem, self.rsem.at[0], {"ty": self.tor.me}).wait_send()


class Exchange:
    def __init__(self, tx_count, src, dst, whole, ssem, rsem):
        self.n, self.src, self.dst, self.whole, self.ssem, self.rsem = tx_count, src, dst, whole, ssem, rsem
        self.me = lax.axis_index("tx")

    def start(self):
        for k in range(1, self.n):
            p = lax.rem(self.me + k, self.n)
            remote(self.src(p), self.dst(self.me), self.ssem, self.rsem, {"tx": p}).start()
        pltpu.make_async_copy(self.src(self.me), self.dst(self.me), self.rsem).start()

    def wait(self):
        view = self.whole(self.n)
        remote(view, view, self.ssem, self.rsem, {"tx": self.me}).wait_recv()

    def drain(self):
        view = self.whole(self.n - 1)
        remote(view, view, self.ssem, self.rsem, {"tx": self.me}).wait_send()


def norm_rows(src, dst):
    tok, d = src.shape
    step = 16

    @pl.loop(0, tok // step)
    def _(i):
        rows = pl.ds(pl.multiple_of(i * step, step), step)
        v = src[rows, :].astype(F32)
        mean = jnp.sum(v, axis=-1, keepdims=True) * (1.0 / d)
        var = jnp.sum(v * v, axis=-1, keepdims=True) * (1.0 / d) - mean * mean
        dst[rows, :] = ((v - mean) * lax.rsqrt(var + EPS)).astype(BF16)


class Ring:
    SEMS = 5

    def __init__(self, tx_count, rows, src, slot, whole, ssem, rsem):
        self.nx, self.rows, self.src, self.slot, self.whole, self.ssem, self.rsem = tx_count // 2, rows, src, slot, whole, ssem, rsem
        me = lax.axis_index("tx")
        self.me, self.x, self.core = me, lax.div(me, 2), lax.rem(me, 2)
        self.split = (rows // 2 + 15) // 16 * 16

    def tx(self, dx, other=False):
        return wrap(self.x + dx, self.nx) * 2 + (1 - self.core if other else self.core)

    def half(self, view, d):
        return view.at[pl.ds(0, self.split)] if d == 1 else view.at[pl.ds(self.split, self.rows - self.split)]

    def copy(self, i, src, dst, to):
        return remote(src, dst, self.ssem, self.rsem.at[i], {"tx": to})

    def pass_on(self, d, recv=False):
        view = self.slot(self.tx(-d if recv else 0))
        return self.copy(0 if d == 1 else 1, view if recv else self.src, view, self.tx(d))

    def relay(self, d, recv=False):
        view = self.half(self.slot(self.tx(-2 * d if recv else -d)), d)
        return self.copy(2 if d == 1 else 3, view, view, self.tx(d))

    def across(self, which, recv=False):
        view = self.slot(self.tx(which, recv))
        if abs(which) == 2:
            view = self.half(view, which // 2)
        src = self.src if which == 0 and not recv else view
        return self.copy(4, src, view, self.tx(0, True))

    def all_across(self):
        return (0, 1, -1, 2, -2) if self.nx > 1 else (0,)

    def own(self):
        return pltpu.make_async_copy(self.src, self.slot(self.me), self.rsem.at[4])

    def start(self, place=True):
        if self.nx > 1:
            for d in DIRS:
                self.pass_on(d).start()
        self.across(0).start()
        if place:
            self.own().start()

    def step(self):
        if self.nx > 1:
            for d in DIRS:
                self.pass_on(d, True).wait_recv()
                self.relay(d).start()
                self.across(-d).start()

    def step2(self):
        if self.nx > 1:
            for d in DIRS:
                self.relay(d, True).wait_recv()
                self.across(2 * d).start()

    def finish(self, place=True):
        view = self.whole(self.nx + (1 if place else 0))
        remote(view, view, self.ssem, self.rsem.at[4], {"tx": self.me}).wait_recv()

    def drain(self):
        view = self.whole(2 * self.nx - 1)
        remote(view, view, self.ssem, self.rsem.at[4], {"tx": self.me}).wait_send()


def layer_kernel(tx_count, x_ref, wq_ref, wk_ref, wv_ref, wo_ref, wg_ref, wu_ref, wd_ref, cos_hbm, sin_hbm, y_ref,
                 xp, x2, wqkv, wo, wg, wu, wd, xs, os_, act, kv, xt, h, yr, cos_ref, sin_ref,
                 load_sem, a2a_s, a2a_r, qkv_s, qkv_r, via_s, via_r, gs, gr, ws, wr, *rs_bufs):
    n_dev, tok, d = xp.shape
    dx = x_ref.shape[1]
    hc = wq_ref.shape[1]
    f, fp = wg_ref.shape[0], wg.shape[2]
    seq = tok * tx_count
    spd = n_dev // tx_count
    heads = hc // HEAD_DIM
    q2 = tok // 2
    c3 = 3 * hc
    tor = Torus()
    me_tx = lax.axis_index("tx")

    def exchange(i, src, dst, whole):
        return Exchange(tx_count, src, dst, whole, a2a_s.at[i], a2a_r.at[i])

    def col(start, width):
        return pl.ds(pl.multiple_of(start, width), width)

    def ring(i, src, buf, inner):
        return Ring(tx_count, src.shape[0], src, lambda o: buf.at[(o, *inner)], lambda n: buf.at[(pl.ds(0, n), *inner)], ws.at[i], wr.at[i])

    every = pl.ds(0, dx)
    rings = [ring(i, src, wqkv, (every, pl.ds(i * hc, hc))) for i, src in enumerate((wq_ref, wk_ref, wv_ref))]
    r_o = ring(3, wo_ref, wo, ())
    r_gate = ring(4, wg.at[me_tx], wg, ())
    r_up = ring(5, wu.at[me_tx], wu, ())
    r_down = ring(6, wd_ref, wd, (pl.ds(0, f),))

    x_in = pltpu.make_async_copy(x_ref, yr, load_sem.at[2])
    x_in.start()
    raw = [pltpu.make_async_copy(src, wd.at[i, pl.ds(0, f)], load_sem.at[i]) for i, src in enumerate((wg_ref, wu_ref))]
    raw += [pltpu.make_async_copy(cos_hbm, cos_ref, load_sem.at[3]), pltpu.make_async_copy(sin_hbm, sin_ref, load_sem.at[4])]
    for cp in raw:
        cp.start()
    entry_barrier(tor, tx_count)
    x_in.wait()
    xe = exchange(
        0,
        lambda p: yr.at[pl.ds(pl.multiple_of(p * tok, tok), tok)],
        lambda o: xt.at[:, col(o * dx, dx)],
        lambda n: yr.at[pl.ds(0, n * tok)],
    )
    xe.start()
    if fp > f:
        wd[:, pl.ds(f, fp - f), :] = jnp.zeros((tx_count, fp - f, dx), BF16)
    xe.wait()
    norm_rows(xt, xp.at[tor.me])
    g1 = Gather(tor, xp, gs, gr)
    g1.start()
    for r in rings:
        r.start()
    for cp in raw:
        cp.wait()
    for i, dst in enumerate((wg, wu)):
        for j in range(fp // 128):
            dst[me_tx, :, pl.ds(j * 128, 128)] = wd[i, pl.ds(j * 128, 128), :].T

    def pieces(off):
        return [(c, tor.slot(1 - c, off, n), (c * 4 + n) * q2) for c in BOTH for n in range(RING)]

    def stage(src, off, dst, cols):
        for c, s, at in pieces(off):
            dst[pl.ds(at, q2), :] = src[s, pl.ds(c * q2, q2), cols]

    detours = False
    x_pos = lax.div(me_tx, 2)
    edge = (x_pos == 0) | (x_pos == 3)
    opposite = jnp.where(x_pos == 0, 2, 1)
    inner = jnp.where(x_pos == 0, 1, 2)
    over = (3 - x_pos) * 2 + lax.rem(me_tx, 2)
    via = pl.ds(2 * c3 + 2 * hc, c3)

    def qkv_group(off):
        stage(xp, off, xs, pl.ds(0, d))

        @pl.loop(0, 3)
        def _(n):
            cols = col(n * hc, hc)
            out = jnp.dot(xs[...], wqkv[:, :, cols].reshape(d, hc), preferred_element_type=F32).astype(BF16)
            for c, s, at in pieces(off):
                x2[s, pl.ds(c * q2, q2), cols] = out[at : at + q2]

        for c, s, _ in pieces(off):
            p, sl = lax.div(s, spd), lax.rem(s, spd)
            rows = pl.ds(c * q2, q2)
            src = x2.at[s, rows, pl.ds(0, c3)]
            dst = x2.at[sl * tx_count + me_tx, rows, pl.ds(c3, c3)]

            detour = (p != p) if off > 0 or not detours else edge & (lax.div(p, 2) == opposite)

            @pl.when(p == me_tx)
            def _():
                pltpu.make_async_copy(src, dst, qkv_r.at[sl]).start()

            @pl.when(detour)
            def _():
                remote(src, x2.at[s, rows, via], qkv_s, via_r.at[2 * AWAY.index(off) + c], {"tx": over}).start()

            @pl.when((p != me_tx) & jnp.logical_not(detour))
            def _():
                remote(src, dst, qkv_s, qkv_r.at[sl], {"tx": p}).start()

    def detour_rows(off, c):
        rows = pl.ds(c * q2, q2)
        return [(s, rows) for s in ([inner * RING + wrap(tor.pos[1] + off, RING)] if c == 0 else [inner * RING + y for y in range(RING)])]

    def pass_detour(off):
        if not detours:
            return
        for c in BOTH:

            @pl.when(edge if c == 0 else edge & (wrap(tor.pos[0] + off, RING) == inner))
            def _():
                for s, rows in detour_rows(off, c):
                    view = x2.at[s, rows, via]
                    if c == 0:
                        remote(view, view, via_s, via_r.at[2 * AWAY.index(off) + c], {"tx": me_tx}).wait_recv()
                if c == 1:
                    view = x2.at[pl.ds(inner * RING, 2), :, via]
                    remote(view, view, via_s, via_r.at[2 * AWAY.index(off) + c], {"tx": me_tx}).wait_recv()
                for s, rows in detour_rows(off, c):
                    p, sl = lax.div(s, spd), lax.rem(s, spd)
                    remote(x2.at[s, rows, via], x2.at[sl * tx_count + over, rows, pl.ds(c3, c3)], via_s, qkv_r.at[sl], {"tx": p}).start()

    def drain_detours():
        if not detours:
            return
        for off in (0, -1):
            for c in BOTH:

                @pl.when(edge if c == 0 else edge & (wrap(tor.pos[0] + off, RING) == inner))
                def _():
                    view = x2.at[0, pl.ds(0, q2), via] if c == 0 else x2.at[pl.ds(0, 2), :, via]
                    remote(view, view, via_s, via_r.at[0], {"tx": me_tx}).wait_send()

    xe.drain()
    wq_r, wk_r, wv_r = rings
    g1.near()
    wq_r.step()
    g1.relay(0)
    g1.spread(-1)
    g1.spread(1)
    wk_r.step()
    wv_r.step()
    g1.halves(0)
    wq_r.step2()
    wk_r.step2()
    g1.relay(-1)
    g1.far(False)
    wv_r.step2()
    for r in rings:
        r.finish()
    qkv_group(0)
    g1.relay(1)
    g1.far(True)
    g1.halves(-1)
    qkv_group(-1)
    g1.relay(2)
    g1.halves(1)
    qkv_group(1)
    pass_detour(0)
    g1.halves(2)
    qkv_group(2)
    pass_detour(-1)
    r_o.start()

    block = min(seq, 128)
    sends = []
    for s in range(spd):
        view = x2.at[pl.ds(s * tx_count, tx_count), :, pl.ds(c3, c3)]
        remote(view, view, qkv_s, qkv_r.at[s], {"tx": me_tx}).wait_recv()

        @pl.loop(0, heads)
        def _(hd):
            def part(which):
                return x2[pl.ds(s * tx_count, tx_count), :, col(c3 + which * hc + hd * HEAD_DIM, HEAD_DIM)].reshape(seq, HEAD_DIM)

            for which in BOTH:
                v = part(which).astype(F32)
                rot = v * cos_ref[...] + pltpu.roll(v, HEAD_DIM // 2, 1) * sin_ref[...]
                kv[which] = rot.astype(BF16)
            kv[2] = part(2)
            for b in range(seq // block):
                keys = (b + 1) * block
                sc = lax.dot_general(kv[0, pl.ds(b * block, block)], kv[1, pl.ds(0, keys)], (((1,), (1,)), ((), ())), preferred_element_type=F32)
                sc = sc * HEAD_DIM ** -0.5
                q_pos = b * block + lax.broadcasted_iota(jnp.int32, (block, keys), 0)
                k_pos = lax.broadcasted_iota(jnp.int32, (block, keys), 1)
                sc = jnp.where(q_pos >= k_pos, sc, -1e30)
                e = jnp.exp(sc - jnp.max(sc, axis=-1, keepdims=True))
                prob = (e / jnp.sum(e, axis=-1, keepdims=True)).astype(BF16)
                o = jnp.dot(prob, kv[2, pl.ds(0, keys)], preferred_element_type=F32).astype(BF16)
                for n in range(block // tok):
                    at = (b * (block // tok) + n) * spd + s
                    x2[at, :, col(2 * c3 + hd * HEAD_DIM, HEAD_DIM)] = o[n * tok : (n + 1) * tok]

        oe = exchange(
            1 + s,
            lambda p, s=s: x2.at[p * spd + s, :, pl.ds(2 * c3, hc)],
            lambda o, s=s: x2.at[o * spd + s, :, pl.ds(2 * c3 + hc, hc)],
            lambda n: x2.at[pl.ds(0, n), :, pl.ds(2 * c3, hc)],
        )
        oe.start()
        sends.append(oe)

    r_o.step()
    g1.drain()
    drain_detours()
    view = x2.at[pl.ds(0, (tx_count - 1) * spd), :, pl.ds(0, c3)]
    remote(view, view, qkv_s, qkv_r.at[0], {"tx": me_tx}).wait_send()
    for oe in sends:
        oe.wait()
        oe.drain()
    r_o.step2()
    r_gate.start(place=False)
    r_up.start(place=False)
    r_down.start()
    r_o.finish()

    def put(off, x, out):
        for c, s, at in pieces(off):
            xp[s, pl.ds(c * q2, q2), col(x * dx, dx)] = out[at : at + q2]

    def o_group(off):
        stage(x2, off, os_, pl.ds(2 * c3 + hc, hc))

        @pl.loop(0, tx_count)
        def _(x):
            put(off, x, jnp.dot(os_[...], wo[x], preferred_element_type=F32).astype(BF16))

    order = (2, -1, 1, 0)
    sc1 = Scatter(tor, xp, rs_bufs, order)
    o_group(order[0])
    sc1.issue(0)
    o_group(order[1])
    sc1.issue(1)
    o_group(order[2])
    sc1.augment(0)
    sc1.issue(2)
    o_group(order[3])
    sc1.augment(1)
    sc1.issue(3)
    sc1.arrived(0)
    r_gate.step()
    sc1.augment(2)
    sc1.arrived(1)
    sc1.augment2(-1)
    sc1.augment(3)
    sc1.arrived(2)
    sc1.augment2(1)
    r_up.step()
    sc1.arrived(3)
    sc1.last()
    sc1.finish(xt, h)
    norm_rows(h, x2.at[tor.me])
    g2 = Gather(tor, x2, gs, gr)
    g2.start()
    sc1.drain()

    def mlp_group(off, between, mid):
        stage(x2, off, xs, pl.ds(0, d))
        width = 256 if fp % 256 == 0 else 128

        @pl.loop(0, fp // width)
        def _(n):
            cols = col(n * width, width)
            gate = jnp.dot(xs[...], wg[:, :, cols].reshape(d, width), preferred_element_type=F32).astype(BF16).astype(F32)
            up = jnp.dot(xs[...], wu[:, :, cols].reshape(d, width), preferred_element_type=F32).astype(BF16).astype(F32)
            act[:, cols] = (gate * jax.nn.sigmoid(gate) * up).astype(BF16)

        between()
        half = tx_count // 2
        for lo, then in ((0, mid), (half, nothing)):

            @pl.loop(lo, lo + half)
            def _(x):
                put(off, x, jnp.dot(act[...], wd[x], preferred_element_type=F32).astype(BF16))

            then()

    sc2 = Scatter(tor, xp, rs_bufs, (-1, 1, 2, 0))
    g2.near()
    r_down.step()
    g2.relay(0)
    g2.spread(-1)
    g2.spread(1)
    r_gate.step2()
    r_up.step2()
    g2.halves(0)
    r_gate.finish(place=False)
    r_up.finish(place=False)

    def onward():
        g2.relay(-1)
        g2.far(False)
        r_down.step2()
        r_down.finish()

    mlp_group(0, onward, nothing)
    g2.relay(1)
    g2.far(True)
    g2.halves(-1)
    mlp_group(-1, nothing, lambda: g2.relay(2))
    sc2.issue(0)
    g2.halves(1)
    mlp_group(1, nothing, nothing)
    sc2.issue(1)
    g2.halves(2)
    mlp_group(2, nothing, nothing)
    sc2.issue(2)
    sc2.augment(0)
    sc2.augment(1)
    sc2.issue(3)
    sc2.arrived(0)
    sc2.augment(2)
    sc2.arrived(1)
    sc2.arrived(2)
    sc2.augment(3)
    sc2.augment2(-1)
    sc2.augment2(1)
    sc2.arrived(3)
    sc2.last()
    sc2.finish(h, xt)
    ye = exchange(
        1 + spd,
        lambda p: xt.at[:, col(p * dx, dx)],
        lambda o: yr.at[pl.ds(pl.multiple_of(o * tok, tok), tok)],
        lambda n: yr.at[pl.ds(0, n * tok)],
    )
    ye.start()
    g2.drain()
    sc2.drain()
    for r in rings + [r_o, r_gate, r_up, r_down]:
        r.drain()
    ye.wait()
    out = pltpu.make_async_copy(yr, y_ref, load_sem.at[0])
    out.start()
    ye.drain()
    out.wait()


ANY_SPEC = pl.BlockSpec(memory_space=pl.ANY)


def rotary_tables(seq_len):
    half = HEAD_DIM // 2
    inv_freq = (THETA ** (-2.0 * np.arange(half) / HEAD_DIM)).astype(np.float32)
    angles = np.arange(seq_len, dtype=np.float32)[:, None] * inv_freq[None, :]
    cos_t, sin_t = np.cos(angles), np.sin(angles)
    return np.concatenate([cos_t, cos_t], -1), np.concatenate([-sin_t, sin_t], -1)


def solution(mesh):
    tx_count, n_dev = mesh.shape["tx"], mesh.shape["ty"]
    act_spec = P(("dp", "ty"), None, "tx")
    col_spec = P("tx", "ty")
    row_spec = P("ty", "tx")
    dma = pltpu.SemaphoreType.DMA

    def layer_fn(x_blk, w_q, w_k, w_v, w_o, w_gate, w_up, w_down):
        seq, dx = x_blk.shape[1:]
        hc, f = w_q.shape[1], w_gate.shape[1]
        tok, d = seq // tx_count, dx * tx_count
        fp = -(-f // 128) * 128
        rows, spd = 4 * tok, n_dev // tx_count
        cos_t, sin_t = rotary_tables(seq)
        bf = lambda *shape: pltpu.VMEM(shape, BF16)
        scratch = [
            bf(n_dev, tok, d), bf(n_dev, tok, d), bf(tx_count, dx, 3 * hc), bf(tx_count, hc, dx),
            bf(tx_count, dx, fp), bf(tx_count, dx, fp), bf(tx_count, fp, dx),
            bf(rows, d), bf(rows, hc), bf(rows, fp), bf(3, seq, HEAD_DIM), bf(tok, d), bf(tok, d), bf(seq, dx),
            pltpu.VMEM((seq, HEAD_DIM), F32), pltpu.VMEM((seq, HEAD_DIM), F32),
            dma((5,)), dma((spd + 2,)), dma((spd + 2,)), dma, dma((spd,)), dma, dma((4,)),
            dma, dma((Gather.SEMS,)), dma((7,)), dma((7, Ring.SEMS)),
        ] + Scatter.buffers(tok, d)
        y = pl.pallas_call(
            functools.partial(layer_kernel, tx_count),
            name="layer",
            out_shape=jax.ShapeDtypeStruct((seq, dx), BF16),
            in_specs=[ANY_SPEC] * 10,
            out_specs=ANY_SPEC,
            scratch_shapes=scratch,
            compiler_params=pltpu.CompilerParams(collective_id=1, has_side_effects=True, vmem_limit_bytes=67043328),
        )(x_blk[0], w_q, w_k, w_v, w_o, w_gate.T, w_up.T, w_down, cos_t, sin_t)
        return y[None]

    return jax.shard_map(layer_fn, mesh=mesh, in_specs=(act_spec, col_spec, col_spec, col_spec, row_spec, col_spec, col_spec, row_spec), out_specs=act_spec, check_vma=False)
```
